32 devices in a mesh: fsdp: 32 (over z, y, x, core).
Axes of the slice: x: 2, y: 2, z: 4, core: 2. Of those that a mesh axis runs over, the one named last changes fastest.
Arguments:
- token_ids: int32 [128, 384], P('fsdp')
- tok_table: bfloat16 [501248, 768], P('fsdp')
- pos_table: bfloat16 [512, 768], replicated
- type_row: bfloat16 [768], replicated
- emb_gain: float32 [768], P('fsdp')
- emb_bias: float32 [768], P('fsdp')
- w_qkv: bfloat16 [768, 2304], P(None, 'fsdp')
- b_qkv: float32 [2304], P('fsdp')
- w_out: bfloat16 [12, 64, 768], P(None, None, 'fsdp')
- b_out: float32 [768], P('fsdp')
- ln1_gain: float32 [768], P('fsdp')
- ln1_bias: float32 [768], P('fsdp')
- w_ffn_in: bfloat16 [768, 3072], P(None, 'fsdp')
- b_ffn_in: float32 [3072], P('fsdp')
- w_ffn_out: bfloat16 [3072, 768], P('fsdp')
- b_ffn_out: float32 [768], P('fsdp')
- ln2_gain: float32 [768], P('fsdp')
- ln2_bias: float32 [768], P('fsdp')
Outputs:
- output: bfloat16 [128, 384, 768], P('fsdp')
All inputs are finite; a program needn't handle non-finite values.
Results may differ from the reference program's by a relative error of at most 0.00883599.
Values are sent between devices in bfloat16 or wider.
A program may use at most 1 GiB of HBM per device.

```python
import jax
import jax.numpy as jnp
from jax import lax

VOCAB_ROWS = 501248
HIDDEN = 768
NUM_HEADS = 12
HEAD_DIM = 64
FFN_DIM = 3072
POS_ROWS = 512
BATCH_SIZE = 128
SEQ_LEN = 384
PAD_ID = 1
LN_EPS = 1e-5


def layer_norm(values, ln_gain, ln_shift):
    row_mean = jnp.mean(values, axis=-1, keepdims=True)
    centered = values - row_mean
    row_var = jnp.mean(centered * centered, axis=-1, keepdims=True)
    return centered * lax.rsqrt(row_var + LN_EPS) * ln_gain + ln_shift


def draw_ids(id_key):
    id_keys = jax.random.split(id_key, 5)
    id_shape = (BATCH_SIZE, SEQ_LEN)
    pick_kind = jax.random.randint(id_keys[0], id_shape, 0, 2)
    flat_ids = jax.random.randint(id_keys[1], id_shape, 2, VOCAB_ROWS)
    zipf_level = jax.random.randint(id_keys[2], id_shape, 1, 19)
    level_span = jnp.minimum(jnp.left_shift(jnp.ones(id_shape, jnp.int32), zipf_level), VOCAB_ROWS - 2)
    skewed = 2 + jax.random.randint(id_keys[3], id_shape, 0, level_span)
    content = jnp.where(pick_kind == 0, flat_ids, skewed)
    lengths = jax.random.randint(id_keys[4], (BATCH_SIZE,), SEQ_LEN // 4, SEQ_LEN + 1)
    lengths = lengths.at[0].set(SEQ_LEN)
    col_index = jnp.arange(SEQ_LEN)[None, :]
    token_ids = jnp.where(col_index < lengths[:, None], content, PAD_ID)
    token_ids = token_ids.at[:, 0].set(0)
    token_ids = token_ids.at[0, 1].set(VOCAB_ROWS - 1)
    return token_ids.astype(jnp.int32)


def setup_inputs(seed: int = 0) -> dict:
    root_key = jax.random.key(seed)
    draw_keys = jax.random.split(root_key, 18)

    def normal(index, shape):
        return jax.random.normal(draw_keys[index], shape, jnp.float32)

    return {
        'token_ids': draw_ids(draw_keys[0]),
        'tok_table': normal(1, (VOCAB_ROWS, HIDDEN)).astype(jnp.bfloat16),
        'pos_table': normal(2, (POS_ROWS, HIDDEN)).astype(jnp.bfloat16),
        'type_row': normal(3, (HIDDEN,)).astype(jnp.bfloat16),
        'emb_gain': 1.0 + 0.3 * normal(4, (HIDDEN,)),
        'emb_bias': 0.3 * normal(5, (HIDDEN,)),
        'w_qkv': (normal(6, (HIDDEN, 3 * HIDDEN)) * HIDDEN ** -0.5).astype(jnp.bfloat16),
        'b_qkv': 0.3 * normal(7, (3 * HIDDEN,)),
        'w_out': (normal(8, (NUM_HEADS, HEAD_DIM, HIDDEN)) * HIDDEN ** -0.5).astype(jnp.bfloat16),
        'b_out': 0.3 * normal(9, (HIDDEN,)),
        'ln1_gain': 1.0 + 0.3 * normal(10, (HIDDEN,)),
        'ln1_bias': 0.3 * normal(11, (HIDDEN,)),
        'w_ffn_in': (normal(12, (HIDDEN, FFN_DIM)) * HIDDEN ** -0.5).astype(jnp.bfloat16),
        'b_ffn_in': 0.3 * normal(13, (FFN_DIM,)),
        'w_ffn_out': (normal(14, (FFN_DIM, HIDDEN)) * FFN_DIM ** -0.5).astype(jnp.bfloat16),
        'b_ffn_out': 0.3 * normal(15, (HIDDEN,)),
        'ln2_gain': 1.0 + 0.3 * normal(16, (HIDDEN,)),
        'ln2_bias': 0.3 * normal(17, (HIDDEN,)),
    }


def reference(token_ids, tok_table, pos_table, type_row, emb_gain, emb_bias, w_qkv, b_qkv, w_out, b_out,
              ln1_gain, ln1_bias, w_ffn_in, b_ffn_in, w_ffn_out, b_ffn_out, ln2_gain, ln2_bias):
    score_scale = HEAD_DIM ** -0.5
    w_out_flat = w_out.reshape(NUM_HEADS * HEAD_DIM, HIDDEN)

    def one_sequence(seq_ids):
        keep_mask = seq_ids != PAD_ID
        keep_int = keep_mask.astype(jnp.int32)
        positions = jnp.cumsum(keep_int) * keep_int + 1
        embedded = (tok_table[seq_ids].astype(jnp.float32) + pos_table[positions].astype(jnp.float32)
                    + type_row.astype(jnp.float32))
        x_embed = layer_norm(embedded, emb_gain, emb_bias).astype(jnp.bfloat16)
        qkv_rows = (jnp.dot(x_embed, w_qkv, preferred_element_type=jnp.float32) + b_qkv).astype(jnp.bfloat16)
        qkv_heads = qkv_rows.reshape(SEQ_LEN, 3, NUM_HEADS, HEAD_DIM).astype(jnp.float32)
        scores = jnp.einsum('qhd,khd->hqk', qkv_heads[:, 0], qkv_heads[:, 1]) * score_scale
        scores = jnp.where(keep_mask[None, None, :], scores, -1e30)
        attn_probs = jax.nn.softmax(scores, axis=-1).astype(jnp.bfloat16)
        context = jnp.einsum('hqk,khd->qhd', attn_probs.astype(jnp.float32), qkv_heads[:, 2]).astype(jnp.bfloat16)
        attn_out = (jnp.dot(context.reshape(SEQ_LEN, NUM_HEADS * HEAD_DIM), w_out_flat,
                            preferred_element_type=jnp.float32) + b_out).astype(jnp.bfloat16)
        x_attn = layer_norm(x_embed.astype(jnp.float32) + attn_out.astype(jnp.float32),
                            ln1_gain, ln1_bias).astype(jnp.bfloat16)
        hidden = jax.nn.gelu(jnp.dot(x_attn, w_ffn_in, preferred_element_type=jnp.float32) + b_ffn_in,
                             approximate=False).astype(jnp.bfloat16)
        ffn_out = jnp.dot(hidden, w_ffn_out, preferred_element_type=jnp.float32) + b_ffn_out
        return layer_norm(x_attn.astype(jnp.float32) + ffn_out, ln2_gain, ln2_bias).astype(jnp.bfloat16)

    return lax.map(one_sequence, token_ids)
```

```python
import jax
import jax.numpy as jnp
from jax import lax
from jax.experimental import pallas as pl
from jax.experimental.pallas import tpu as pltpu
from jax.sharding import PartitionSpec as P

PAD_ID = 1
LN_EPS = 1e-5


def layer_norm(values, ln_gain, ln_shift):
    row_mean = jnp.mean(values, axis=-1, keepdims=True)
    centered = values - row_mean
    row_var = jnp.mean(centered * centered, axis=-1, keepdims=True)
    return centered * lax.rsqrt(row_var + LN_EPS) * ln_gain + ln_shift


def attention(qkv_heads, keep_mask, head_dim):
    scores = jnp.einsum('bqhd,bkhd->bhqk', qkv_heads[:, :, 0], qkv_heads[:, :, 1],
                        preferred_element_type=jnp.float32) * head_dim ** -0.5
    scores = jnp.where(keep_mask[:, None, None, :], scores, -1e30)
    attn_probs = jax.nn.softmax(scores, axis=-1).astype(jnp.bfloat16)
    return jnp.einsum('bhqk,bkhd->bqhd', attn_probs, qkv_heads[:, :, 2],
                      preferred_element_type=jnp.float32).astype(jnp.bfloat16)


HEAD = 2048
CAPS = ((0, 1, 184), (1, 2, 96), (2, 4, 72), (4, 32, 48))
EXTRA = 48
MESH = pl.DeviceIdType.MESH


def others(n, me, one):
    def body(k, carry):
        one(k, lax.rem(me + k, n))
        return carry

    lax.fori_loop(1, n, body, 0)


def meet(n, me):
    barrier = pltpu.get_barrier_semaphore()
    others(n, me, lambda k, dev: pl.semaphore_signal(barrier, inc=1, device_id=(dev,), device_id_type=MESH))
    pl.semaphore_wait(barrier, n - 1)


def tell_kernel(n, part, msg_ref, table_ref, told_ref, piece_ref, send_sem, recv_sem, out_sem, in_sem, own_sem):
    me = lax.axis_index('fsdp')
    meet(n, me)

    def note(k, dev, slot):
        return pltpu.make_async_remote_copy(msg_ref, told_ref.at[slot], send_sem.at[k], recv_sem.at[slot],
                                            device_id=(dev,), device_id_type=MESH)

    def head(dev):
        return pltpu.make_async_remote_copy(table_ref.at[pl.ds(pl.multiple_of(dev * part, 8), part)], piece_ref,
                                            out_sem.at[dev], in_sem, device_id=(dev,), device_id_type=MESH)

    def own():
        return pltpu.make_async_copy(table_ref.at[pl.ds(0, part)], piece_ref, own_sem)

    others(n, me, lambda k, dev: note(k, dev, me).start())

    @pl.when(me == 0)
    def _():
        others(n, me, lambda k, dev: head(dev).start())
        own().start()

    told_ref[me] = msg_ref[...]
    others(n, me, lambda k, dev: note(k, dev, dev).wait_recv())
    others(n, me, lambda k, dev: note(k, dev, me).wait_send())

    @pl.when(me == 0)
    def _():
        own().wait()
        others(n, me, lambda k, dev: head(dev).wait_send())

    @pl.when(me != 0)
    def _():
        head(me).wait_recv()


def tell(n, msg, table):
    part = HEAD // n
    return pl.pallas_call(
        lambda *refs: tell_kernel(n, part, *refs),
        out_shape=(jax.ShapeDtypeStruct((n,) + msg.shape, msg.dtype),
                   jax.ShapeDtypeStruct((part, table.shape[1]), table.dtype)),
        in_specs=[pl.BlockSpec(memory_space=pltpu.VMEM), pl.BlockSpec(memory_space=pl.ANY)],
        out_specs=(pl.BlockSpec(memory_space=pltpu.VMEM), pl.BlockSpec(memory_space=pltpu.VMEM)),
        scratch_shapes=[pltpu.SemaphoreType.DMA((n,)), pltpu.SemaphoreType.DMA((n,)), pltpu.SemaphoreType.DMA((n,)),
                        pltpu.SemaphoreType.DMA, pltpu.SemaphoreType.DMA],
        compiler_params=pltpu.CompilerParams(collective_id=0, has_side_effects=True))(msg, table)


def bases():
    out, at = [], 0
    for lo, hi, cap in CAPS:
        out.append(at)
        at += (hi - lo) * cap
    return out, at


def swap_kernel(n, send_ref, recv_ref, send_sem, recv_sem, own_sem):
    me = lax.axis_index('fsdp')
    meet(n, me)
    starts, _ = bases()

    def spot(c, dev):
        lo, _, cap = CAPS[c]
        return recv_ref.at[pl.ds(pl.multiple_of(starts[c] + (dev - lo) * cap, 8), cap)]

    def row(c, k, dev, owner):
        return pltpu.make_async_remote_copy(send_ref.at[dev, pl.ds(0, CAPS[c][2])], spot(c, owner), send_sem.at[k],
                                            recv_sem.at[owner], device_id=(dev,), device_id_type=MESH)

    def own(c):
        return pltpu.make_async_copy(send_ref.at[me, pl.ds(0, CAPS[c][2])], spot(c, me), own_sem)

    for c, (lo, hi, cap) in enumerate(CAPS):
        @pl.when((me >= lo) & (me < hi))
        def _(c=c):
            others(n, me, lambda k, dev: row(c, k, dev, me).start())
            own(c).start()

    for c, (lo, hi, cap) in enumerate(CAPS):
        def one(dev, carry, c=c):
            @pl.when(dev != me)
            def _():
                row(c, 0, dev, dev).wait_recv()

            return carry

        lax.fori_loop(lo, hi, one, 0)

    for c, (lo, hi, cap) in enumerate(CAPS):
        @pl.when((me >= lo) & (me < hi))
        def _(c=c):
            others(n, me, lambda k, dev: row(c, k, dev, me).wait_send())
            own(c).wait()


def swap(n, rows):
    return pl.pallas_call(
        lambda *refs: swap_kernel(n, *refs),
        out_shape=jax.ShapeDtypeStruct((bases()[1], rows.shape[2]), rows.dtype),
        in_specs=[pl.BlockSpec(memory_space=pl.ANY)], out_specs=pl.BlockSpec(memory_space=pl.ANY),
        scratch_shapes=[pltpu.SemaphoreType.DMA((n,)), pltpu.SemaphoreType.DMA((n,)), pltpu.SemaphoreType.DMA],
        compiler_params=pltpu.CompilerParams(collective_id=1, has_side_effects=True))(rows)


def solution(mesh):
    def local_step(token_ids, tok_shard, pos_table, type_row, emb_gain, emb_bias, w_qkv, b_qkv, w_out, b_out,
                   ln1_gain, ln1_bias, w_ffn_in, b_ffn_in, w_ffn_out, b_ffn_out, ln2_gain, ln2_bias):
        n_dev = mesh.shape['fsdp']
        me = lax.axis_index('fsdp')
        batch_dev, seq_len = token_ids.shape
        n_tok = batch_dev * seq_len
        shard_rows, width = tok_shard.shape
        num_heads, head_dim = w_out.shape[0], w_out.shape[1]
        pieces = [w_qkv.T, w_out.reshape(num_heads * head_dim, -1).T, w_ffn_in.T, w_ffn_out]
        sizes = [p.shape[0] for p in pieces]
        weights = lax.all_gather(jnp.concatenate(pieces, axis=0), 'fsdp', axis=0, tiled=False)
        full, at = [], 0
        for size in sizes:
            full.append(weights[:, at:at + size].reshape(n_dev * size, width))
            at += size
        w_qkv_t, w_out_t, w_in_t, w_back = full

        ids = token_ids.reshape(n_tok)
        keep = ids != PAD_ID
        asks = keep & (ids >= HEAD)
        owner = jnp.where(asks, ids // shard_rows, n_dev)
        place = jnp.arange(n_tok, dtype=jnp.int32)
        lanes = jnp.arange(128, dtype=jnp.int32)
        mine = (owner[:, None] == lanes[None, :]) & (lanes < n_dev)[None, :]
        before = (place[None, :] < place[:, None]).astype(jnp.bfloat16)
        ranks = jnp.dot(before, mine.astype(jnp.bfloat16), preferred_element_type=jnp.float32)
        count = jnp.sum(mine.astype(jnp.float32), axis=0)
        rank = jnp.sum(jnp.where(mine, ranks, 0.0), axis=1).astype(jnp.int32)
        starts, slots = bases()
        cap, base = jnp.zeros_like(owner), jnp.zeros_like(owner)
        for (lo, hi, c), b in zip(CAPS, starts):
            inside = (owner >= lo) & (owner < hi)
            cap = jnp.where(inside, c, cap)
            base = jnp.where(inside, b + (owner - lo) * c, base)
        fits = rank < cap
        slot = jnp.where(fits, base + rank, -1)
        wide = slots + -slots % 128
        slotted = jnp.sum(jnp.where(slot[:, None] == jnp.arange(wide, dtype=jnp.int32)[None, :],
                                    ids.astype(jnp.float32)[:, None], 0.0), axis=0)

        small = [emb_gain, emb_bias, ln1_gain, ln1_bias, ln2_gain, ln2_bias, b_out, b_ffn_out, b_qkv, b_ffn_in]
        message = jnp.concatenate([slotted, count] + small)
        message = jnp.pad(message, (0, -message.shape[0] % 1024))
        told, piece = tell(n_dev, message.reshape(-1, 128), tok_shard)
        told = told.reshape(n_dev, -1)
        head = lax.all_gather(piece, 'fsdp', axis=0, tiled=True)
        at = wide + 128
        vectors = []
        for v in small:
            vectors.append(told[:, at:at + v.shape[0]].reshape(-1))
            at += v.shape[0]
        emb_g, emb_b, ln1_g, ln1_b, ln2_g, ln2_b, b_out_f, b_back_f, b_qkv_f, b_in_f = vectors

        my_base = jnp.int32(0)
        for (lo, hi, c), b in zip(CAPS, starts):
            my_base = jnp.where((me >= lo) & (me < hi), b + (me - lo) * c, my_base)
        most = max(c for _, _, c in CAPS)
        wanted = lax.dynamic_slice(told, (0, my_base), (n_dev, most)).astype(jnp.int32) - me * shard_rows
        wanted = jnp.clip(wanted, 0, shard_rows - 1)
        rows = jnp.take(tok_shard, wanted.reshape(-1), axis=0, mode='clip').reshape(n_dev, most, width)
        got = swap(n_dev, rows)
        spot = jnp.where(ids < HEAD, ids, HEAD + jnp.maximum(slot, 0))
        tok_rows = jnp.take(jnp.concatenate([head, got], axis=0), spot, axis=0, mode='clip')

        caps = jnp.concatenate([jnp.full((hi - lo,), c, jnp.float32) for lo, hi, c in CAPS])
        left = jnp.max(told[:, wide:wide + n_dev] - caps[None, :])
        rounds = (jnp.maximum(left, 0.0).astype(jnp.int32) + EXTRA - 1) // EXTRA

        def again(state):
            r, rows_now = state
            extra = rank - cap - r * EXTRA
            live = asks & (extra >= 0) & (extra < EXTRA)
            at_slot = jnp.where(live, owner * EXTRA + extra, n_dev * EXTRA)
            ask = jnp.zeros((n_dev * EXTRA + 1,), jnp.int32).at[at_slot].set(ids)[:-1]
            asked = lax.all_to_all(ask.reshape(n_dev, EXTRA), 'fsdp', 0, 0, tiled=True)
            asked = jnp.clip(asked - me * shard_rows, 0, shard_rows - 1)
            found = jnp.take(tok_shard, asked.reshape(-1), axis=0, mode='clip').reshape(n_dev, EXTRA, width)
            back = lax.all_to_all(found, 'fsdp', 0, 0, tiled=True).reshape(n_dev * EXTRA, width)
            new = jnp.take(back, jnp.where(live, at_slot, 0), axis=0, mode='clip')
            return r + 1, jnp.where(live[:, None], new, rows_now)

        _, tok_rows = lax.while_loop(lambda state: state[0] < rounds, again, (jnp.int32(0), tok_rows))
        tok_rows = tok_rows.reshape(batch_dev, seq_len, width)

        keep_mask = token_ids != PAD_ID
        keep_int = keep_mask.astype(jnp.int32)
        positions = jnp.cumsum(keep_int, axis=1) * keep_int + 1
        embedded = (tok_rows.astype(jnp.float32) + jnp.take(pos_table, positions, axis=0).astype(jnp.float32)
                    + type_row.astype(jnp.float32))
        x_embed = layer_norm(embedded, emb_g, emb_b).astype(jnp.bfloat16)
        qkv_rows = (jnp.einsum('btd,ed->bte', x_embed, w_qkv_t, preferred_element_type=jnp.float32)
                    + b_qkv_f).astype(jnp.bfloat16)
        qkv_heads = qkv_rows.reshape(batch_dev, seq_len, 3, num_heads, head_dim)
        context = attention(qkv_heads, keep_mask, head_dim).reshape(batch_dev, seq_len, width)
        attn_out = (jnp.einsum('bqc,ec->bqe', context, w_out_t, preferred_element_type=jnp.float32)
                    + b_out_f).astype(jnp.bfloat16)
        x_attn = layer_norm(x_embed.astype(jnp.float32) + attn_out.astype(jnp.float32), ln1_g, ln1_b).astype(jnp.bfloat16)
        hidden = jax.nn.gelu(jnp.einsum('btd,fd->btf', x_attn, w_in_t, preferred_element_type=jnp.float32)
                             + b_in_f, approximate=False).astype(jnp.bfloat16)
        ffn_out = jnp.einsum('btf,fd->btd', hidden, w_back, preferred_element_type=jnp.float32) + b_back_f
        return layer_norm(x_attn.astype(jnp.float32) + ffn_out, ln2_g, ln2_b).astype(jnp.bfloat16)

    vec_spec = P('fsdp')
    in_specs = (P('fsdp', None), P('fsdp', None), P(None, None), P(None), vec_spec, vec_spec,
                P(None, 'fsdp'), vec_spec, P(None, None, 'fsdp'), vec_spec, vec_spec, vec_spec,
                P(None, 'fsdp'), vec_spec, P('fsdp', None), vec_spec, vec_spec, vec_spec)
    return jax.shard_map(local_step, mesh=mesh, in_specs=in_specs, out_specs=P('fsdp', None, None),
                         check_vma=False)
```

```python
import functools

import jax
import jax.numpy as jnp
from jax import lax
from jax.experimental import pallas as pl
from jax.experimental.pallas import tpu as pltpu
from jax.sharding import PartitionSpec as P


PAD_ID = 1
LN_EPS = 1e-5


SQRT_HALF = 0.5 ** 0.5
FFN_PART = 768


def norm(z, gain, shift):
    centered = z - jnp.mean(z, axis=-1, keepdims=True)
    var = jnp.mean(centered * centered, axis=-1, keepdims=True)
    return centered * lax.rsqrt(var + LN_EPS) * gain + shift


def times(a, b):
    return jnp.dot(a, b, preferred_element_type=jnp.float32)


def times_t(a, b):
    return lax.dot_general(a, b, (((1,), (1,)), ((), ())), preferred_element_type=jnp.float32)


def layer_kernel(dims, spot_ref, keep_col_ref, keep_row_ref, head_ref, got_ref, pos_ref, type_ref, vec_ref, b_qkv_ref, b_in_ref,
                 w_qkv_ref, w_out_ref, w_in_ref, w_back_ref, out_ref, qkv_ref, ctx_ref, x_ref):
    heads, size = dims
    seq, width = out_ref.shape[1:]
    w_qkv_ref, w_out_ref, w_in_ref, w_back_ref = (
        r.reshape(r.shape[0] * r.shape[1], width) for r in (w_qkv_ref, w_out_ref, w_in_ref, w_back_ref))
    spot = spot_ref[0]
    total = jnp.zeros((seq, width), jnp.float32)
    step = 256
    for ref, first in ((head_ref, 0), (got_ref, head_ref.shape[0])):
        for at in range(0, ref.shape[0], step):
            hit = spot == lax.broadcasted_iota(jnp.int32, (seq, step), 1) + (first + at)
            total += times(jnp.where(hit, 1.0, 0.0).astype(jnp.bfloat16), ref[at:at + step, :])
    kept = keep_col_ref[0] > 0
    pos = jnp.where(kept, pos_ref[8:8 + seq, :].astype(jnp.float32), pos_ref[0:1, :].astype(jnp.float32))
    embedded = total + pos + type_ref[...].astype(jnp.float32)
    x_ref[...] = norm(embedded, vec_ref[0:1, :], vec_ref[1:2, :]).astype(jnp.bfloat16)

    part = 2 * width // 2
    for at in range(0, 3 * width, part):
        qkv_ref[:, at:at + part] = (times_t(x_ref[...], w_qkv_ref[at:at + part, :])
                                    + b_qkv_ref[:, at:at + part]).astype(jnp.bfloat16)

    masked = jnp.where(keep_row_ref[0] > 0, 0.0, -1e30)
    low = lax.broadcasted_iota(jnp.int32, (1, 2 * size), 1) < size
    for pair in range(heads // 2):
        at = pair * 2 * size
        q = qkv_ref[:, at:at + 2 * size]
        k = qkv_ref[:, width + at:width + at + 2 * size]
        v = qkv_ref[:, 2 * width + at:2 * width + at + 2 * size]
        zero = jnp.zeros_like(q)
        mixed = []
        for mine in (low, ~low):
            s = times_t(jnp.where(mine, q, zero), k) * size ** -0.5 + masked
            p = jnp.exp(s - jnp.max(s, axis=-1, keepdims=True))
            p = p * (1.0 / jnp.sum(p, axis=-1, keepdims=True))
            mixed.append(times(p.astype(jnp.bfloat16), v))
        ctx_ref[:, at:at + 2 * size] = jnp.where(low, mixed[0], mixed[1]).astype(jnp.bfloat16)

    a = (times_t(ctx_ref[...], w_out_ref[...]) + vec_ref[6:7, :]).astype(jnp.bfloat16)
    z = x_ref[...].astype(jnp.float32) + a.astype(jnp.float32)
    x_ref[...] = norm(z, vec_ref[2:3, :], vec_ref[3:4, :]).astype(jnp.bfloat16)

    total = jnp.zeros((seq, width), jnp.float32)
    for at in range(0, b_in_ref.shape[1], FFN_PART):
        h = times_t(x_ref[...], w_in_ref[at:at + FFN_PART, :]) + b_in_ref[:, at:at + FFN_PART]
        h = (0.5 * h * (1.0 + lax.erf(h * SQRT_HALF))).astype(jnp.bfloat16)
        total += times(h, w_back_ref[at:at + FFN_PART, :])
    z = x_ref[...].astype(jnp.float32) + (total + vec_ref[7:8, :])
    out_ref[0] = norm(z, vec_ref[4:5, :], vec_ref[5:6, :]).astype(jnp.bfloat16)


def layer(heads, size, spot, keep, head, got, pos_table, type_row, vecs, b_qkv, b_in, weights, sizes):
    batch, seq = keep.shape
    width = head.shape[1]
    ffn = b_in.shape[0]
    pos = jnp.concatenate([jnp.broadcast_to(pos_table[1:2], (8, width)), pos_table[2:2 + seq]], axis=0)
    keep = keep.astype(jnp.float32)
    n_dev = weights.shape[0]

    def whole(*shape):
        return pl.BlockSpec(shape, lambda b: (0,) * len(shape), pipeline_mode=pl.Buffered(1))

    def each(*shape):
        return pl.BlockSpec((1,) + shape, lambda b: (b,) + (0,) * len(shape))

    pieces, at = [], 0
    for rows in sizes:
        pieces.append(pl.BlockSpec((n_dev, rows, width), functools.partial(lambda i, b: (0, i, 0), at // rows),
                                   pipeline_mode=pl.Buffered(1)))
        at += rows

    return pl.pallas_call(
        functools.partial(layer_kernel, (heads, size)),
        out_shape=jax.ShapeDtypeStruct((batch, seq, width), jnp.bfloat16),
        grid=(batch,),
        in_specs=[each(seq, 1), each(seq, 1), each(1, seq), whole(*head.shape), whole(*got.shape), whole(*pos.shape),
                  whole(1, width), whole(8, width), whole(1, 3 * width), whole(1, ffn)] + pieces,
        out_specs=each(seq, width),
        scratch_shapes=[pltpu.VMEM((seq, 3 * width), jnp.bfloat16), pltpu.VMEM((seq, width), jnp.bfloat16),
                        pltpu.VMEM((seq, width), jnp.bfloat16)],
        compiler_params=pltpu.CompilerParams(vmem_limit_bytes=60 << 20),
        cost_estimate=pl.CostEstimate(flops=40 * 10 ** 9, bytes_accessed=30 * 10 ** 6, transcendentals=10 ** 7))(
            spot.reshape(batch, seq, 1), keep[:, :, None], keep[:, None, :], head, got, pos, type_row[None, :], vecs,
            b_qkv[None, :], b_in[None, :], *([weights] * len(sizes)))


HEAD = 2048
CAPS = ((0, 1, 192), (1, 2, 96), (2, 4, 80), (4, 32, 48))
EXTRA = 48
MESH = pl.DeviceIdType.MESH


def others(n, me, one):
    def body(k, carry):
        one(k, lax.rem(me + k, n))
        return carry

    lax.fori_loop(1, n, body, 0)


def meet(n, me):
    barrier = pltpu.get_barrier_semaphore()
    others(n, me, lambda k, dev: pl.semaphore_signal(barrier, inc=1, device_id=(dev,), device_id_type=MESH))
    pl.semaphore_wait(barrier, n - 1)


def tell_kernel(n, part, msg_ref, table_ref, told_ref, piece_ref, send_sem, recv_sem, out_sem, in_sem, own_sem):
    me = lax.axis_index('fsdp')
    meet(n, me)

    def note(k, dev, slot):
        return pltpu.make_async_remote_copy(msg_ref, told_ref.at[slot], send_sem.at[k], recv_sem.at[slot],
                                            device_id=(dev,), device_id_type=MESH)

    def head(dev):
        return pltpu.make_async_remote_copy(table_ref.at[pl.ds(pl.multiple_of(dev * part, 8), part)], piece_ref,
                                            out_sem.at[dev], in_sem, device_id=(dev,), device_id_type=MESH)

    def own():
        return pltpu.make_async_copy(table_ref.at[pl.ds(0, part)], piece_ref, own_sem)

    others(n, me, lambda k, dev: note(k, dev, me).start())

    @pl.when(me == 0)
    def _():
        others(n, me, lambda k, dev: head(dev).start())
        own().start()

    told_ref[me] = msg_ref[...]
    others(n, me, lambda k, dev: note(k, dev, dev).wait_recv())
    others(n, me, lambda k, dev: note(k, dev, me).wait_send())

    @pl.when(me == 0)
    def _():
        own().wait()
        others(n, me, lambda k, dev: head(dev).wait_send())

    @pl.when(me != 0)
    def _():
        head(me).wait_recv()


def tell(n, msg, table):
    part = HEAD // n
    return pl.pallas_call(
        lambda *refs: tell_kernel(n, part, *refs),
        out_shape=(jax.ShapeDtypeStruct((n,) + msg.shape, msg.dtype),
                   jax.ShapeDtypeStruct((part, table.shape[1]), table.dtype)),
        in_specs=[pl.BlockSpec(memory_space=pltpu.VMEM), pl.BlockSpec(memory_space=pl.ANY)],
        out_specs=(pl.BlockSpec(memory_space=pltpu.VMEM), pl.BlockSpec(memory_space=pltpu.VMEM)),
        scratch_shapes=[pltpu.SemaphoreType.DMA((n,)), pltpu.SemaphoreType.DMA((n,)), pltpu.SemaphoreType.DMA((n,)),
                        pltpu.SemaphoreType.DMA, pltpu.SemaphoreType.DMA],
        compiler_params=pltpu.CompilerParams(collective_id=0, has_side_effects=True))(msg, table)


def bases():
    out, at = [], 0
    for lo, hi, cap in CAPS:
        out.append(at)
        at += (hi - lo) * cap
    return out, at


def swap_kernel(n, send_ref, recv_ref, send_sem, recv_sem, own_sem):
    me = lax.axis_index('fsdp')
    meet(n, me)
    starts, _ = bases()

    def spot(c, dev):
        lo, _, cap = CAPS[c]
        return recv_ref.at[pl.ds(pl.multiple_of(starts[c] + (dev - lo) * cap, 8), cap)]

    def row(c, k, dev, owner):
        return pltpu.make_async_remote_copy(send_ref.at[dev, pl.ds(0, CAPS[c][2])], spot(c, owner), send_sem.at[k],
                                            recv_sem.at[owner], device_id=(dev,), device_id_type=MESH)

    def own(c):
        return pltpu.make_async_copy(send_ref.at[me, pl.ds(0, CAPS[c][2])], spot(c, me), own_sem)

    for c, (lo, hi, cap) in enumerate(CAPS):
        @pl.when((me >= lo) & (me < hi))
        def _(c=c):
            others(n, me, lambda k, dev: row(c, k, dev, me).start())
            own(c).start()

    for c, (lo, hi, cap) in enumerate(CAPS):
        def one(dev, carry, c=c):
            @pl.when(dev != me)
            def _():
                row(c, 0, dev, dev).wait_recv()

            return carry

        lax.fori_loop(lo, hi, one, 0)

    for c, (lo, hi, cap) in enumerate(CAPS):
        @pl.when((me >= lo) & (me < hi))
        def _(c=c):
            others(n, me, lambda k, dev: row(c, k, dev, me).wait_send())
            own(c).wait()


def swap(n, rows):
    return pl.pallas_call(
        lambda *refs: swap_kernel(n, *refs),
        out_shape=jax.ShapeDtypeStruct((bases()[1], rows.shape[2]), rows.dtype),
        in_specs=[pl.BlockSpec(memory_space=pl.ANY)], out_specs=pl.BlockSpec(memory_space=pl.ANY),
        scratch_shapes=[pltpu.SemaphoreType.DMA((n,)), pltpu.SemaphoreType.DMA((n,)), pltpu.SemaphoreType.DMA],
        compiler_params=pltpu.CompilerParams(collective_id=1, has_side_effects=True))(rows)


def solution(mesh):
    def local_step(token_ids, tok_shard, pos_table, type_row, emb_gain, emb_bias, w_qkv, b_qkv, w_out, b_out,
                   ln1_gain, ln1_bias, w_ffn_in, b_ffn_in, w_ffn_out, b_ffn_out, ln2_gain, ln2_bias):
        n_dev = mesh.shape['fsdp']
        me = lax.axis_index('fsdp')
        batch_dev, seq_len = token_ids.shape
        n_tok = batch_dev * seq_len
        shard_rows, width = tok_shard.shape
        num_heads, head_dim = w_out.shape[0], w_out.shape[1]
        pieces = [w_qkv.T, w_out.reshape(num_heads * head_dim, -1).T, w_ffn_in.T, w_ffn_out]
        sizes = [p.shape[0] for p in pieces]
        weights = lax.all_gather(jnp.concatenate(pieces, axis=0), 'fsdp', axis=0, tiled=False)

        ids = token_ids.reshape(n_tok)
        keep = ids != PAD_ID
        asks = keep & (ids >= HEAD)
        owner = jnp.where(asks, ids // shard_rows, n_dev)
        place = jnp.arange(n_tok, dtype=jnp.int32)
        lanes = jnp.arange(128, dtype=jnp.int32)
        mine = (owner[:, None] == lanes[None, :]) & (lanes < n_dev)[None, :]
        before = (place[None, :] < place[:, None]).astype(jnp.bfloat16)
        ranks = jnp.dot(before, mine.astype(jnp.bfloat16), preferred_element_type=jnp.float32)
        count = jnp.sum(mine.astype(jnp.float32), axis=0)
        rank = jnp.sum(jnp.where(mine, ranks, 0.0), axis=1).astype(jnp.int32)
        starts, slots = bases()
        cap, base = jnp.zeros_like(owner), jnp.zeros_like(owner)
        for (lo, hi, c), b in zip(CAPS, starts):
            inside = (owner >= lo) & (owner < hi)
            cap = jnp.where(inside, c, cap)
            base = jnp.where(inside, b + (owner - lo) * c, base)
        fits = rank < cap
        slot = jnp.where(fits, base + rank, -1)
        wide = slots + -slots % 128
        slotted = jnp.sum(jnp.where(slot[:, None] == jnp.arange(wide, dtype=jnp.int32)[None, :],
                                    ids.astype(jnp.float32)[:, None], 0.0), axis=0)

        small = [emb_gain, emb_bias, ln1_gain, ln1_bias, ln2_gain, ln2_bias, b_out, b_ffn_out, b_qkv, b_ffn_in]
        message = jnp.concatenate([slotted, count] + small)
        message = jnp.pad(message, (0, -message.shape[0] % 1024))
        told, piece = tell(n_dev, message.reshape(-1, 128), tok_shard)
        told = told.reshape(n_dev, -1)
        head = lax.all_gather(piece, 'fsdp', axis=0, tiled=True)
        at = wide + 128
        vectors = []
        for v in small:
            vectors.append(told[:, at:at + v.shape[0]].reshape(-1))
            at += v.shape[0]
        emb_g, emb_b, ln1_g, ln1_b, ln2_g, ln2_b, b_out_f, b_back_f, b_qkv_f, b_in_f = vectors

        my_base = jnp.int32(0)
        for (lo, hi, c), b in zip(CAPS, starts):
            my_base = jnp.where((me >= lo) & (me < hi), b + (me - lo) * c, my_base)
        most = max(c for _, _, c in CAPS)
        wanted = lax.dynamic_slice(told, (0, my_base), (n_dev, most)).astype(jnp.int32) - me * shard_rows
        wanted = jnp.clip(wanted, 0, shard_rows - 1)
        rows = jnp.take(tok_shard, wanted.reshape(-1), axis=0, mode='clip').reshape(n_dev, most, width)
        got = swap(n_dev, rows)
        spot = jnp.where(ids < HEAD, ids, HEAD + jnp.maximum(slot, 0))

        caps = jnp.concatenate([jnp.full((hi - lo,), c, jnp.float32) for lo, hi, c in CAPS])
        left = jnp.max(told[:, wide:wide + n_dev] - caps[None, :])
        rounds = (jnp.maximum(left, 0.0).astype(jnp.int32) + EXTRA - 1) // EXTRA

        def again(state):
            r, rows_now = state
            extra = rank - cap - r * EXTRA
            live = asks & (extra >= 0) & (extra < EXTRA)
            at_slot = jnp.where(live, owner * EXTRA + extra, n_dev * EXTRA)
            ask = jnp.zeros((n_dev * EXTRA + 1,), jnp.int32).at[at_slot].set(ids)[:-1]
            asked = lax.all_to_all(ask.reshape(n_dev, EXTRA), 'fsdp', 0, 0, tiled=True)
            asked = jnp.clip(asked - me * shard_rows, 0, shard_rows - 1)
            found = jnp.take(tok_shard, asked.reshape(-1), axis=0, mode='clip').reshape(n_dev, EXTRA, width)
            back = lax.all_to_all(found, 'fsdp', 0, 0, tiled=True).reshape(n_dev * EXTRA, width)
            new = jnp.take(back, jnp.where(live, at_slot, 0), axis=0, mode='clip')
            return r + 1, jnp.where(live[:, None], new, rows_now)

        def slow(got_now, spot_now):
            rows_now = jnp.take(jnp.concatenate([head, got_now], axis=0), spot_now, axis=0, mode='clip')
            _, rows_now = lax.while_loop(lambda state: state[0] < rounds, again, (jnp.int32(0), rows_now))
            return jnp.pad(rows_now, ((0, slots - n_tok), (0, 0))), HEAD + place

        got, spot = lax.cond(rounds > 0, slow, lambda g, p: (g, p), got, spot)
        vecs = jnp.stack([emb_g, emb_b, ln1_g, ln1_b, ln2_g, ln2_b, b_out_f, b_back_f])
        return layer(num_heads, head_dim, spot, token_ids != PAD_ID, head, got, pos_table, type_row, vecs, b_qkv_f, b_in_f,
                     weights, sizes)

    vec_spec = P('fsdp')
    in_specs = (P('fsdp', None), P('fsdp', None), P(None, None), P(None), vec_spec, vec_spec,
                P(None, 'fsdp'), vec_spec, P(None, None, 'fsdp'), vec_spec, vec_spec, vec_spec,
                P(None, 'fsdp'), vec_spec, P('fsdp', None), vec_spec, vec_spec, vec_spec)
    return jax.shard_map(local_step, mesh=mesh, in_specs=in_specs, out_specs=P('fsdp', None, None), check_vma=False)
```

```python
import functools

import jax
import jax.numpy as jnp
from jax import lax
from jax.experimental import pallas as pl
from jax.experimental.pallas import tpu as pltpu
from jax.sharding import PartitionSpec as P


PAD_ID = 1
LN_EPS = 1e-5


SQRT_HALF = 0.5 ** 0.5
FFN_PART = 768


def norm(z, gain, shift):
    centered = z - jnp.mean(z, axis=-1, keepdims=True)
    var = jnp.mean(centered * centered, axis=-1, keepdims=True)
    return centered * lax.rsqrt(var + LN_EPS) * gain + shift


def times(a, b):
    return jnp.dot(a, b, preferred_element_type=jnp.float32)


def times_t(a, b):
    return lax.dot_general(a, b, (((1,), (1,)), ((), ())), preferred_element_type=jnp.float32)


def layer_kernel(dims, spot_ref, spot_row_ref, head_ref, got_ref, pos_ref, type_ref, vec_ref, b_qkv_ref, b_in_ref,
                 w_qkv_ref, w_out_ref, w_in_ref, w_back_ref, out_ref, qkv_ref, ctx_ref, x_ref):
    heads, size = dims
    seq, width = out_ref.shape[1:]
    w_qkv_ref, w_out_ref, w_in_ref, w_back_ref = (
        r.reshape(r.shape[0] * r.shape[1], width) for r in (w_qkv_ref, w_out_ref, w_in_ref, w_back_ref))
    spot = spot_ref[0]
    total = jnp.zeros((seq, width), jnp.float32)
    step = 256
    for ref, first in ((head_ref, 0), (got_ref, head_ref.shape[0])):
        for at in range(0, ref.shape[0], step):
            hit = spot == lax.broadcasted_iota(jnp.int32, (seq, step), 1) + (first + at)
            total += times(jnp.where(hit, 1.0, 0.0).astype(jnp.bfloat16), ref[at:at + step, :])
    pos = jnp.where(spot != PAD_ID, pos_ref[2:2 + seq, :].astype(jnp.float32), pos_ref[1:2, :].astype(jnp.float32))
    embedded = total + pos + type_ref[...].astype(jnp.float32)
    x_ref[...] = norm(embedded, vec_ref[0:1, :], vec_ref[1:2, :]).astype(jnp.bfloat16)

    part = 2 * width // 2
    for at in range(0, 3 * width, part):
        qkv_ref[:, at:at + part] = (times_t(x_ref[...], w_qkv_ref[at:at + part, :])
                                    + b_qkv_ref[:, at:at + part]).astype(jnp.bfloat16)

    masked = jnp.where(spot_row_ref[0] != PAD_ID, 0.0, -1e30)
    low = lax.broadcasted_iota(jnp.int32, (1, 2 * size), 1) < size
    for pair in range(heads // 2):
        at = pair * 2 * size
        q = qkv_ref[:, at:at + 2 * size]
        k = qkv_ref[:, width + at:width + at + 2 * size]
        v = qkv_ref[:, 2 * width + at:2 * width + at + 2 * size]
        zero = jnp.zeros_like(q)
        mixed = []
        for mine in (low, ~low):
            s = times_t(jnp.where(mine, q, zero), k) * size ** -0.5 + masked
            p = jnp.exp(s - jnp.max(s, axis=-1, keepdims=True))
            p = p * (1.0 / jnp.sum(p, axis=-1, keepdims=True))
            mixed.append(times(p.astype(jnp.bfloat16), v))
        ctx_ref[:, at:at + 2 * size] = jnp.where(low, mixed[0], mixed[1]).astype(jnp.bfloat16)

    a = (times_t(ctx_ref[...], w_out_ref[...]) + vec_ref[6:7, :]).astype(jnp.bfloat16)
    z = x_ref[...].astype(jnp.float32) + a.astype(jnp.float32)
    x_ref[...] = norm(z, vec_ref[2:3, :], vec_ref[3:4, :]).astype(jnp.bfloat16)

    total = jnp.zeros((seq, width), jnp.float32)
    for at in range(0, b_in_ref.shape[1], FFN_PART):
        h = times_t(x_ref[...], w_in_ref[at:at + FFN_PART, :]) + b_in_ref[:, at:at + FFN_PART]
        h = (0.5 * h * (1.0 + lax.erf(h * SQRT_HALF))).astype(jnp.bfloat16)
        total += times(h, w_back_ref[at:at + FFN_PART, :])
    z = x_ref[...].astype(jnp.float32) + (total + vec_ref[7:8, :])
    out_ref[0] = norm(z, vec_ref[4:5, :], vec_ref[5:6, :]).astype(jnp.bfloat16)


def layer(heads, size, batch, spot, head, got, pos_table, type_row, vecs, b_qkv, b_in, weights, sizes):
    seq = spot.shape[0] // batch
    width = head.shape[1]
    ffn = b_in.shape[0]
    n_dev = weights.shape[0]

    def whole(*shape):
        return pl.BlockSpec(shape, lambda b: (0,) * len(shape), pipeline_mode=pl.Buffered(1))

    def each(*shape):
        return pl.BlockSpec((1,) + shape, lambda b: (b,) + (0,) * len(shape))

    pieces, at = [], 0
    for rows in sizes:
        pieces.append(pl.BlockSpec((n_dev, rows, width), functools.partial(lambda i, b: (0, i, 0), at // rows),
                                   pipeline_mode=pl.Buffered(1)))
        at += rows

    return pl.pallas_call(
        functools.partial(layer_kernel, (heads, size)),
        out_shape=jax.ShapeDtypeStruct((batch, seq, width), jnp.bfloat16),
        grid=(batch,),
        in_specs=[each(seq, 1), each(1, seq), whole(*head.shape), whole(*got.shape), whole(*pos_table.shape),
                  whole(1, width), whole(8, width), whole(1, 3 * width), whole(1, ffn)] + pieces,
        out_specs=each(seq, width),
        scratch_shapes=[pltpu.VMEM((seq, 3 * width), jnp.bfloat16), pltpu.VMEM((seq, width), jnp.bfloat16),
                        pltpu.VMEM((seq, width), jnp.bfloat16)],
        compiler_params=pltpu.CompilerParams(vmem_limit_bytes=60 << 20),
        cost_estimate=pl.CostEstimate(flops=40 * 10 ** 9, bytes_accessed=30 * 10 ** 6, transcendentals=10 ** 7))(
            spot.reshape(batch, seq, 1), spot.reshape(batch, 1, seq), head, got, pos_table, type_row[None, :], vecs,
            b_qkv[None, :], b_in[None, :], *([weights] * len(sizes)))


HEAD = 2048
CAPS = ((0, 1, 176), (1, 2, 96), (2, 4, 72), (4, 8, 56), (8, 32, 48))
HOT = 2
EXTRA = 48
PLANE = 8
MESH = pl.DeviceIdType.MESH


def others(n, me, one):
    def body(k, carry):
        one(k, lax.rem(me + k, n))
        return carry

    lax.fori_loop(1, n, body, 0)


def meet(n, me):
    barrier = pltpu.get_barrier_semaphore()
    others(n, me, lambda k, dev: pl.semaphore_signal(barrier, inc=1, device_id=(dev,), device_id_type=MESH))
    pl.semaphore_wait(barrier, n - 1)


def tell_kernel(n, part, msg_ref, table_ref, told_ref, piece_ref, relay_ref, send_sem, recv_sem, out_sem, in_sem, relay_sem,
                own_sem):
    me = lax.axis_index('fsdp')
    planes = n // PLANE
    group = part * planes
    meet(n, me)

    def note(k, dev, slot):
        return pltpu.make_async_remote_copy(msg_ref, told_ref.at[slot], send_sem.at[k], recv_sem.at[slot],
                                            device_id=(dev,), device_id_type=MESH)

    def lend(p):
        return pltpu.make_async_remote_copy(table_ref.at[pl.ds(p * group, group)], relay_ref, out_sem.at[p], relay_sem,
                                            device_id=(p,), device_id_type=MESH)

    def part_of(ref, z, dev):
        return pltpu.make_async_remote_copy(ref.at[pl.ds(z * part, part)], piece_ref, out_sem.at[PLANE + z], in_sem,
                                            device_id=(dev,), device_id_type=MESH)

    def own():
        return pltpu.make_async_copy(table_ref.at[pl.ds(0, part)], piece_ref, own_sem)

    others(n, me, lambda k, dev: note(k, dev, me).start())

    @pl.when(me == 0)
    def _():
        for p in range(PLANE - 1, 0, -1):
            lend(p).start()
        for z in range(1, planes):
            part_of(table_ref, z, z * PLANE).start()
        own().start()

    told_ref[me] = msg_ref[...]

    @pl.when((me > 0) & (me < PLANE))
    def _():
        lend(0).wait_recv()
        for z in range(planes - 1, 0, -1):
            part_of(relay_ref, z, z * PLANE + me).start()
        piece_ref[...] = relay_ref[0:part, :]

    others(n, me, lambda k, dev: note(k, dev, dev).wait_recv())
    others(n, me, lambda k, dev: note(k, dev, me).wait_send())

    @pl.when(me == 0)
    def _():
        own().wait()
        for p in range(1, PLANE):
            lend(p).wait_send()
        for z in range(1, planes):
            part_of(table_ref, z, z * PLANE).wait_send()

    @pl.when((me > 0) & (me < PLANE))
    def _():
        for z in range(1, planes):
            part_of(relay_ref, z, z * PLANE + me).wait_send()

    @pl.when(me >= PLANE)
    def _():
        part_of(relay_ref, 0, me).wait_recv()


def tell(n, msg, table):
    part = HEAD // n
    return pl.pallas_call(
        lambda *refs: tell_kernel(n, part, *refs),
        out_shape=(jax.ShapeDtypeStruct((n,) + msg.shape, msg.dtype),
                   jax.ShapeDtypeStruct((part, table.shape[1]), table.dtype)),
        in_specs=[pl.BlockSpec(memory_space=pltpu.VMEM), pl.BlockSpec(memory_space=pl.ANY)],
        out_specs=(pl.BlockSpec(memory_space=pltpu.VMEM), pl.BlockSpec(memory_space=pltpu.VMEM)),
        scratch_shapes=[pltpu.VMEM((part * (n // PLANE), table.shape[1]), table.dtype),
                        pltpu.SemaphoreType.DMA((n,)), pltpu.SemaphoreType.DMA((n,)),
                        pltpu.SemaphoreType.DMA((PLANE + n // PLANE,)), pltpu.SemaphoreType.DMA, pltpu.SemaphoreType.DMA,
                        pltpu.SemaphoreType.DMA],
        compiler_params=pltpu.CompilerParams(collective_id=0, has_side_effects=True))(msg, table)


def head_spot(n, ids):
    part = HEAD // n
    planes = n // PLANE
    at = ids // part
    return ((at % planes) * PLANE + at // planes) * part + ids % part


def bases():
    out, at = [], 0
    for lo, hi, cap in CAPS:
        out.append(at)
        at += (hi - lo) * cap
    return out, at


def relayed(p, z):
    return z > 0 and 2 <= p and p < PLANE - 1 and (p, z) != (PLANE - 2, 3)


def swap_kernel(n, send_ref, recv_ref, relay_ref, send_sem, recv_sem, lend_sem, pass_sem, own_sem):
    me = lax.axis_index('fsdp')
    planes = n // PLANE
    meet(n, me)
    starts, _ = bases()

    def spot(c, dev):
        lo, _, cap = CAPS[c]
        return recv_ref.at[pl.ds(pl.multiple_of(starts[c] + (dev - lo) * cap, 8), cap)]

    def block(c, dev):
        return send_ref.at[lax.rem(dev, PLANE) * planes + lax.div(dev, PLANE), pl.ds(0, CAPS[c][2])]

    def row(c, k, dev, owner):
        return pltpu.make_async_remote_copy(block(c, dev), spot(c, owner), send_sem.at[k], recv_sem.at[owner],
                                            device_id=(dev,), device_id_type=MESH)

    def held(c, z):
        return relay_ref.at[c, z - 1, pl.ds(0, CAPS[c][2])]

    def lend(c, p, z):
        return pltpu.make_async_remote_copy(send_ref.at[p * planes + z, pl.ds(0, CAPS[c][2])], held(c, z),
                                            send_sem.at[z * PLANE + p], lend_sem.at[c, z - 1], device_id=(p,),
                                            device_id_type=MESH)

    def hand_on(c, z):
        return pltpu.make_async_remote_copy(held(c, z), spot(c, c), pass_sem.at[c, z - 1], recv_sem.at[c],
                                            device_id=(z * PLANE + me,), device_id_type=MESH)

    def own(c):
        return pltpu.make_async_copy(block(c, me), spot(c, me), own_sem)

    def hot_sends(c):
        for z in range(planes - 1, -1, -1):
            for p in range(PLANE):
                dev = z * PLANE + p
                if relayed(p, z):
                    yield lend(c, p, z)
                elif dev != c:
                    yield row(c, dev, jnp.int32(dev), c)

    def relays():
        for p in range(PLANE):
            zs = [z for z in range(planes - 1, 0, -1) if relayed(p, z)]
            if zs:
                yield p, zs

    for c, (lo, hi, cap) in enumerate(CAPS):
        @pl.when((me >= lo) & (me < hi))
        def _(c=c):
            own(c).start()
            if c < HOT:
                for copy in hot_sends(c):
                    copy.start()
            else:
                others(n, me, lambda k, dev: row(c, k, dev, me).start())

    for p, zs in relays():
        @pl.when(me == p)
        def _(zs=zs):
            for z in zs:
                for c in range(HOT):
                    lend(c, 0, z).wait_recv()
                    hand_on(c, z).start()

    for c, (lo, hi, cap) in enumerate(CAPS):
        def one(dev, carry, c=c):
            @pl.when(dev != me)
            def _():
                row(c, 0, dev, dev).wait_recv()

            return carry

        lax.fori_loop(lo, hi, one, 0)

    for c, (lo, hi, cap) in enumerate(CAPS):
        @pl.when((me >= lo) & (me < hi))
        def _(c=c):
            own(c).wait()
            if c < HOT:
                for copy in hot_sends(c):
                    copy.wait_send()
            else:
                others(n, me, lambda k, dev: row(c, k, dev, me).wait_send())

    for p, zs in relays():
        @pl.when(me == p)
        def _(zs=zs):
            for z in zs:
                for c in range(HOT):
                    hand_on(c, z).wait_send()


def swap(n, rows):
    planes = n // PLANE
    most = max(cap for _, _, cap in CAPS[:HOT])
    return pl.pallas_call(
        lambda *refs: swap_kernel(n, *refs),
        out_shape=jax.ShapeDtypeStruct((bases()[1], rows.shape[2]), rows.dtype),
        in_specs=[pl.BlockSpec(memory_space=pl.ANY)], out_specs=pl.BlockSpec(memory_space=pl.ANY),
        scratch_shapes=[pltpu.VMEM((HOT, planes - 1, most, rows.shape[2]), rows.dtype), pltpu.SemaphoreType.DMA((n,)),
                        pltpu.SemaphoreType.DMA((n,)), pltpu.SemaphoreType.DMA((HOT, planes - 1)),
                        pltpu.SemaphoreType.DMA((HOT, planes - 1)), pltpu.SemaphoreType.DMA],
        compiler_params=pltpu.CompilerParams(collective_id=1, has_side_effects=True))(rows)


def solution(mesh):
    def local_step(token_ids, tok_shard, pos_table, type_row, emb_gain, emb_bias, w_qkv, b_qkv, w_out, b_out,
                   ln1_gain, ln1_bias, w_ffn_in, b_ffn_in, w_ffn_out, b_ffn_out, ln2_gain, ln2_bias):
        n_dev = mesh.shape['fsdp']
        me = lax.axis_index('fsdp')
        batch_dev, seq_len = token_ids.shape
        n_tok = batch_dev * seq_len
        shard_rows, width = tok_shard.shape
        num_heads, head_dim = w_out.shape[0], w_out.shape[1]
        pieces = [w_qkv.T, w_out.reshape(num_heads * head_dim, -1).T, w_ffn_in.T, w_ffn_out]
        sizes = [p.shape[0] for p in pieces]
        weights = lax.all_gather(jnp.concatenate(pieces, axis=0), 'fsdp', axis=0, tiled=False)

        ids = token_ids.reshape(n_tok)
        keep = ids != PAD_ID
        asks = keep & (ids >= HEAD)
        owner = jnp.where(asks, ids // shard_rows, n_dev)
        place = jnp.arange(n_tok, dtype=jnp.int32)
        lanes = jnp.arange(128, dtype=jnp.int32)
        mine = (owner[:, None] == lanes[None, :]) & (lanes < n_dev)[None, :]
        before = (place[None, :] < place[:, None]).astype(jnp.bfloat16)
        ranks = jnp.dot(before, mine.astype(jnp.bfloat16), preferred_element_type=jnp.float32)
        count = jnp.sum(mine.astype(jnp.float32), axis=0)
        rank = jnp.sum(jnp.where(mine, ranks, 0.0), axis=1).astype(jnp.int32)
        starts, slots = bases()
        cap, base = jnp.zeros_like(owner), jnp.zeros_like(owner)
        for (lo, hi, c), b in zip(CAPS, starts):
            inside = (owner >= lo) & (owner < hi)
            cap = jnp.where(inside, c, cap)
            base = jnp.where(inside, b + (owner - lo) * c, base)
        fits = rank < cap
        slot = jnp.where(fits, base + rank, -1)
        wide = slots + -slots % 128
        slotted = jnp.sum(jnp.where(slot[:, None] == jnp.arange(wide, dtype=jnp.int32)[None, :],
                                    ids.astype(jnp.float32)[:, None], 0.0), axis=0)

        small = [emb_gain, emb_bias, ln1_gain, ln1_bias, ln2_gain, ln2_bias, b_out, b_ffn_out, b_qkv, b_ffn_in]
        message = jnp.concatenate([slotted, count] + small)
        message = jnp.pad(message, (0, -message.shape[0] % 1024))
        told, piece = tell(n_dev, message.reshape(-1, 128), tok_shard)
        told = told.reshape(n_dev, -1)
        head = lax.all_gather(piece, 'fsdp', axis=0, tiled=True)
        at = wide + 128
        vectors = []
        for v in small:
            vectors.append(told[:, at:at + v.shape[0]].reshape(-1))
            at += v.shape[0]
        emb_g, emb_b, ln1_g, ln1_b, ln2_g, ln2_b, b_out_f, b_back_f, b_qkv_f, b_in_f = vectors

        my_base = jnp.int32(0)
        for (lo, hi, c), b in zip(CAPS, starts):
            my_base = jnp.where((me >= lo) & (me < hi), b + (me - lo) * c, my_base)
        most = max(c for _, _, c in CAPS)
        wanted = lax.dynamic_slice(told, (0, my_base), (n_dev, most)).astype(jnp.int32) - me * shard_rows
        wanted = jnp.clip(wanted, 0, shard_rows - 1)
        wanted = wanted.reshape(n_dev // PLANE, PLANE, most).transpose(1, 0, 2)
        rows = jnp.take(tok_shard, wanted.reshape(-1), axis=0, mode='clip').reshape(n_dev, most, width)
        got = swap(n_dev, rows)
        spot = jnp.where(ids < HEAD, head_spot(n_dev, ids), HEAD + jnp.maximum(slot, 0))

        caps = jnp.concatenate([jnp.full((hi - lo,), c, jnp.float32) for lo, hi, c in CAPS])
        left = jnp.max(told[:, wide:wide + n_dev] - caps[None, :])
        rounds = (jnp.maximum(left, 0.0).astype(jnp.int32) + EXTRA - 1) // EXTRA

        def again(state):
            r, rows_now = state
            extra = rank - cap - r * EXTRA
            live = asks & (extra >= 0) & (extra < EXTRA)
            at_slot = jnp.where(live, owner * EXTRA + extra, n_dev * EXTRA)
            ask = jnp.zeros((n_dev * EXTRA + 1,), jnp.int32).at[at_slot].set(ids)[:-1]
            asked = lax.all_to_all(ask.reshape(n_dev, EXTRA), 'fsdp', 0, 0, tiled=True)
            asked = jnp.clip(asked - me * shard_rows, 0, shard_rows - 1)
            found = jnp.take(tok_shard, asked.reshape(-1), axis=0, mode='clip').reshape(n_dev, EXTRA, width)
            back = lax.all_to_all(found, 'fsdp', 0, 0, tiled=True).reshape(n_dev * EXTRA, width)
            new = jnp.take(back, jnp.where(live, at_slot, 0), axis=0, mode='clip')
            return r + 1, jnp.where(live[:, None], new, rows_now)

        def slow(got_now, spot_now):
            rows_now = jnp.take(jnp.concatenate([head, got_now], axis=0), spot_now, axis=0, mode='clip')
            _, rows_now = lax.while_loop(lambda state: state[0] < rounds, again, (jnp.int32(0), rows_now))
            return jnp.pad(rows_now, ((0, slots - n_tok), (0, 0))), jnp.where(ids == PAD_ID, spot_now, HEAD + place)

        got, spot = lax.cond(rounds > 0, slow, lambda g, p: (g, p), got, spot)
        vecs = jnp.stack([emb_g, emb_b, ln1_g, ln1_b, ln2_g, ln2_b, b_out_f, b_back_f])
        return layer(num_heads, head_dim, batch_dev, spot, head, got, pos_table, type_row, vecs, b_qkv_f, b_in_f,
                     weights, sizes)

    vec_spec = P('fsdp')
    in_specs = (P('fsdp', None), P('fsdp', None), P(None, None), P(None), vec_spec, vec_spec,
                P(None, 'fsdp'), vec_spec, P(None, None, 'fsdp'), vec_spec, vec_spec, vec_spec,
                P(None, 'fsdp'), vec_spec, P('fsdp', None), vec_spec, vec_spec, vec_spec)
    return jax.shard_map(local_step, mesh=mesh, in_specs=in_specs, out_specs=P('fsdp', None, None), check_vma=False)
```

```python
import functools

import jax
import jax.numpy as jnp
from jax import lax
from jax.experimental import pallas as pl
from jax.experimental.pallas import tpu as pltpu
from jax.sharding import PartitionSpec as P

PAD_ID = 1
LN_EPS = 1e-5


SQRT_HALF = 0.5 ** 0.5
FFN_PART = 768


def norm(z, gain, shift):
    centered = z - jnp.mean(z, axis=-1, keepdims=True)
    var = jnp.mean(centered * centered, axis=-1, keepdims=True)
    return centered * lax.rsqrt(var + LN_EPS) * gain + shift


def times(a, b):
    return jnp.dot(a, b, preferred_element_type=jnp.float32)


def times_t(a, b):
    return lax.dot_general(a, b, (((1,), (1,)), ((), ())), preferred_element_type=jnp.float32)


def layer_kernel(dims, spot_ref, spot_row_ref, head_ref, got_ref, pos_ref, type_ref, vec_ref, b_qkv_ref, b_in_ref,
                 w_qkv_ref, w_out_ref, w_in_ref, w_back_ref, out_ref, qkv_ref, ctx_ref, x_ref):
    heads, size = dims
    seq, width = out_ref.shape[1:]
    w_qkv_ref, w_out_ref, w_in_ref, w_back_ref = (
        r.reshape(r.shape[0] * r.shape[1], width) for r in (w_qkv_ref, w_out_ref, w_in_ref, w_back_ref))
    spot = spot_ref[0]
    total = jnp.zeros((seq, width), jnp.float32)
    step = 256
    for ref, first in ((head_ref, 0), (got_ref, head_ref.shape[0])):
        for at in range(0, ref.shape[0], step):
            hit = spot == lax.broadcasted_iota(jnp.int32, (seq, step), 1) + (first + at)
            total += times(jnp.where(hit, 1.0, 0.0).astype(jnp.bfloat16), ref[at:at + step, :])
    pos = jnp.where(spot != PAD_ID, pos_ref[2:2 + seq, :].astype(jnp.float32), pos_ref[1:2, :].astype(jnp.float32))
    embedded = total + pos + type_ref[...].astype(jnp.float32)
    x_ref[...] = norm(embedded, vec_ref[0:1, :], vec_ref[1:2, :]).astype(jnp.bfloat16)

    part = 2 * width // 2
    for at in range(0, 3 * width, part):
        qkv_ref[:, at:at + part] = (times_t(x_ref[...], w_qkv_ref[at:at + part, :])
                                    + b_qkv_ref[:, at:at + part]).astype(jnp.bfloat16)

    masked = jnp.where(spot_row_ref[0] != PAD_ID, 0.0, -1e30)
    low = lax.broadcasted_iota(jnp.int32, (1, 2 * size), 1) < size
    for pair in range(heads // 2):
        at = pair * 2 * size
        q = qkv_ref[:, at:at + 2 * size]
        k = qkv_ref[:, width + at:width + at + 2 * size]
        v = qkv_ref[:, 2 * width + at:2 * width + at + 2 * size]
        zero = jnp.zeros_like(q)
        mixed = []
        for mine in (low, ~low):
            s = times_t(jnp.where(mine, q, zero), k) * size ** -0.5 + masked
            p = jnp.exp(s - jnp.max(s, axis=-1, keepdims=True))
            p = p * (1.0 / jnp.sum(p, axis=-1, keepdims=True))
            mixed.append(times(p.astype(jnp.bfloat16), v))
        ctx_ref[:, at:at + 2 * size] = jnp.where(low, mixed[0], mixed[1]).astype(jnp.bfloat16)

    a = (times_t(ctx_ref[...], w_out_ref[...]) + vec_ref[6:7, :]).astype(jnp.bfloat16)
    z = x_ref[...].astype(jnp.float32) + a.astype(jnp.float32)
    x_ref[...] = norm(z, vec_ref[2:3, :], vec_ref[3:4, :]).astype(jnp.bfloat16)

    total = jnp.zeros((seq, width), jnp.float32)
    for at in range(0, b_in_ref.shape[1], FFN_PART):
        h = times_t(x_ref[...], w_in_ref[at:at + FFN_PART, :]) + b_in_ref[:, at:at + FFN_PART]
        h = (0.5 * h * (1.0 + lax.erf(h * SQRT_HALF))).astype(jnp.bfloat16)
        total += times(h, w_back_ref[at:at + FFN_PART, :])
    z = x_ref[...].astype(jnp.float32) + (total + vec_ref[7:8, :])
    out_ref[0] = norm(z, vec_ref[4:5, :], vec_ref[5:6, :]).astype(jnp.bfloat16)


def layer(heads, size, batch, spot, head, got, pos_table, type_row, vecs, b_qkv, b_in, weights, sizes):
    seq = spot.shape[0] // batch
    width = head.shape[1]
    ffn = b_in.shape[0]
    n_dev = weights.shape[0]

    def whole(*shape):
        return pl.BlockSpec(shape, lambda b: (0,) * len(shape), pipeline_mode=pl.Buffered(1))

    def each(*shape):
        return pl.BlockSpec((1,) + shape, lambda b: (b,) + (0,) * len(shape))

    pieces, at = [], 0
    for rows in sizes:
        pieces.append(pl.BlockSpec((n_dev, rows, width), functools.partial(lambda i, b: (0, i, 0), at // rows),
                                   pipeline_mode=pl.Buffered(1)))
        at += rows

    return pl.pallas_call(
        functools.partial(layer_kernel, (heads, size)),
        out_shape=jax.ShapeDtypeStruct((batch, seq, width), jnp.bfloat16),
        grid=(batch,),
        in_specs=[each(seq, 1), each(1, seq), whole(*head.shape), whole(*got.shape), whole(*pos_table.shape),
                  whole(1, width), whole(8, width), whole(1, 3 * width), whole(1, ffn)] + pieces,
        out_specs=each(seq, width),
        scratch_shapes=[pltpu.VMEM((seq, 3 * width), jnp.bfloat16), pltpu.VMEM((seq, width), jnp.bfloat16),
                        pltpu.VMEM((seq, width), jnp.bfloat16)],
        compiler_params=pltpu.CompilerParams(vmem_limit_bytes=60 << 20),
        cost_estimate=pl.CostEstimate(flops=40 * 10 ** 9, bytes_accessed=30 * 10 ** 6, transcendentals=10 ** 7))(
            spot.reshape(batch, seq, 1), spot.reshape(batch, 1, seq), head, got, pos_table, type_row[None, :], vecs,
            b_qkv[None, :], b_in[None, :], *([weights] * len(sizes)))


HEAD = 2048
CAPS = ((0, 1, 160), (1, 2, 80), (2, 4, 72), (4, 8, 48), (8, 32, 40))
HOT = 2
EXTRA = 48
PLANE = 8
MESH = pl.DeviceIdType.MESH


def others(n, me, one):
    def body(k, carry):
        one(k, lax.rem(me + k, n))
        return carry

    lax.fori_loop(1, n, body, 0)


def meet(n, me):
    barrier = pltpu.get_barrier_semaphore()
    others(n, me, lambda k, dev: pl.semaphore_signal(barrier, inc=1, device_id=(dev,), device_id_type=MESH))
    pl.semaphore_wait(barrier, n - 1)


def tell_kernel(n, msg_ref, table_ref, told_ref, group_ref, send_sem, recv_sem, out_sem, in_sem, own_sem):
    me = lax.axis_index('fsdp')
    group = HEAD // PLANE
    meet(n, me)

    def note(k, dev, slot):
        return pltpu.make_async_remote_copy(msg_ref, told_ref.at[slot], send_sem.at[k], recv_sem.at[slot],
                                            device_id=(dev,), device_id_type=MESH)

    def lend(p):
        return pltpu.make_async_remote_copy(table_ref.at[pl.ds(p * group, group)], group_ref, out_sem.at[p], in_sem,
                                            device_id=(p,), device_id_type=MESH)

    def own():
        return pltpu.make_async_copy(table_ref.at[pl.ds(0, group)], group_ref, own_sem)

    others(n, me, lambda k, dev: note(k, dev, me).start())

    @pl.when(me == 0)
    def _():
        for p in range(PLANE - 1, 0, -1):
            lend(p).start()
        own().start()

    told_ref[me] = msg_ref[...]
    others(n, me, lambda k, dev: note(k, dev, dev).wait_recv())
    others(n, me, lambda k, dev: note(k, dev, me).wait_send())

    @pl.when(me == 0)
    def _():
        own().wait()
        for p in range(1, PLANE):
            lend(p).wait_send()

    @pl.when((me > 0) & (me < PLANE))
    def _():
        lend(0).wait_recv()


def tell(n, msg, table):
    vmem = pl.BlockSpec(memory_space=pltpu.VMEM)
    return pl.pallas_call(
        lambda *refs: tell_kernel(n, *refs),
        out_shape=(jax.ShapeDtypeStruct((n,) + msg.shape, msg.dtype),
                   jax.ShapeDtypeStruct((HEAD // PLANE, table.shape[1]), table.dtype)),
        in_specs=[vmem, pl.BlockSpec(memory_space=pl.ANY)], out_specs=(vmem, vmem),
        scratch_shapes=[pltpu.SemaphoreType.DMA((n,)), pltpu.SemaphoreType.DMA((n,)), pltpu.SemaphoreType.DMA((PLANE,)),
                        pltpu.SemaphoreType.DMA, pltpu.SemaphoreType.DMA],
        compiler_params=pltpu.CompilerParams(collective_id=0, has_side_effects=True))(msg, table)


def bases():
    out, at = [], 0
    for lo, hi, cap in CAPS:
        out.append(at)
        at += (hi - lo) * cap
    return out, at


def relayed(p, z):
    return z > 0 and 2 <= p and p < PLANE - 1 and (p, z) != (PLANE - 2, 3)


def swap_kernel(n, send_ref, group_ref, recv_ref, head_ref, relay_ref, send_sem, recv_sem, lend_sem, pass_sem, own_sem,
                up_send, up_recv, flat_send, head_recv, core_send):
    me = lax.axis_index('fsdp')
    planes = n // PLANE
    group = HEAD // PLANE
    place = lax.rem(me, PLANE)
    level = lax.div(me, PLANE)
    base = level * PLANE
    partner = base + place + 1 - 2 * lax.rem(place, 2)

    def slot(p):
        return head_ref.at[pl.ds(pl.multiple_of(p * group, 8), group)]

    def pass_up(dev):
        return pltpu.make_async_remote_copy(slot(place), slot(place), up_send, up_recv, device_id=(dev,), device_id_type=MESH)

    def across(k):
        p = lax.rem(place + 2 * k, PLANE)
        return pltpu.make_async_remote_copy(slot(place), slot(place), flat_send.at[k], head_recv.at[place],
                                            device_id=(base + p,), device_id_type=MESH)

    def arrival(p):
        return pltpu.make_async_remote_copy(slot(p), slot(p), core_send.at[0], head_recv.at[p], device_id=(me,),
                                            device_id_type=MESH)

    def share(k):
        p = lax.rem(place + 2 * k, PLANE)
        return pltpu.make_async_remote_copy(slot(p), slot(p), core_send.at[k], head_recv.at[p], device_id=(partner,),
                                            device_id_type=MESH)

    meet(n, me)
    starts, _ = bases()

    def spot(c, dev):
        lo, _, cap = CAPS[c]
        return recv_ref.at[pl.ds(pl.multiple_of(starts[c] + (dev - lo) * cap, 8), cap)]

    def block(c, dev):
        return send_ref.at[lax.rem(dev, PLANE) * planes + lax.div(dev, PLANE), pl.ds(0, CAPS[c][2])]

    def row(c, k, dev, owner):
        return pltpu.make_async_remote_copy(block(c, dev), spot(c, owner), send_sem.at[k], recv_sem.at[owner],
                                            device_id=(dev,), device_id_type=MESH)

    def held(c, z):
        return relay_ref.at[c, z - 1, pl.ds(0, CAPS[c][2])]

    def lend(c, p, z):
        return pltpu.make_async_remote_copy(send_ref.at[p * planes + z, pl.ds(0, CAPS[c][2])], held(c, z),
                                            send_sem.at[z * PLANE + p], lend_sem.at[c, z - 1], device_id=(p,),
                                            device_id_type=MESH)

    def hand_on(c, z):
        return pltpu.make_async_remote_copy(held(c, z), spot(c, c), pass_sem.at[c, z - 1], recv_sem.at[c],
                                            device_id=(z * PLANE + me,), device_id_type=MESH)

    def own(c):
        return pltpu.make_async_copy(block(c, me), spot(c, me), own_sem)

    def hot_sends(c):
        for z in range(planes - 1, -1, -1):
            for p in range(PLANE):
                dev = z * PLANE + p
                if relayed(p, z):
                    yield lend(c, p, z)
                elif dev != c:
                    yield row(c, dev, jnp.int32(dev), c)

    def relays():
        for p in range(PLANE):
            zs = [z for z in range(planes - 1, 0, -1) if relayed(p, z)]
            if zs:
                yield p, zs

    for c, (lo, hi, cap) in enumerate(CAPS):
        @pl.when((me >= lo) & (me < hi))
        def _(c=c):
            own(c).start()
            if c < HOT:
                for copy in hot_sends(c):
                    copy.start()
            else:
                others(n, me, lambda k, dev: row(c, k, dev, me).start())

    @pl.when(level == 0)
    def _():
        keep = pltpu.make_async_copy(group_ref, slot(place), up_recv)
        keep.start()
        keep.wait()

    @pl.when(level > 0)
    def _():
        pass_up(me).wait_recv()

    @pl.when(level < planes - 1)
    def _():
        pass_up(me + PLANE).start()

    for k in range(1, PLANE // 2):
        across(k).start()
    share(0).start()

    for p, zs in relays():
        @pl.when(me == p)
        def _(zs=zs):
            for z in zs:
                for c in range(HOT):
                    lend(c, 0, z).wait_recv()
                    hand_on(c, z).start()

    for k in range(PLANE // 2 - 1, 0, -1):
        arrival(lax.rem(place + 2 * k, PLANE)).wait_recv()
        share(k).start()

    for c, (lo, hi, cap) in enumerate(CAPS):
        def one(dev, carry, c=c):
            @pl.when(dev != me)
            def _():
                row(c, 0, dev, dev).wait_recv()

            return carry

        lax.fori_loop(lo, hi, one, 0)

    for c, (lo, hi, cap) in enumerate(CAPS):
        @pl.when((me >= lo) & (me < hi))
        def _(c=c):
            own(c).wait()
            if c < HOT:
                for copy in hot_sends(c):
                    copy.wait_send()
            else:
                others(n, me, lambda k, dev: row(c, k, dev, me).wait_send())

    for p, zs in relays():
        @pl.when(me == p)
        def _(zs=zs):
            for z in zs:
                for c in range(HOT):
                    hand_on(c, z).wait_send()

    for k in range(PLANE // 2):
        arrival(lax.rem(partner + 2 * k, PLANE)).wait_recv()
    for k in range(1, PLANE // 2):
        across(k).wait_send()
    for k in range(PLANE // 2):
        share(k).wait_send()

    @pl.when(level < planes - 1)
    def _():
        pass_up(me + PLANE).wait_send()


def swap(n, rows, group):
    planes = n // PLANE
    most = max(cap for _, _, cap in CAPS[:HOT])
    vmem = pl.BlockSpec(memory_space=pltpu.VMEM)
    dma = pltpu.SemaphoreType.DMA
    return pl.pallas_call(
        lambda *refs: swap_kernel(n, *refs),
        out_shape=(jax.ShapeDtypeStruct((bases()[1], rows.shape[2]), rows.dtype),
                   jax.ShapeDtypeStruct((HEAD, rows.shape[2]), rows.dtype)),
        in_specs=[pl.BlockSpec(memory_space=pl.ANY), vmem], out_specs=(pl.BlockSpec(memory_space=pl.ANY), vmem),
        scratch_shapes=[pltpu.VMEM((HOT, planes - 1, most, rows.shape[2]), rows.dtype), dma((n,)), dma((n,)),
                        dma((HOT, planes - 1)), dma((HOT, planes - 1)), dma, dma, dma, dma((PLANE // 2,)), dma((PLANE,)),
                        dma((PLANE // 2,))],
        compiler_params=pltpu.CompilerParams(collective_id=1, has_side_effects=True))(rows, group)


def solution(mesh):
    def local_step(token_ids, tok_shard, pos_table, type_row, emb_gain, emb_bias, w_qkv, b_qkv, w_out, b_out,
                   ln1_gain, ln1_bias, w_ffn_in, b_ffn_in, w_ffn_out, b_ffn_out, ln2_gain, ln2_bias):
        n_dev = mesh.shape['fsdp']
        me = lax.axis_index('fsdp')
        batch_dev, seq_len = token_ids.shape
        n_tok = batch_dev * seq_len
        shard_rows, width = tok_shard.shape
        num_heads, head_dim = w_out.shape[0], w_out.shape[1]
        pieces = [w_qkv.T, w_out.reshape(num_heads * head_dim, -1).T, w_ffn_in.T, w_ffn_out]
        sizes = [p.shape[0] for p in pieces]
        weights = lax.all_gather(jnp.concatenate(pieces, axis=0), 'fsdp', axis=0, tiled=False)

        ids = token_ids.reshape(n_tok)
        keep = ids != PAD_ID
        asks = keep & (ids >= HEAD)
        owner = jnp.where(asks, ids // shard_rows, n_dev)
        place = jnp.arange(n_tok, dtype=jnp.int32)
        lanes = jnp.arange(128, dtype=jnp.int32)
        mine = (owner[:, None] == lanes[None, :]) & (lanes < n_dev)[None, :]
        before = (place[None, :] < place[:, None]).astype(jnp.bfloat16)
        ranks = jnp.dot(before, mine.astype(jnp.bfloat16), preferred_element_type=jnp.float32)
        count = jnp.sum(mine.astype(jnp.float32), axis=0)
        rank = jnp.sum(jnp.where(mine, ranks, 0.0), axis=1).astype(jnp.int32)
        starts, slots = bases()
        cap, base = jnp.zeros_like(owner), jnp.zeros_like(owner)
        for (lo, hi, c), b in zip(CAPS, starts):
            inside = (owner >= lo) & (owner < hi)
            cap = jnp.where(inside, c, cap)
            base = jnp.where(inside, b + (owner - lo) * c, base)
        fits = rank < cap
        slot = jnp.where(fits, base + rank, -1)
        wide = slots + -slots % 128
        slotted = jnp.sum(jnp.where(slot[:, None] == jnp.arange(wide, dtype=jnp.int32)[None, :],
                                    ids.astype(jnp.float32)[:, None], 0.0), axis=0)

        small = [emb_gain, emb_bias, ln1_gain, ln1_bias, ln2_gain, ln2_bias, b_out, b_ffn_out, b_qkv, b_ffn_in]
        message = jnp.concatenate([slotted, count] + small)
        message = jnp.pad(message, (0, -message.shape[0] % 1024))
        told, group = tell(n_dev, message.reshape(-1, 128), tok_shard)
        told = told.reshape(n_dev, -1)
        at = wide + 128
        vectors = []
        for v in small:
            vectors.append(told[:, at:at + v.shape[0]].reshape(-1))
            at += v.shape[0]
        emb_g, emb_b, ln1_g, ln1_b, ln2_g, ln2_b, b_out_f, b_back_f, b_qkv_f, b_in_f = vectors

        my_base = jnp.int32(0)
        for (lo, hi, c), b in zip(CAPS, starts):
            my_base = jnp.where((me >= lo) & (me < hi), b + (me - lo) * c, my_base)
        most = max(c for _, _, c in CAPS)
        wanted = lax.dynamic_slice(told, (0, my_base), (n_dev, most)).astype(jnp.int32) - me * shard_rows
        wanted = jnp.clip(wanted, 0, shard_rows - 1)
        wanted = wanted.reshape(n_dev // PLANE, PLANE, most).transpose(1, 0, 2)
        rows = jnp.take(tok_shard, wanted.reshape(-1), axis=0, mode='clip').reshape(n_dev, most, width)
        got, head = swap(n_dev, rows, group)
        spot = jnp.where(ids < HEAD, ids, HEAD + jnp.maximum(slot, 0))

        caps = jnp.concatenate([jnp.full((hi - lo,), c, jnp.float32) for lo, hi, c in CAPS])
        left = jnp.max(told[:, wide:wide + n_dev] - caps[None, :])
        rounds = (jnp.maximum(left, 0.0).astype(jnp.int32) + EXTRA - 1) // EXTRA

        def again(state):
            r, rows_now = state
            extra = rank - cap - r * EXTRA
            live = asks & (extra >= 0) & (extra < EXTRA)
            at_slot = jnp.where(live, owner * EXTRA + extra, n_dev * EXTRA)
            ask = jnp.zeros((n_dev * EXTRA + 1,), jnp.int32).at[at_slot].set(ids)[:-1]
            asked = lax.all_to_all(ask.reshape(n_dev, EXTRA), 'fsdp', 0, 0, tiled=True)
            asked = jnp.clip(asked - me * shard_rows, 0, shard_rows - 1)
            found = jnp.take(tok_shard, asked.reshape(-1), axis=0, mode='clip').reshape(n_dev, EXTRA, width)
            back = lax.all_to_all(found, 'fsdp', 0, 0, tiled=True).reshape(n_dev * EXTRA, width)
            new = jnp.take(back, jnp.where(live, at_slot, 0), axis=0, mode='clip')
            return r + 1, jnp.where(live[:, None], new, rows_now)

        def slow(got_now, spot_now):
            rows_now = jnp.take(jnp.concatenate([head, got_now], axis=0), spot_now, axis=0, mode='clip')
            _, rows_now = lax.while_loop(lambda state: state[0] < rounds, again, (jnp.int32(0), rows_now))
            return jnp.pad(rows_now, ((0, slots - n_tok), (0, 0))), jnp.where(ids == PAD_ID, spot_now, HEAD + place)

        got, spot = lax.cond(rounds > 0, slow, lambda g, p: (g, p), got, spot)
        vecs = jnp.stack([emb_g, emb_b, ln1_g, ln1_b, ln2_g, ln2_b, b_out_f, b_back_f])
        return layer(num_heads, head_dim, batch_dev, spot, head, got, pos_table, type_row, vecs, b_qkv_f, b_in_f,
                     weights, sizes)

    vec_spec = P('fsdp')
    in_specs = (P('fsdp', None), P('fsdp', None), P(None, None), P(None), vec_spec, vec_spec,
                P(None, 'fsdp'), vec_spec, P(None, None, 'fsdp'), vec_spec, vec_spec, vec_spec,
                P(None, 'fsdp'), vec_spec, P('fsdp', None), vec_spec, vec_spec, vec_spec)
    return jax.shard_map(local_step, mesh=mesh, in_specs=in_specs, out_specs=P('fsdp', None, None), check_vma=False)
```

```python
import functools

import jax
import jax.numpy as jnp
from jax import lax
from jax.experimental import pallas as pl
from jax.experimental.pallas import tpu as pltpu
from jax.sharding import PartitionSpec as P


PAD_ID = 1
LN_EPS = 1e-5


SQRT_HALF = 0.5 ** 0.5
FFN_PART = 768


def norm(z, gain, shift):
    centered = z - jnp.mean(z, axis=-1, keepdims=True)
    var = jnp.mean(centered * centered, axis=-1, keepdims=True)
    return centered * lax.rsqrt(var + LN_EPS) * gain + shift


def times(a, b):
    return jnp.dot(a, b, preferred_element_type=jnp.float32)


def times_t(a, b):
    return lax.dot_general(a, b, (((1,), (1,)), ((), ())), preferred_element_type=jnp.float32)


def flat(ref):
    return ref.reshape(ref.shape[0] * ref.shape[1], ref.shape[2])


def attention_kernel(dims, spot_ref, spot_row_ref, head_ref, got_ref, pos_ref, type_ref, vec_ref, b_qkv_ref, w_qkv_ref, w_out_ref,
                     out_ref, qkv_ref, ctx_ref, x_ref):
    heads, size = dims
    seq, width = out_ref.shape[1:]
    w_qkv_ref, w_out_ref = flat(w_qkv_ref), flat(w_out_ref)
    spot = spot_ref[0]
    total = jnp.zeros((seq, width), jnp.float32)
    step = 256
    for ref, first in ((head_ref, 0), (got_ref, head_ref.shape[0])):
        for at in range(0, ref.shape[0], step):
            hit = spot == lax.broadcasted_iota(jnp.int32, (seq, step), 1) + (first + at)
            total += times(jnp.where(hit, 1.0, 0.0).astype(jnp.bfloat16), ref[at:at + step, :])
    pos = jnp.where(spot != PAD_ID, pos_ref[2:2 + seq, :].astype(jnp.float32), pos_ref[1:2, :].astype(jnp.float32))
    embedded = total + pos + type_ref[...].astype(jnp.float32)
    x_ref[...] = norm(embedded, vec_ref[0:1, :], vec_ref[1:2, :]).astype(jnp.bfloat16)

    part = 2 * width // 2
    for at in range(0, 3 * width, part):
        qkv_ref[:, at:at + part] = (times_t(x_ref[...], w_qkv_ref[at:at + part, :])
                                    + b_qkv_ref[:, at:at + part]).astype(jnp.bfloat16)

    masked = jnp.where(spot_row_ref[0] != PAD_ID, 0.0, -1e30)
    low = lax.broadcasted_iota(jnp.int32, (1, 2 * size), 1) < size
    for pair in range(heads // 2):
        at = pair * 2 * size
        q = qkv_ref[:, at:at + 2 * size]
        k = qkv_ref[:, width + at:width + at + 2 * size]
        v = qkv_ref[:, 2 * width + at:2 * width + at + 2 * size]
        zero = jnp.zeros_like(q)
        mixed = []
        for mine in (low, ~low):
            s = times_t(jnp.where(mine, q, zero), k) * size ** -0.5 + masked
            p = jnp.exp(s - jnp.max(s, axis=-1, keepdims=True))
            p = p * (1.0 / jnp.sum(p, axis=-1, keepdims=True))
            mixed.append(times(p.astype(jnp.bfloat16), v))
        ctx_ref[:, at:at + 2 * size] = jnp.where(low, mixed[0], mixed[1]).astype(jnp.bfloat16)

    a = (times_t(ctx_ref[...], w_out_ref[...]) + vec_ref[6:7, :]).astype(jnp.bfloat16)
    z = x_ref[...].astype(jnp.float32) + a.astype(jnp.float32)
    out_ref[0] = norm(z, vec_ref[2:3, :], vec_ref[3:4, :]).astype(jnp.bfloat16)


def ffn_kernel(x_ref, vec_ref, b_in_ref, w_in_ref, w_back_ref, out_ref):
    w_in_ref, w_back_ref = flat(w_in_ref), flat(w_back_ref)
    x = x_ref[0]
    total = jnp.zeros(x.shape, jnp.float32)
    for at in range(0, b_in_ref.shape[1], FFN_PART):
        h = times_t(x, w_in_ref[at:at + FFN_PART, :]) + b_in_ref[:, at:at + FFN_PART]
        h = (0.5 * h * (1.0 + lax.erf(h * SQRT_HALF))).astype(jnp.bfloat16)
        total += times(h, w_back_ref[at:at + FFN_PART, :])
    z = x.astype(jnp.float32) + (total + vec_ref[7:8, :])
    out_ref[0] = norm(z, vec_ref[4:5, :], vec_ref[5:6, :]).astype(jnp.bfloat16)


def whole(*shape):
    return pl.BlockSpec(shape, lambda b: (0,) * len(shape), pipeline_mode=pl.Buffered(1))


def each(*shape):
    return pl.BlockSpec((1,) + shape, lambda b: (b,) + (0,) * len(shape))


def pieces(weights, sizes):
    out, at = [], 0
    for rows in sizes:
        out.append(pl.BlockSpec((weights.shape[0], rows, weights.shape[2]),
                                functools.partial(lambda i, b: (0, i, 0), at // rows), pipeline_mode=pl.Buffered(1)))
        at += rows
    return out


def attend(heads, size, batch, spot, head, got, pos_table, type_row, vecs, b_qkv, weights, sizes):
    seq = spot.shape[0] // batch
    width = head.shape[1]
    block = pltpu.VMEM((seq, width), jnp.bfloat16)
    return pl.pallas_call(
        functools.partial(attention_kernel, (heads, size)),
        out_shape=jax.ShapeDtypeStruct((batch, seq, width), jnp.bfloat16),
        grid=(batch,),
        in_specs=[each(seq, 1), each(1, seq), whole(*head.shape), whole(*got.shape), whole(*pos_table.shape), whole(1, width),
                  whole(8, width), whole(1, 3 * width)] + pieces(weights, sizes),
        out_specs=each(seq, width),
        scratch_shapes=[pltpu.VMEM((seq, 3 * width), jnp.bfloat16), block, block],
        compiler_params=pltpu.CompilerParams(vmem_limit_bytes=60 << 20),
        cost_estimate=pl.CostEstimate(flops=20 * 10 ** 9, bytes_accessed=15 * 10 ** 6, transcendentals=7 * 10 ** 6))(
            spot.reshape(batch, seq, 1), spot.reshape(batch, 1, seq), head, got, pos_table, type_row[None, :], vecs,
            b_qkv[None, :], *([weights] * len(sizes)))


def feed(x, vecs, b_in, weights, sizes):
    batch, seq, width = x.shape
    return pl.pallas_call(
        ffn_kernel, out_shape=jax.ShapeDtypeStruct(x.shape, jnp.bfloat16), grid=(batch,),
        in_specs=[each(seq, width), whole(8, width), whole(1, b_in.shape[0])] + pieces(weights, sizes),
        out_specs=each(seq, width),
        compiler_params=pltpu.CompilerParams(vmem_limit_bytes=60 << 20),
        cost_estimate=pl.CostEstimate(flops=15 * 10 ** 9, bytes_accessed=15 * 10 ** 6, transcendentals=5 * 10 ** 6))(
            x, vecs, b_in[None, :], *([weights] * len(sizes)))


HEAD = 2048
CAPS = ((0, 1, 160), (1, 2, 80), (2, 4, 72), (4, 8, 48), (8, 32, 40))
HOT = 2
EXTRA = 48
PLANE = 8
MESH = pl.DeviceIdType.MESH


def others(n, me, one):
    def body(k, carry):
        one(k, lax.rem(me + k, n))
        return carry

    lax.fori_loop(1, n, body, 0)


def meet(n, me):
    barrier = pltpu.get_barrier_semaphore()
    others(n, me, lambda k, dev: pl.semaphore_signal(barrier, inc=1, device_id=(dev,), device_id_type=MESH))
    pl.semaphore_wait(barrier, n - 1)


def tell_kernel(n, part, msg_ref, table_ref, told_ref, piece_ref, relay_ref, send_sem, recv_sem, out_sem, in_sem, relay_sem,
                own_sem):
    me = lax.axis_index('fsdp')
    planes = n // PLANE
    group = part * planes
    meet(n, me)

    def note(k, dev, slot):
        return pltpu.make_async_remote_copy(msg_ref, told_ref.at[slot], send_sem.at[k], recv_sem.at[slot],
                                            device_id=(dev,), device_id_type=MESH)

    def lend(p):
        return pltpu.make_async_remote_copy(table_ref.at[pl.ds(p * group, group)], relay_ref, out_sem.at[p], relay_sem,
                                            device_id=(p,), device_id_type=MESH)

    def part_of(ref, z, dev):
        return pltpu.make_async_remote_copy(ref.at[pl.ds(z * part, part)], piece_ref, out_sem.at[PLANE + z], in_sem,
                                            device_id=(dev,), device_id_type=MESH)

    def own():
        return pltpu.make_async_copy(table_ref.at[pl.ds(0, part)], piece_ref, own_sem)

    others(n, me, lambda k, dev: note(k, dev, me).start())

    @pl.when(me == 0)
    def _():
        for p in range(PLANE - 1, 0, -1):
            lend(p).start()
        for z in range(1, planes):
            part_of(table_ref, z, z * PLANE).start()
        own().start()

    told_ref[me] = msg_ref[...]

    @pl.when((me > 0) & (me < PLANE))
    def _():
        lend(0).wait_recv()
        for z in range(planes - 1, 0, -1):
            part_of(relay_ref, z, z * PLANE + me).start()
        piece_ref[...] = relay_ref[0:part, :]

    others(n, me, lambda k, dev: note(k, dev, dev).wait_recv())
    others(n, me, lambda k, dev: note(k, dev, me).wait_send())

    @pl.when(me == 0)
    def _():
        own().wait()
        for p in range(1, PLANE):
            lend(p).wait_send()
        for z in range(1, planes):
            part_of(table_ref, z, z * PLANE).wait_send()

    @pl.when((me > 0) & (me < PLANE))
    def _():
        for z in range(1, planes):
            part_of(relay_ref, z, z * PLANE + me).wait_send()

    @pl.when(me >= PLANE)
    def _():
        part_of(relay_ref, 0, me).wait_recv()


def tell(n, msg, table):
    part = HEAD // n
    return pl.pallas_call(
        lambda *refs: tell_kernel(n, part, *refs),
        out_shape=(jax.ShapeDtypeStruct((n,) + msg.shape, msg.dtype),
                   jax.ShapeDtypeStruct((part, table.shape[1]), table.dtype)),
        in_specs=[pl.BlockSpec(memory_space=pltpu.VMEM), pl.BlockSpec(memory_space=pl.ANY)],
        out_specs=(pl.BlockSpec(memory_space=pltpu.VMEM), pl.BlockSpec(memory_space=pltpu.VMEM)),
        scratch_shapes=[pltpu.VMEM((part * (n // PLANE), table.shape[1]), table.dtype),
                        pltpu.SemaphoreType.DMA((n,)), pltpu.SemaphoreType.DMA((n,)),
                        pltpu.SemaphoreType.DMA((PLANE + n // PLANE,)), pltpu.SemaphoreType.DMA, pltpu.SemaphoreType.DMA,
                        pltpu.SemaphoreType.DMA],
        compiler_params=pltpu.CompilerParams(collective_id=0, has_side_effects=True))(msg, table)


def head_spot(n, ids):
    part = HEAD // n
    planes = n // PLANE
    at = ids // part
    return ((at % planes) * PLANE + at // planes) * part + ids % part


def bases():
    out, at = [], 0
    for lo, hi, cap in CAPS:
        out.append(at)
        at += (hi - lo) * cap
    return out, at


def relayed(p, z):
    return z > 0 and 2 <= p and p < PLANE - 1 and (p, z) != (PLANE - 2, 3)


def swap_kernel(n, send_ref, recv_ref, relay_ref, send_sem, recv_sem, lend_sem, pass_sem, own_sem):
    me = lax.axis_index('fsdp')
    planes = n // PLANE
    meet(n, me)
    starts, _ = bases()

    def spot(c, dev):
        lo, _, cap = CAPS[c]
        return recv_ref.at[pl.ds(pl.multiple_of(starts[c] + (dev - lo) * cap, 8), cap)]

    def block(c, dev):
        return send_ref.at[lax.rem(dev, PLANE) * planes + lax.div(dev, PLANE), pl.ds(0, CAPS[c][2])]

    def row(c, k, dev, owner):
        return pltpu.make_async_remote_copy(block(c, dev), spot(c, owner), send_sem.at[k], recv_sem.at[owner],
                                            device_id=(dev,), device_id_type=MESH)

    def held(c, z):
        return relay_ref.at[c, z - 1, pl.ds(0, CAPS[c][2])]

    def lend(c, p, z):
        return pltpu.make_async_remote_copy(send_ref.at[p * planes + z, pl.ds(0, CAPS[c][2])], held(c, z),
                                            send_sem.at[z * PLANE + p], lend_sem.at[c, z - 1], device_id=(p,),
                                            device_id_type=MESH)

    def hand_on(c, z):
        return pltpu.make_async_remote_copy(held(c, z), spot(c, c), pass_sem.at[c, z - 1], recv_sem.at[c],
                                            device_id=(z * PLANE + me,), device_id_type=MESH)

    def own(c):
        return pltpu.make_async_copy(block(c, me), spot(c, me), own_sem)

    def hot_sends(c):
        for z in range(planes - 1, -1, -1):
            for p in range(PLANE):
                dev = z * PLANE + p
                if relayed(p, z):
                    yield lend(c, p, z)
                elif dev != c:
                    yield row(c, dev, jnp.int32(dev), c)

    def relays():
        for p in range(PLANE):
            zs = [z for z in range(planes - 1, 0, -1) if relayed(p, z)]
            if zs:
                yield p, zs

    for c, (lo, hi, cap) in enumerate(CAPS):
        @pl.when((me >= lo) & (me < hi))
        def _(c=c):
            own(c).start()
            if c < HOT:
                for copy in hot_sends(c):
                    copy.start()
            else:
                others(n, me, lambda k, dev: row(c, k, dev, me).start())

    for p, zs in relays():
        @pl.when(me == p)
        def _(zs=zs):
            for z in zs:
                for c in range(HOT):
                    lend(c, 0, z).wait_recv()
                    hand_on(c, z).start()

    for c, (lo, hi, cap) in enumerate(CAPS):
        def one(dev, carry, c=c):
            @pl.when(dev != me)
            def _():
                row(c, 0, dev, dev).wait_recv()

            return carry

        lax.fori_loop(lo, hi, one, 0)

    for c, (lo, hi, cap) in enumerate(CAPS):
        @pl.when((me >= lo) & (me < hi))
        def _(c=c):
            own(c).wait()
            if c < HOT:
                for copy in hot_sends(c):
                    copy.wait_send()
            else:
                others(n, me, lambda k, dev: row(c, k, dev, me).wait_send())

    for p, zs in relays():
        @pl.when(me == p)
        def _(zs=zs):
            for z in zs:
                for c in range(HOT):
                    hand_on(c, z).wait_send()


def swap(n, rows):
    planes = n // PLANE
    most = max(cap for _, _, cap in CAPS[:HOT])
    return pl.pallas_call(
        lambda *refs: swap_kernel(n, *refs),
        out_shape=jax.ShapeDtypeStruct((bases()[1], rows.shape[2]), rows.dtype),
        in_specs=[pl.BlockSpec(memory_space=pl.ANY)], out_specs=pl.BlockSpec(memory_space=pl.ANY),
        scratch_shapes=[pltpu.VMEM((HOT, planes - 1, most, rows.shape[2]), rows.dtype), pltpu.SemaphoreType.DMA((n,)),
                        pltpu.SemaphoreType.DMA((n,)), pltpu.SemaphoreType.DMA((HOT, planes - 1)),
                        pltpu.SemaphoreType.DMA((HOT, planes - 1)), pltpu.SemaphoreType.DMA],
        compiler_params=pltpu.CompilerParams(collective_id=1, has_side_effects=True))(rows)


def solution(mesh):
    def local_step(token_ids, tok_shard, pos_table, type_row, emb_gain, emb_bias, w_qkv, b_qkv, w_out, b_out,
                   ln1_gain, ln1_bias, w_ffn_in, b_ffn_in, w_ffn_out, b_ffn_out, ln2_gain, ln2_bias):
        n_dev = mesh.shape['fsdp']
        me = lax.axis_index('fsdp')
        batch_dev, seq_len = token_ids.shape
        n_tok = batch_dev * seq_len
        shard_rows, width = tok_shard.shape
        num_heads, head_dim = w_out.shape[0], w_out.shape[1]
        first = [w_qkv.T, w_out.reshape(num_heads * head_dim, -1).T]
        second = [w_ffn_in.T, w_ffn_out]
        weights_a = lax.all_gather(jnp.concatenate(first, axis=0), 'fsdp', axis=0, tiled=False)
        weights_b = lax.all_gather(jnp.concatenate(second, axis=0), 'fsdp', axis=0, tiled=False)

        ids = token_ids.reshape(n_tok)
        keep = ids != PAD_ID
        asks = keep & (ids >= HEAD)
        owner = jnp.where(asks, ids // shard_rows, n_dev)
        place = jnp.arange(n_tok, dtype=jnp.int32)
        lanes = jnp.arange(128, dtype=jnp.int32)
        mine = (owner[:, None] == lanes[None, :]) & (lanes < n_dev)[None, :]
        before = (place[None, :] < place[:, None]).astype(jnp.bfloat16)
        ranks = jnp.dot(before, mine.astype(jnp.bfloat16), preferred_element_type=jnp.float32)
        count = jnp.sum(mine.astype(jnp.float32), axis=0)
        rank = jnp.sum(jnp.where(mine, ranks, 0.0), axis=1).astype(jnp.int32)
        starts, slots = bases()
        cap, base = jnp.zeros_like(owner), jnp.zeros_like(owner)
        for (lo, hi, c), b in zip(CAPS, starts):
            inside = (owner >= lo) & (owner < hi)
            cap = jnp.where(inside, c, cap)
            base = jnp.where(inside, b + (owner - lo) * c, base)
        fits = rank < cap
        slot = jnp.where(fits, base + rank, -1)
        wide = slots + -slots % 128
        slotted = jnp.sum(jnp.where(slot[:, None] == jnp.arange(wide, dtype=jnp.int32)[None, :],
                                    ids.astype(jnp.float32)[:, None], 0.0), axis=0)

        small = [emb_gain, emb_bias, ln1_gain, ln1_bias, ln2_gain, ln2_bias, b_out, b_ffn_out, b_qkv, b_ffn_in]
        message = jnp.concatenate([slotted, count] + small)
        message = jnp.pad(message, (0, -message.shape[0] % 1024))
        told, piece = tell(n_dev, message.reshape(-1, 128), tok_shard)
        told = told.reshape(n_dev, -1)
        head = lax.all_gather(piece, 'fsdp', axis=0, tiled=True)
        at = wide + 128
        vectors = []
        for v in small:
            vectors.append(told[:, at:at + v.shape[0]].reshape(-1))
            at += v.shape[0]
        emb_g, emb_b, ln1_g, ln1_b, ln2_g, ln2_b, b_out_f, b_back_f, b_qkv_f, b_in_f = vectors

        my_base = jnp.int32(0)
        for (lo, hi, c), b in zip(CAPS, starts):
            my_base = jnp.where((me >= lo) & (me < hi), b + (me - lo) * c, my_base)
        most = max(c for _, _, c in CAPS)
        wanted = lax.dynamic_slice(told, (0, my_base), (n_dev, most)).astype(jnp.int32) - me * shard_rows
        wanted = jnp.clip(wanted, 0, shard_rows - 1)
        wanted = wanted.reshape(n_dev // PLANE, PLANE, most).transpose(1, 0, 2)
        rows = jnp.take(tok_shard, wanted.reshape(-1), axis=0, mode='clip').reshape(n_dev, most, width)
        got = swap(n_dev, rows)
        spot = jnp.where(ids < HEAD, head_spot(n_dev, ids), HEAD + jnp.maximum(slot, 0))

        caps = jnp.concatenate([jnp.full((hi - lo,), c, jnp.float32) for lo, hi, c in CAPS])
        left = jnp.max(told[:, wide:wide + n_dev] - caps[None, :])
        rounds = (jnp.maximum(left, 0.0).astype(jnp.int32) + EXTRA - 1) // EXTRA

        def again(state):
            r, rows_now = state
            extra = rank - cap - r * EXTRA
            live = asks & (extra >= 0) & (extra < EXTRA)
            at_slot = jnp.where(live, owner * EXTRA + extra, n_dev * EXTRA)
            ask = jnp.zeros((n_dev * EXTRA + 1,), jnp.int32).at[at_slot].set(ids)[:-1]
            asked = lax.all_to_all(ask.reshape(n_dev, EXTRA), 'fsdp', 0, 0, tiled=True)
            asked = jnp.clip(asked - me * shard_rows, 0, shard_rows - 1)
            found = jnp.take(tok_shard, asked.reshape(-1), axis=0, mode='clip').reshape(n_dev, EXTRA, width)
            back = lax.all_to_all(found, 'fsdp', 0, 0, tiled=True).reshape(n_dev * EXTRA, width)
            new = jnp.take(back, jnp.where(live, at_slot, 0), axis=0, mode='clip')
            return r + 1, jnp.where(live[:, None], new, rows_now)

        def slow(got_now, spot_now):
            rows_now = jnp.take(jnp.concatenate([head, got_now], axis=0), spot_now, axis=0, mode='clip')
            _, rows_now = lax.while_loop(lambda state: state[0] < rounds, again, (jnp.int32(0), rows_now))
            return jnp.pad(rows_now, ((0, slots - n_tok), (0, 0))), jnp.where(ids == PAD_ID, spot_now, HEAD + place)

        got, spot = lax.cond(rounds > 0, slow, lambda g, p: (g, p), got, spot)
        vecs = jnp.stack([emb_g, emb_b, ln1_g, ln1_b, ln2_g, ln2_b, b_out_f, b_back_f])
        x = attend(num_heads, head_dim, batch_dev, spot, head, got, pos_table, type_row, vecs, b_qkv_f, weights_a,
                   [w.shape[0] for w in first])
        return feed(x, vecs, b_in_f, weights_b, [w.shape[0] for w in second])

    vec_spec = P('fsdp')
    in_specs = (P('fsdp', None), P('fsdp', None), P(None, None), P(None), vec_spec, vec_spec,
                P(None, 'fsdp'), vec_spec, P(None, None, 'fsdp'), vec_spec, vec_spec, vec_spec,
                P(None, 'fsdp'), vec_spec, P('fsdp', None), vec_spec, vec_spec, vec_spec)
    return jax.shard_map(local_step, mesh=mesh, in_specs=in_specs, out_specs=P('fsdp', None, None), check_vma=False)
```

```python
import functools

import jax
import jax.numpy as jnp
from jax import lax
from jax.experimental import pallas as pl
from jax.experimental.pallas import tpu as pltpu
from jax.sharding import PartitionSpec as P


PAD_ID = 1
LN_EPS = 1e-5


SQRT_HALF = 0.5 ** 0.5
FFN_PART = 768


def norm(z, gain, shift):
    centered = z - jnp.mean(z, axis=-1, keepdims=True)
    var = jnp.mean(centered * centered, axis=-1, keepdims=True)
    return centered * lax.rsqrt(var + LN_EPS) * gain + shift


def times(a, b):
    return jnp.dot(a, b, preferred_element_type=jnp.float32)


def times_t(a, b):
    return lax.dot_general(a, b, (((1,), (1,)), ((), ())), preferred_element_type=jnp.float32)


def flat(ref):
    return ref.reshape(ref.shape[0] * ref.shape[1], ref.shape[2])


def attention_kernel(dims, spot_row_ref, got_ref, pos_ref, type_ref, vec_ref, b_qkv_ref, head_ref, w_qkv_ref, w_out_ref, out_ref,
                     qkv_ref, ctx_ref, x_ref):
    heads, size = dims
    seq, width = out_ref.shape[1:]
    head_ref, w_qkv_ref, w_out_ref = flat(head_ref), flat(w_qkv_ref), flat(w_out_ref)
    spot = jnp.transpose(jnp.broadcast_to(spot_row_ref[0].astype(jnp.float32), (8, seq)))[:, 0:1].astype(jnp.int32)
    total = jnp.zeros((seq, width), jnp.float32)
    step = 256
    for ref, first in ((head_ref, 0), (got_ref, head_ref.shape[0])):
        for at in range(0, ref.shape[0], step):
            hit = spot == lax.broadcasted_iota(jnp.int32, (seq, step), 1) + (first + at)
            total += times(jnp.where(hit, 1.0, 0.0).astype(jnp.bfloat16), ref[at:at + step, :])
    pos = jnp.where(spot != PAD_ID, pos_ref[2:2 + seq, :].astype(jnp.float32), pos_ref[1:2, :].astype(jnp.float32))
    embedded = total + pos + type_ref[...].astype(jnp.float32)
    x_ref[...] = norm(embedded, vec_ref[0:1, :], vec_ref[1:2, :]).astype(jnp.bfloat16)

    part = 2 * width // 2
    for at in range(0, 3 * width, part):
        qkv_ref[:, at:at + part] = (times_t(x_ref[...], w_qkv_ref[at:at + part, :])
                                    + b_qkv_ref[:, at:at + part]).astype(jnp.bfloat16)

    masked = jnp.where(spot_row_ref[0] != PAD_ID, 0.0, -1e30)
    low = lax.broadcasted_iota(jnp.int32, (1, 2 * size), 1) < size
    for pair in range(heads // 2):
        at = pair * 2 * size
        q = qkv_ref[:, at:at + 2 * size]
        k = qkv_ref[:, width + at:width + at + 2 * size]
        v = qkv_ref[:, 2 * width + at:2 * width + at + 2 * size]
        zero = jnp.zeros_like(q)
        mixed = []
        for mine in (low, ~low):
            s = times_t(jnp.where(mine, q, zero), k) * size ** -0.5 + masked
            p = jnp.exp(s - jnp.max(s, axis=-1, keepdims=True))
            p = p * (1.0 / jnp.sum(p, axis=-1, keepdims=True))
            mixed.append(times(p.astype(jnp.bfloat16), v))
        ctx_ref[:, at:at + 2 * size] = jnp.where(low, mixed[0], mixed[1]).astype(jnp.bfloat16)

    a = (times_t(ctx_ref[...], w_out_ref[...]) + vec_ref[6:7, :]).astype(jnp.bfloat16)
    z = x_ref[...].astype(jnp.float32) + a.astype(jnp.float32)
    out_ref[0] = norm(z, vec_ref[2:3, :], vec_ref[3:4, :]).astype(jnp.bfloat16)


def ffn_kernel(x_ref, vec_ref, b_in_ref, w_in_ref, w_back_ref, out_ref):
    w_in_ref, w_back_ref = flat(w_in_ref), flat(w_back_ref)
    x = x_ref[0]
    total = jnp.zeros(x.shape, jnp.float32)
    for at in range(0, b_in_ref.shape[1], FFN_PART):
        h = times_t(x, w_in_ref[at:at + FFN_PART, :]) + b_in_ref[:, at:at + FFN_PART]
        h = (0.5 * h * (1.0 + lax.erf(h * SQRT_HALF))).astype(jnp.bfloat16)
        total += times(h, w_back_ref[at:at + FFN_PART, :])
    z = x.astype(jnp.float32) + (total + vec_ref[7:8, :])
    out_ref[0] = norm(z, vec_ref[4:5, :], vec_ref[5:6, :]).astype(jnp.bfloat16)


def whole(*shape):
    return pl.BlockSpec(shape, lambda b: (0,) * len(shape), pipeline_mode=pl.Buffered(1))


def each(*shape):
    return pl.BlockSpec((1,) + shape, lambda b: (b,) + (0,) * len(shape))


def pieces(weights, sizes):
    out, at = [], 0
    for rows in sizes:
        out.append(pl.BlockSpec((pl.Element(weights.shape[0]), pl.Element(rows), pl.Element(weights.shape[2])),
                                functools.partial(lambda i, b: (0, i, 0), at), pipeline_mode=pl.Buffered(1)))
        at += rows
    return out


def attend(heads, size, batch, spot, got, pos_table, type_row, vecs, b_qkv, weights, sizes):
    seq = spot.shape[0] // batch
    width = got.shape[1]
    block = pltpu.VMEM((seq, width), jnp.bfloat16)
    return pl.pallas_call(
        functools.partial(attention_kernel, (heads, size)),
        out_shape=jax.ShapeDtypeStruct((batch, seq, width), jnp.bfloat16),
        grid=(batch,),
        in_specs=[each(1, seq), whole(*got.shape), whole(*pos_table.shape), whole(1, width),
                  whole(8, width), whole(1, 3 * width)] + pieces(weights, sizes),
        out_specs=each(seq, width),
        scratch_shapes=[pltpu.VMEM((seq, 3 * width), jnp.bfloat16), block, block],
        compiler_params=pltpu.CompilerParams(vmem_limit_bytes=60 << 20),
        cost_estimate=pl.CostEstimate(flops=20 * 10 ** 9, bytes_accessed=15 * 10 ** 6, transcendentals=7 * 10 ** 6))(
            spot.reshape(batch, 1, seq), got, pos_table, type_row[None, :], vecs,
            b_qkv[None, :], *([weights] * len(sizes)))


def feed(x, vecs, b_in, weights, sizes):
    batch, seq, width = x.shape
    return pl.pallas_call(
        ffn_kernel, out_shape=jax.ShapeDtypeStruct(x.shape, jnp.bfloat16), grid=(batch,),
        in_specs=[each(seq, width), whole(8, width), whole(1, b_in.shape[0])] + pieces(weights, sizes),
        out_specs=each(seq, width),
        compiler_params=pltpu.CompilerParams(vmem_limit_bytes=60 << 20),
        cost_estimate=pl.CostEstimate(flops=15 * 10 ** 9, bytes_accessed=15 * 10 ** 6, transcendentals=5 * 10 ** 6))(
            x, vecs, b_in[None, :], *([weights] * len(sizes)))


HEAD = 2048
CAPS = ((0, 1, 168), (1, 2, 88), (2, 4, 64), (4, 8, 48), (8, 32, 40))
HOT = 2
EXTRA = 48
PLANE = 8
MESH = pl.DeviceIdType.MESH


def others(n, me, one):
    def body(k, carry):
        one(k, lax.rem(me + k, n))
        return carry

    lax.fori_loop(1, n, body, 0)


def meet(n, me):
    barrier = pltpu.get_barrier_semaphore()
    others(n, me, lambda k, dev: pl.semaphore_signal(barrier, inc=1, device_id=(dev,), device_id_type=MESH))
    pl.semaphore_wait(barrier, n - 1)


def tell_kernel(n, part, msg_ref, table_ref, told_ref, piece_ref, relay_ref, send_sem, recv_sem, out_sem, in_sem, relay_sem,
                own_sem):
    me = lax.axis_index('fsdp')
    planes = n // PLANE
    group = part * planes
    meet(n, me)

    def note(k, dev, slot):
        return pltpu.make_async_remote_copy(msg_ref, told_ref.at[slot], send_sem.at[k], recv_sem.at[slot],
                                            device_id=(dev,), device_id_type=MESH)

    def lend(p):
        return pltpu.make_async_remote_copy(table_ref.at[pl.ds(p * group, group)], relay_ref, out_sem.at[p], relay_sem,
                                            device_id=(p,), device_id_type=MESH)

    def part_of(ref, z, dev):
        return pltpu.make_async_remote_copy(ref.at[pl.ds(z * part, part)], piece_ref, out_sem.at[PLANE + z], in_sem,
                                            device_id=(dev,), device_id_type=MESH)

    def own():
        return pltpu.make_async_copy(table_ref.at[pl.ds(0, part)], piece_ref, own_sem)

    others(n, me, lambda k, dev: note(k, dev, me).start())

    @pl.when(me == 0)
    def _():
        for p in range(PLANE - 1, 0, -1):
            lend(p).start()
        for z in range(1, planes):
            part_of(table_ref, z, z * PLANE).start()
        own().start()

    told_ref[me] = msg_ref[...]

    @pl.when((me > 0) & (me < PLANE))
    def _():
        lend(0).wait_recv()
        for z in range(planes - 1, 0, -1):
            part_of(relay_ref, z, z * PLANE + me).start()
        piece_ref[...] = relay_ref[0:part, :]

    others(n, me, lambda k, dev: note(k, dev, dev).wait_recv())
    others(n, me, lambda k, dev: note(k, dev, me).wait_send())

    @pl.when(me == 0)
    def _():
        own().wait()
        for p in range(1, PLANE):
            lend(p).wait_send()
        for z in range(1, planes):
            part_of(table_ref, z, z * PLANE).wait_send()

    @pl.when((me > 0) & (me < PLANE))
    def _():
        for z in range(1, planes):
            part_of(relay_ref, z, z * PLANE + me).wait_send()

    @pl.when(me >= PLANE)
    def _():
        part_of(relay_ref, 0, me).wait_recv()


def tell(n, msg, table):
    part = HEAD // n
    return pl.pallas_call(
        lambda *refs: tell_kernel(n, part, *refs),
        out_shape=(jax.ShapeDtypeStruct((n,) + msg.shape, msg.dtype),
                   jax.ShapeDtypeStruct((part, table.shape[1]), table.dtype)),
        in_specs=[pl.BlockSpec(memory_space=pltpu.VMEM), pl.BlockSpec(memory_space=pl.ANY)],
        out_specs=(pl.BlockSpec(memory_space=pltpu.VMEM), pl.BlockSpec(memory_space=pltpu.VMEM)),
        scratch_shapes=[pltpu.VMEM((part * (n // PLANE), table.shape[1]), table.dtype),
                        pltpu.SemaphoreType.DMA((n,)), pltpu.SemaphoreType.DMA((n,)),
                        pltpu.SemaphoreType.DMA((PLANE + n // PLANE,)), pltpu.SemaphoreType.DMA, pltpu.SemaphoreType.DMA,
                        pltpu.SemaphoreType.DMA],
        compiler_params=pltpu.CompilerParams(collective_id=0, has_side_effects=True))(msg, table)


def head_spot(n, ids):
    part = HEAD // n
    planes = n // PLANE
    at = ids // part
    return ((at % planes) * PLANE + at // planes) * part + ids % part


def bases():
    out, at = [], 0
    for lo, hi, cap in CAPS:
        out.append(at)
        at += (hi - lo) * cap
    return out, at


def relayed(p, z):
    return z > 0 and 2 <= p and p < PLANE - 1 and (p, z) != (PLANE - 2, 3)


def swap_kernel(n, send_ref, recv_ref, relay_ref, send_sem, recv_sem, lend_sem, pass_sem, own_sem):
    me = lax.axis_index('fsdp')
    planes = n // PLANE
    meet(n, me)
    starts, _ = bases()

    def spot(c, dev):
        lo, _, cap = CAPS[c]
        return recv_ref.at[pl.ds(pl.multiple_of(starts[c] + (dev - lo) * cap, 8), cap)]

    def block(c, dev):
        return send_ref.at[lax.rem(dev, PLANE) * planes + lax.div(dev, PLANE), pl.ds(0, CAPS[c][2])]

    def row(c, k, dev, owner):
        return pltpu.make_async_remote_copy(block(c, dev), spot(c, owner), send_sem.at[k], recv_sem.at[owner],
                                            device_id=(dev,), device_id_type=MESH)

    def held(c, z):
        return relay_ref.at[c, z - 1, pl.ds(0, CAPS[c][2])]

    def lend(c, p, z):
        return pltpu.make_async_remote_copy(send_ref.at[p * planes + z, pl.ds(0, CAPS[c][2])], held(c, z),
                                            send_sem.at[z * PLANE + p], lend_sem.at[c, z - 1], device_id=(p,),
                                            device_id_type=MESH)

    def hand_on(c, z):
        return pltpu.make_async_remote_copy(held(c, z), spot(c, c), pass_sem.at[c, z - 1], recv_sem.at[c],
                                            device_id=(z * PLANE + me,), device_id_type=MESH)

    def own(c):
        return pltpu.make_async_copy(block(c, me), spot(c, me), own_sem)

    def hot_sends(c):
        for z in range(planes - 1, -1, -1):
            for p in range(PLANE):
                dev = z * PLANE + p
                if relayed(p, z):
                    yield lend(c, p, z)
                elif dev != c:
                    yield row(c, dev, jnp.int32(dev), c)

    def relays():
        for p in range(PLANE):
            zs = [z for z in range(planes - 1, 0, -1) if relayed(p, z)]
            if zs:
                yield p, zs

    for c, (lo, hi, cap) in enumerate(CAPS):
        @pl.when((me >= lo) & (me < hi))
        def _(c=c):
            own(c).start()
            if c < HOT:
                for copy in hot_sends(c):
                    copy.start()
            else:
                others(n, me, lambda k, dev: row(c, k, dev, me).start())

    for p, zs in relays():
        @pl.when(me == p)
        def _(zs=zs):
            for z in zs:
                for c in range(HOT):
                    lend(c, 0, z).wait_recv()
                    hand_on(c, z).start()

    for c, (lo, hi, cap) in enumerate(CAPS):
        def one(dev, carry, c=c):
            @pl.when(dev != me)
            def _():
                row(c, 0, dev, dev).wait_recv()

            return carry

        lax.fori_loop(lo, hi, one, 0)

    for c, (lo, hi, cap) in enumerate(CAPS):
        @pl.when((me >= lo) & (me < hi))
        def _(c=c):
            own(c).wait()
            if c < HOT:
                for copy in hot_sends(c):
                    copy.wait_send()
            else:
                others(n, me, lambda k, dev: row(c, k, dev, me).wait_send())

    for p, zs in relays():
        @pl.when(me == p)
        def _(zs=zs):
            for z in zs:
                for c in range(HOT):
                    hand_on(c, z).wait_send()


def swap(n, rows):
    planes = n // PLANE
    most = max(cap for _, _, cap in CAPS[:HOT])
    return pl.pallas_call(
        lambda *refs: swap_kernel(n, *refs),
        out_shape=jax.ShapeDtypeStruct((bases()[1], rows.shape[2]), rows.dtype),
        in_specs=[pl.BlockSpec(memory_space=pl.ANY)], out_specs=pl.BlockSpec(memory_space=pl.ANY),
        scratch_shapes=[pltpu.VMEM((HOT, planes - 1, most, rows.shape[2]), rows.dtype), pltpu.SemaphoreType.DMA((n,)),
                        pltpu.SemaphoreType.DMA((n,)), pltpu.SemaphoreType.DMA((HOT, planes - 1)),
                        pltpu.SemaphoreType.DMA((HOT, planes - 1)), pltpu.SemaphoreType.DMA],
        compiler_params=pltpu.CompilerParams(collective_id=1, has_side_effects=True))(rows)


def solution(mesh):
    def local_step(token_ids, tok_shard, pos_table, type_row, emb_gain, emb_bias, w_qkv, b_qkv, w_out, b_out,
                   ln1_gain, ln1_bias, w_ffn_in, b_ffn_in, w_ffn_out, b_ffn_out, ln2_gain, ln2_bias):
        n_dev = mesh.shape['fsdp']
        me = lax.axis_index('fsdp')
        batch_dev, seq_len = token_ids.shape
        n_tok = batch_dev * seq_len
        shard_rows, width = tok_shard.shape
        num_heads, head_dim = w_out.shape[0], w_out.shape[1]
        ids = token_ids.reshape(n_tok)
        keep = ids != PAD_ID
        asks = keep & (ids >= HEAD)
        owner = jnp.where(asks, ids // shard_rows, n_dev)
        place = jnp.arange(n_tok, dtype=jnp.int32)
        lanes = jnp.arange(128, dtype=jnp.int32)
        mine = (owner[:, None] == lanes[None, :]) & (lanes < n_dev)[None, :]
        before = (place[None, :] < place[:, None]).astype(jnp.bfloat16)
        ranks = jnp.dot(before, mine.astype(jnp.bfloat16), preferred_element_type=jnp.float32)
        count = jnp.sum(mine.astype(jnp.float32), axis=0)
        rank = jnp.sum(jnp.where(mine, ranks, 0.0), axis=1).astype(jnp.int32)
        starts, slots = bases()
        cap, base = jnp.zeros_like(owner), jnp.zeros_like(owner)
        for (lo, hi, c), b in zip(CAPS, starts):
            inside = (owner >= lo) & (owner < hi)
            cap = jnp.where(inside, c, cap)
            base = jnp.where(inside, b + (owner - lo) * c, base)
        fits = rank < cap
        slot = jnp.where(fits, base + rank, -1)
        wide = slots + -slots % 128
        slotted = jnp.sum(jnp.where(slot[:, None] == jnp.arange(wide, dtype=jnp.int32)[None, :],
                                    ids.astype(jnp.float32)[:, None], 0.0), axis=0)

        small = [emb_gain, emb_bias, ln1_gain, ln1_bias, ln2_gain, ln2_bias, b_out, b_ffn_out, b_qkv, b_ffn_in]
        message = jnp.concatenate([slotted, count] + small)
        message = jnp.pad(message, (0, -message.shape[0] % 1024))
        told, piece = tell(n_dev, message.reshape(-1, 128), tok_shard)
        told = told.reshape(n_dev, -1)
        first = [piece, w_qkv.T, w_out.reshape(num_heads * head_dim, -1).T]
        second = [w_ffn_in.T, w_ffn_out]
        weights_a = lax.all_gather(jnp.concatenate(first, axis=0), 'fsdp', axis=0, tiled=False)
        weights_b = lax.all_gather(jnp.concatenate(second, axis=0), 'fsdp', axis=0, tiled=False)

        at = wide + 128
        vectors = []
        for v in small:
            vectors.append(told[:, at:at + v.shape[0]].reshape(-1))
            at += v.shape[0]
        emb_g, emb_b, ln1_g, ln1_b, ln2_g, ln2_b, b_out_f, b_back_f, b_qkv_f, b_in_f = vectors

        my_base = jnp.int32(0)
        for (lo, hi, c), b in zip(CAPS, starts):
            my_base = jnp.where((me >= lo) & (me < hi), b + (me - lo) * c, my_base)
        most = max(c for _, _, c in CAPS)
        wanted = lax.dynamic_slice(told, (0, my_base), (n_dev, most)).astype(jnp.int32) - me * shard_rows
        wanted = jnp.clip(wanted, 0, shard_rows - 1)
        wanted = wanted.reshape(n_dev // PLANE, PLANE, most).transpose(1, 0, 2)
        rows = jnp.take(tok_shard, wanted.reshape(-1), axis=0, mode='clip').reshape(n_dev, most, width)
        got = swap(n_dev, rows)
        spot = jnp.where(ids < HEAD, head_spot(n_dev, ids), HEAD + jnp.maximum(slot, 0))

        caps = jnp.concatenate([jnp.full((hi - lo,), c, jnp.float32) for lo, hi, c in CAPS])
        left = jnp.max(told[:, wide:wide + n_dev] - caps[None, :])
        rounds = (jnp.maximum(left, 0.0).astype(jnp.int32) + EXTRA - 1) // EXTRA

        def again(state):
            r, rows_now = state
            extra = rank - cap - r * EXTRA
            live = asks & (extra >= 0) & (extra < EXTRA)
            at_slot = jnp.where(live, owner * EXTRA + extra, n_dev * EXTRA)
            ask = jnp.zeros((n_dev * EXTRA + 1,), jnp.int32).at[at_slot].set(ids)[:-1]
            asked = lax.all_to_all(ask.reshape(n_dev, EXTRA), 'fsdp', 0, 0, tiled=True)
            asked = jnp.clip(asked - me * shard_rows, 0, shard_rows - 1)
            found = jnp.take(tok_shard, asked.reshape(-1), axis=0, mode='clip').reshape(n_dev, EXTRA, width)
            back = lax.all_to_all(found, 'fsdp', 0, 0, tiled=True).reshape(n_dev * EXTRA, width)
            new = jnp.take(back, jnp.where(live, at_slot, 0), axis=0, mode='clip')
            return r + 1, jnp.where(live[:, None], new, rows_now)

        def slow(got_now, spot_now):
            head = weights_a[:, :piece.shape[0]].reshape(HEAD, width)
            rows_now = jnp.take(jnp.concatenate([head, got_now], axis=0), spot_now, axis=0, mode='clip')
            _, rows_now = lax.while_loop(lambda state: state[0] < rounds, again, (jnp.int32(0), rows_now))
            return jnp.pad(rows_now, ((0, slots - n_tok), (0, 0))), jnp.where(ids == PAD_ID, spot_now, HEAD + place)

        got, spot = lax.cond(rounds > 0, slow, lambda g, p: (g, p), got, spot)
        vecs = jnp.stack([emb_g, emb_b, ln1_g, ln1_b, ln2_g, ln2_b, b_out_f, b_back_f])
        x = attend(num_heads, head_dim, batch_dev, spot, got, pos_table, type_row, vecs, b_qkv_f, weights_a,
                   [w.shape[0] for w in first])
        return feed(x, vecs, b_in_f, weights_b, [w.shape[0] for w in second])

    vec_spec = P('fsdp')
    in_specs = (P('fsdp', None), P('fsdp', None), P(None, None), P(None), vec_spec, vec_spec,
                P(None, 'fsdp'), vec_spec, P(None, None, 'fsdp'), vec_spec, vec_spec, vec_spec,
                P(None, 'fsdp'), vec_spec, P('fsdp', None), vec_spec, vec_spec, vec_spec)
    return jax.shard_map(local_step, mesh=mesh, in_specs=in_specs, out_specs=P('fsdp', None, None), check_vma=False)
```

```python
import functools

import jax
import jax.numpy as jnp
from jax import lax
from jax.experimental import pallas as pl
from jax.experimental.pallas import tpu as pltpu
from jax.sharding import PartitionSpec as P


PAD_ID = 1
LN_EPS = 1e-5


SQRT_HALF = 0.5 ** 0.5
LOG2_E = 1.4426950408889634
FFN_PART = 768


def norm(z, gain, shift):
    centered = z - jnp.mean(z, axis=-1, keepdims=True)
    var = jnp.mean(centered * centered, axis=-1, keepdims=True)
    return centered * lax.rsqrt(var + LN_EPS) * gain + shift


def times(a, b):
    return jnp.dot(a, b, preferred_element_type=jnp.float32)


def times_t(a, b):
    return lax.dot_general(a, b, (((1,), (1,)), ((), ())), preferred_element_type=jnp.float32)


def flat(ref):
    return ref.reshape(ref.shape[0] * ref.shape[1], ref.shape[2])


def attention_kernel(dims, spot_row_ref, got_ref, pos_ref, type_ref, vec_ref, b_qkv_ref, head_ref, w_qkv_ref, w_out_ref, out_ref,
                     qkv_ref, ctx_ref, x_ref):
    heads, size = dims
    seq, width = out_ref.shape[1:]
    head_ref, w_qkv_ref, w_out_ref = flat(head_ref), flat(w_qkv_ref), flat(w_out_ref)
    spot = jnp.transpose(jnp.broadcast_to(spot_row_ref[0].astype(jnp.float32), (8, seq)))[:, 0:1].astype(jnp.int32)
    total = jnp.zeros((seq, width), jnp.float32)
    step = 256
    for ref, first in ((head_ref, 0), (got_ref, head_ref.shape[0])):
        for at in range(0, ref.shape[0], step):
            hit = spot == lax.broadcasted_iota(jnp.int32, (seq, step), 1) + (first + at)
            total += times(jnp.where(hit, 1.0, 0.0).astype(jnp.bfloat16), ref[at:at + step, :])
    pos = jnp.where(spot != PAD_ID, pos_ref[2:2 + seq, :].astype(jnp.float32), pos_ref[1:2, :].astype(jnp.float32))
    embedded = total + pos + type_ref[...].astype(jnp.float32)
    x_ref[...] = norm(embedded, vec_ref[0:1, :], vec_ref[1:2, :]).astype(jnp.bfloat16)

    part = 2 * width // 2
    for at in range(0, 3 * width, part):
        qkv_ref[:, at:at + part] = (times_t(x_ref[...], w_qkv_ref[at:at + part, :])
                                    + b_qkv_ref[:, at:at + part]).astype(jnp.bfloat16)

    masked = jnp.where(spot_row_ref[0] != PAD_ID, 0.0, -1e30)
    low = lax.broadcasted_iota(jnp.int32, (1, 2 * size), 1) < size
    for pair in range(heads // 2):
        at = pair * 2 * size
        q = qkv_ref[:, at:at + 2 * size]
        k = qkv_ref[:, width + at:width + at + 2 * size]
        v = qkv_ref[:, 2 * width + at:2 * width + at + 2 * size]
        zero = jnp.zeros_like(q)
        mixed = []
        for mine in (low, ~low):
            s = times_t(jnp.where(mine, q, zero), k) + masked
            p = jnp.exp2((s - jnp.max(s, axis=-1, keepdims=True)) * (size ** -0.5 * LOG2_E))
            p = p * (1.0 / jnp.sum(p, axis=-1, keepdims=True))
            mixed.append(times(p.astype(jnp.bfloat16), v))
        ctx_ref[:, at:at + 2 * size] = jnp.where(low, mixed[0], mixed[1]).astype(jnp.bfloat16)

    a = (times_t(ctx_ref[...], w_out_ref[...]) + vec_ref[6:7, :]).astype(jnp.bfloat16)
    z = x_ref[...].astype(jnp.float32) + a.astype(jnp.float32)
    out_ref[0] = norm(z, vec_ref[2:3, :], vec_ref[3:4, :]).astype(jnp.bfloat16)


def ffn_kernel(x_ref, vec_ref, b_in_ref, w_in_ref, w_back_ref, out_ref):
    x = x_ref[0]
    total = jnp.zeros(x.shape, jnp.float32)
    for at in range(0, b_in_ref.shape[1], FFN_PART):
        h = times_t(x, w_in_ref[at:at + FFN_PART, :]) + b_in_ref[:, at:at + FFN_PART]
        h = (0.5 * h * (1.0 + lax.erf(h * SQRT_HALF))).astype(jnp.bfloat16)
        total += times(h, w_back_ref[at:at + FFN_PART, :])
    z = x.astype(jnp.float32) + (total + vec_ref[7:8, :])
    out_ref[0] = norm(z, vec_ref[4:5, :], vec_ref[5:6, :]).astype(jnp.bfloat16)


def whole(*shape):
    return pl.BlockSpec(shape, lambda b: (0,) * len(shape), pipeline_mode=pl.Buffered(1))


def each(*shape):
    return pl.BlockSpec((1,) + shape, lambda b: (b,) + (0,) * len(shape))


def pieces(weights, sizes):
    out, at = [], 0
    for rows in sizes:
        out.append(pl.BlockSpec((pl.Element(weights.shape[0]), pl.Element(rows), pl.Element(weights.shape[2])),
                                functools.partial(lambda i, b: (0, i, 0), at), pipeline_mode=pl.Buffered(1)))
        at += rows
    return out


def attend(heads, size, batch, spot, got, pos_table, type_row, vecs, b_qkv, weights, sizes):
    seq = spot.shape[0] // batch
    width = got.shape[1]
    block = pltpu.VMEM((seq, width), jnp.bfloat16)
    return pl.pallas_call(
        functools.partial(attention_kernel, (heads, size)),
        out_shape=jax.ShapeDtypeStruct((batch, seq, width), jnp.bfloat16),
        grid=(batch,),
        in_specs=[each(1, seq), whole(*got.shape), whole(*pos_table.shape), whole(1, width),
                  whole(8, width), whole(1, 3 * width)] + pieces(weights, sizes),
        out_specs=each(seq, width),
        scratch_shapes=[pltpu.VMEM((seq, 3 * width), jnp.bfloat16), block, block],
        compiler_params=pltpu.CompilerParams(vmem_limit_bytes=60 << 20),
        cost_estimate=pl.CostEstimate(flops=20 * 10 ** 9, bytes_accessed=15 * 10 ** 6, transcendentals=7 * 10 ** 6))(
            spot.reshape(batch, 1, seq), got, pos_table, type_row[None, :], vecs,
            b_qkv[None, :], *([weights] * len(sizes)))


def feed(x, vecs, b_in, w_in, w_back):
    batch, seq, width = x.shape
    return pl.pallas_call(
        ffn_kernel, out_shape=jax.ShapeDtypeStruct(x.shape, jnp.bfloat16), grid=(batch,),
        in_specs=[each(seq, width), whole(8, width), whole(1, b_in.shape[0]), whole(*w_in.shape), whole(*w_back.shape)],
        out_specs=each(seq, width),
        compiler_params=pltpu.CompilerParams(vmem_limit_bytes=60 << 20),
        cost_estimate=pl.CostEstimate(flops=15 * 10 ** 9, bytes_accessed=15 * 10 ** 6, transcendentals=5 * 10 ** 6))(
            x, vecs, b_in[None, :], w_in, w_back)


HEAD = 2048
CAPS = ((0, 1, 152), (1, 2, 88), (2, 4, 72), (4, 8, 48), (8, 32, 40))
HOT = 2
EXTRA = 48
PLANE = 8
MESH = pl.DeviceIdType.MESH


def others(n, me, one):
    def body(k, carry):
        one(k, lax.rem(me + k, n))
        return carry

    lax.fori_loop(1, n, body, 0)


def meet(n, me):
    barrier = pltpu.get_barrier_semaphore()
    others(n, me, lambda k, dev: pl.semaphore_signal(barrier, inc=1, device_id=(dev,), device_id_type=MESH))
    pl.semaphore_wait(barrier, n - 1)


def tell_kernel(n, part, msg_ref, table_ref, told_ref, piece_ref, relay_ref, send_sem, recv_sem, out_sem, in_sem, relay_sem,
                own_sem):
    me = lax.axis_index('fsdp')
    planes = n // PLANE
    group = part * planes
    meet(n, me)

    def note(k, dev, slot):
        return pltpu.make_async_remote_copy(msg_ref, told_ref.at[slot], send_sem.at[k], recv_sem.at[slot],
                                            device_id=(dev,), device_id_type=MESH)

    def lend(p):
        return pltpu.make_async_remote_copy(table_ref.at[pl.ds(p * group, group)], relay_ref, out_sem.at[p], relay_sem,
                                            device_id=(p,), device_id_type=MESH)

    def part_of(ref, z, dev):
        return pltpu.make_async_remote_copy(ref.at[pl.ds(z * part, part)], piece_ref, out_sem.at[PLANE + z], in_sem,
                                            device_id=(dev,), device_id_type=MESH)

    def own():
        return pltpu.make_async_copy(table_ref.at[pl.ds(0, part)], piece_ref, own_sem)

    others(n, me, lambda k, dev: note(k, dev, me).start())

    @pl.when(me == 0)
    def _():
        for p in range(PLANE - 1, 0, -1):
            lend(p).start()
        for z in range(1, planes):
            part_of(table_ref, z, z * PLANE).start()
        own().start()

    told_ref[me] = msg_ref[...]

    @pl.when((me > 0) & (me < PLANE))
    def _():
        lend(0).wait_recv()
        for z in range(planes - 1, 0, -1):
            part_of(relay_ref, z, z * PLANE + me).start()
        piece_ref[...] = relay_ref[0:part, :]

    others(n, me, lambda k, dev: note(k, dev, dev).wait_recv())
    others(n, me, lambda k, dev: note(k, dev, me).wait_send())

    @pl.when(me == 0)
    def _():
        own().wait()
        for p in range(1, PLANE):
            lend(p).wait_send()
        for z in range(1, planes):
            part_of(table_ref, z, z * PLANE).wait_send()

    @pl.when((me > 0) & (me < PLANE))
    def _():
        for z in range(1, planes):
            part_of(relay_ref, z, z * PLANE + me).wait_send()

    @pl.when(me >= PLANE)
    def _():
        part_of(relay_ref, 0, me).wait_recv()


def tell(n, msg, table):
    part = HEAD // n
    return pl.pallas_call(
        lambda *refs: tell_kernel(n, part, *refs),
        out_shape=(jax.ShapeDtypeStruct((n,) + msg.shape, msg.dtype),
                   jax.ShapeDtypeStruct((part, table.shape[1]), table.dtype)),
        in_specs=[pl.BlockSpec(memory_space=pltpu.VMEM), pl.BlockSpec(memory_space=pl.ANY)],
        out_specs=(pl.BlockSpec(memory_space=pltpu.VMEM), pl.BlockSpec(memory_space=pltpu.VMEM)),
        scratch_shapes=[pltpu.VMEM((part * (n // PLANE), table.shape[1]), table.dtype),
                        pltpu.SemaphoreType.DMA((n,)), pltpu.SemaphoreType.DMA((n,)),
                        pltpu.SemaphoreType.DMA((PLANE + n // PLANE,)), pltpu.SemaphoreType.DMA, pltpu.SemaphoreType.DMA,
                        pltpu.SemaphoreType.DMA],
        compiler_params=pltpu.CompilerParams(collective_id=0, has_side_effects=True))(msg, table)


def head_spot(n, ids):
    part = HEAD // n
    planes = n // PLANE
    at = ids // part
    return ((at % planes) * PLANE + at // planes) * part + ids % part


def bases():
    out, at = [], 0
    for lo, hi, cap in CAPS:
        out.append(at)
        at += (hi - lo) * cap
    return out, at


def relayed(p, z):
    return z > 0 and 2 <= p and p < PLANE - 1 and (p, z) != (PLANE - 2, 3)


def swap_kernel(n, send_ref, recv_ref, relay_ref, send_sem, recv_sem, lend_sem, pass_sem, own_sem):
    me = lax.axis_index('fsdp')
    planes = n // PLANE
    meet(n, me)
    starts, _ = bases()

    def spot(c, dev):
        lo, _, cap = CAPS[c]
        return recv_ref.at[pl.ds(pl.multiple_of(starts[c] + (dev - lo) * cap, 8), cap)]

    def block(c, dev):
        return send_ref.at[lax.rem(dev, PLANE) * planes + lax.div(dev, PLANE), pl.ds(0, CAPS[c][2])]

    def row(c, k, dev, owner):
        return pltpu.make_async_remote_copy(block(c, dev), spot(c, owner), send_sem.at[k], recv_sem.at[owner],
                                            device_id=(dev,), device_id_type=MESH)

    def held(c, z):
        return relay_ref.at[c, z - 1, pl.ds(0, CAPS[c][2])]

    def lend(c, p, z):
        return pltpu.make_async_remote_copy(send_ref.at[p * planes + z, pl.ds(0, CAPS[c][2])], held(c, z),
                                            send_sem.at[z * PLANE + p], lend_sem.at[c, z - 1], device_id=(p,),
                                            device_id_type=MESH)

    def hand_on(c, z):
        return pltpu.make_async_remote_copy(held(c, z), spot(c, c), pass_sem.at[c, z - 1], recv_sem.at[c],
                                            device_id=(z * PLANE + me,), device_id_type=MESH)

    def own(c):
        return pltpu.make_async_copy(block(c, me), spot(c, me), own_sem)

    def hot_sends(c):
        for z in range(planes - 1, -1, -1):
            for p in range(PLANE):
                dev = z * PLANE + p
                if relayed(p, z):
                    yield lend(c, p, z)
                elif dev != c:
                    yield row(c, dev, jnp.int32(dev), c)

    def relays():
        for p in range(PLANE):
            zs = [z for z in range(planes - 1, 0, -1) if relayed(p, z)]
            if zs:
                yield p, zs

    for c, (lo, hi, cap) in enumerate(CAPS):
        @pl.when((me >= lo) & (me < hi))
        def _(c=c):
            own(c).start()
            if c < HOT:
                for copy in hot_sends(c):
                    copy.start()
            else:
                others(n, me, lambda k, dev: row(c, k, dev, me).start())

    for p, zs in relays():
        @pl.when(me == p)
        def _(zs=zs):
            for z in zs:
                for c in range(HOT):
                    lend(c, 0, z).wait_recv()
                    hand_on(c, z).start()

    for c, (lo, hi, cap) in enumerate(CAPS):
        def one(dev, carry, c=c):
            @pl.when(dev != me)
            def _():
                row(c, 0, dev, dev).wait_recv()

            return carry

        lax.fori_loop(lo, hi, one, 0)

    for c, (lo, hi, cap) in enumerate(CAPS):
        @pl.when((me >= lo) & (me < hi))
        def _(c=c):
            own(c).wait()
            if c < HOT:
                for copy in hot_sends(c):
                    copy.wait_send()
            else:
                others(n, me, lambda k, dev: row(c, k, dev, me).wait_send())

    for p, zs in relays():
        @pl.when(me == p)
        def _(zs=zs):
            for z in zs:
                for c in range(HOT):
                    hand_on(c, z).wait_send()


def swap(n, rows):
    planes = n // PLANE
    most = max(cap for _, _, cap in CAPS[:HOT])
    return pl.pallas_call(
        lambda *refs: swap_kernel(n, *refs),
        out_shape=jax.ShapeDtypeStruct((bases()[1], rows.shape[2]), rows.dtype),
        in_specs=[pl.BlockSpec(memory_space=pl.ANY)], out_specs=pl.BlockSpec(memory_space=pl.ANY),
        scratch_shapes=[pltpu.VMEM((HOT, planes - 1, most, rows.shape[2]), rows.dtype), pltpu.SemaphoreType.DMA((n,)),
                        pltpu.SemaphoreType.DMA((n,)), pltpu.SemaphoreType.DMA((HOT, planes - 1)),
                        pltpu.SemaphoreType.DMA((HOT, planes - 1)), pltpu.SemaphoreType.DMA],
        compiler_params=pltpu.CompilerParams(collective_id=1, has_side_effects=True))(rows)


def solution(mesh):
    def local_step(token_ids, tok_shard, pos_table, type_row, emb_gain, emb_bias, w_qkv, b_qkv, w_out, b_out,
                   ln1_gain, ln1_bias, w_ffn_in, b_ffn_in, w_ffn_out, b_ffn_out, ln2_gain, ln2_bias):
        n_dev = mesh.shape['fsdp']
        me = lax.axis_index('fsdp')
        batch_dev, seq_len = token_ids.shape
        n_tok = batch_dev * seq_len
        shard_rows, width = tok_shard.shape
        num_heads, head_dim = w_out.shape[0], w_out.shape[1]
        ids = token_ids.reshape(n_tok)
        keep = ids != PAD_ID
        asks = keep & (ids >= HEAD)
        owner = jnp.where(asks, ids // shard_rows, n_dev)
        place = jnp.arange(n_tok, dtype=jnp.int32)
        lanes = jnp.arange(128, dtype=jnp.int32)
        mine = (owner[:, None] == lanes[None, :]) & (lanes < n_dev)[None, :]
        before = (place[None, :] < place[:, None]).astype(jnp.bfloat16)
        ranks = jnp.dot(before, mine.astype(jnp.bfloat16), preferred_element_type=jnp.float32)
        count = jnp.sum(mine.astype(jnp.float32), axis=0)
        rank = jnp.sum(jnp.where(mine, ranks, 0.0), axis=1).astype(jnp.int32)
        starts, slots = bases()
        cap, base = jnp.zeros_like(owner), jnp.zeros_like(owner)
        for (lo, hi, c), b in zip(CAPS, starts):
            inside = (owner >= lo) & (owner < hi)
            cap = jnp.where(inside, c, cap)
            base = jnp.where(inside, b + (owner - lo) * c, base)
        fits = rank < cap
        slot = jnp.where(fits, base + rank, -1)
        wide = slots + -slots % 128
        slotted = jnp.sum(jnp.where(slot[:, None] == jnp.arange(wide, dtype=jnp.int32)[None, :],
                                    ids.astype(jnp.float32)[:, None], 0.0), axis=0)

        small = [emb_gain, emb_bias, ln1_gain, ln1_bias, ln2_gain, ln2_bias, b_out, b_ffn_out, b_qkv, b_ffn_in]
        message = jnp.concatenate([slotted, count] + small)
        message = jnp.pad(message, (0, -message.shape[0] % 1024))
        told, piece = tell(n_dev, message.reshape(-1, 128), tok_shard)
        told = told.reshape(n_dev, -1)
        first = [piece, w_qkv.T, w_out.reshape(num_heads * head_dim, -1).T]
        w_in_full = lax.all_gather(w_ffn_in.T, 'fsdp', axis=0, tiled=True)
        weights_a = lax.all_gather(jnp.concatenate(first, axis=0), 'fsdp', axis=0, tiled=False)
        w_back_full = lax.all_gather(w_ffn_out, 'fsdp', axis=0, tiled=True)

        at = wide + 128
        vectors = []
        for v in small:
            vectors.append(told[:, at:at + v.shape[0]].reshape(-1))
            at += v.shape[0]
        emb_g, emb_b, ln1_g, ln1_b, ln2_g, ln2_b, b_out_f, b_back_f, b_qkv_f, b_in_f = vectors

        my_base = jnp.int32(0)
        for (lo, hi, c), b in zip(CAPS, starts):
            my_base = jnp.where((me >= lo) & (me < hi), b + (me - lo) * c, my_base)
        most = max(c for _, _, c in CAPS)
        wanted = lax.dynamic_slice(told, (0, my_base), (n_dev, most)).astype(jnp.int32) - me * shard_rows
        wanted = jnp.clip(wanted, 0, shard_rows - 1)
        wanted = wanted.reshape(n_dev // PLANE, PLANE, most).transpose(1, 0, 2)
        rows = jnp.take(tok_shard, wanted.reshape(-1), axis=0, mode='clip').reshape(n_dev, most, width)
        got = swap(n_dev, rows)
        spot = jnp.where(ids < HEAD, head_spot(n_dev, ids), HEAD + jnp.maximum(slot, 0))

        caps = jnp.concatenate([jnp.full((hi - lo,), c, jnp.float32) for lo, hi, c in CAPS])
        left = jnp.max(told[:, wide:wide + n_dev] - caps[None, :])
        rounds = (jnp.maximum(left, 0.0).astype(jnp.int32) + EXTRA - 1) // EXTRA

        def again(state):
            r, rows_now = state
            extra = rank - cap - r * EXTRA
            live = asks & (extra >= 0) & (extra < EXTRA)
            at_slot = jnp.where(live, owner * EXTRA + extra, n_dev * EXTRA)
            ask = jnp.zeros((n_dev * EXTRA + 1,), jnp.int32).at[at_slot].set(ids)[:-1]
            asked = lax.all_to_all(ask.reshape(n_dev, EXTRA), 'fsdp', 0, 0, tiled=True)
            asked = jnp.clip(asked - me * shard_rows, 0, shard_rows - 1)
            found = jnp.take(tok_shard, asked.reshape(-1), axis=0, mode='clip').reshape(n_dev, EXTRA, width)
            back = lax.all_to_all(found, 'fsdp', 0, 0, tiled=True).reshape(n_dev * EXTRA, width)
            new = jnp.take(back, jnp.where(live, at_slot, 0), axis=0, mode='clip')
            return r + 1, jnp.where(live[:, None], new, rows_now)

        def slow(got_now, spot_now):
            head = weights_a[:, :piece.shape[0]].reshape(HEAD, width)
            rows_now = jnp.take(jnp.concatenate([head, got_now], axis=0), spot_now, axis=0, mode='clip')
            _, rows_now = lax.while_loop(lambda state: state[0] < rounds, again, (jnp.int32(0), rows_now))
            return jnp.pad(rows_now, ((0, slots - n_tok), (0, 0))), jnp.where(ids == PAD_ID, spot_now, HEAD + place)

        got, spot = lax.cond(rounds > 0, slow, lambda g, p: (g, p), got, spot)
        vecs = jnp.stack([emb_g, emb_b, ln1_g, ln1_b, ln2_g, ln2_b, b_out_f, b_back_f])
        x = attend(num_heads, head_dim, batch_dev, spot, got, pos_table, type_row, vecs, b_qkv_f, weights_a,
                   [w.shape[0] for w in first])
        return feed(x, vecs, b_in_f, w_in_full, w_back_full)

    vec_spec = P('fsdp')
    in_specs = (P('fsdp', None), P('fsdp', None), P(None, None), P(None), vec_spec, vec_spec,
                P(None, 'fsdp'), vec_spec, P(None, None, 'fsdp'), vec_spec, vec_spec, vec_spec,
                P(None, 'fsdp'), vec_spec, P('fsdp', None), vec_spec, vec_spec, vec_spec)
    return jax.shard_map(local_step, mesh=mesh, in_specs=in_specs, out_specs=P('fsdp', None, None), check_vma=False)
```

```python
import functools

import jax
import jax.numpy as jnp
from jax import lax
from jax.experimental import pallas as pl
from jax.experimental.pallas import tpu as pltpu
from jax.sharding import PartitionSpec as P

PAD_ID = 1
LN_EPS = 1e-5


SQRT_HALF = 0.5 ** 0.5
LOG2_E = 1.4426950408889634
FFN_PART = 768


def norm(z, gain, shift):
    centered = z - jnp.mean(z, axis=-1, keepdims=True)
    var = jnp.mean(centered * centered, axis=-1, keepdims=True)
    return centered * lax.rsqrt(var + LN_EPS) * gain + shift


def times(a, b):
    return jnp.dot(a, b, preferred_element_type=jnp.float32)


def times_t(a, b):
    return lax.dot_general(a, b, (((1,), (1,)), ((), ())), preferred_element_type=jnp.float32)


def flat(ref):
    return ref.reshape(ref.shape[0] * ref.shape[1], ref.shape[2])


def layer_kernel(dims, spot_row_ref, got_ref, pos_ref, type_ref, vec_ref, b_qkv_ref, b_in_ref, head_ref, w_qkv_ref, w_out_ref,
                 w_in_ref, w_back_ref, out_ref, qkv_ref, ctx_ref, x_ref):
    heads, size = dims
    seq, width = out_ref.shape[1:]
    head_ref, w_qkv_ref, w_out_ref, w_in_ref, w_back_ref = (
        flat(r) for r in (head_ref, w_qkv_ref, w_out_ref, w_in_ref, w_back_ref))
    spot = jnp.transpose(jnp.broadcast_to(spot_row_ref[0].astype(jnp.float32), (8, seq)))[:, 0:1].astype(jnp.int32)
    total = jnp.zeros((seq, width), jnp.float32)
    step = 256
    for ref, first in ((head_ref, 0), (got_ref, head_ref.shape[0])):
        for at in range(0, ref.shape[0], step):
            hit = spot == lax.broadcasted_iota(jnp.int32, (seq, step), 1) + (first + at)
            total += times(jnp.where(hit, 1.0, 0.0).astype(jnp.bfloat16), ref[at:at + step, :])
    pos = jnp.where(spot != PAD_ID, pos_ref[2:2 + seq, :].astype(jnp.float32), pos_ref[1:2, :].astype(jnp.float32))
    embedded = total + pos + type_ref[...].astype(jnp.float32)
    x_ref[...] = norm(embedded, vec_ref[0:1, :], vec_ref[1:2, :]).astype(jnp.bfloat16)

    part = 2 * width // 2
    for at in range(0, 3 * width, part):
        qkv_ref[:, at:at + part] = (times_t(x_ref[...], w_qkv_ref[at:at + part, :])
                                    + b_qkv_ref[:, at:at + part]).astype(jnp.bfloat16)

    masked = jnp.where(spot_row_ref[0] != PAD_ID, 0.0, -1e30)
    low = lax.broadcasted_iota(jnp.int32, (1, 2 * size), 1) < size
    for pair in range(heads // 2):
        at = pair * 2 * size
        q = qkv_ref[:, at:at + 2 * size]
        k = qkv_ref[:, width + at:width + at + 2 * size]
        v = qkv_ref[:, 2 * width + at:2 * width + at + 2 * size]
        zero = jnp.zeros_like(q)
        mixed = []
        for mine in (low, ~low):
            s = times_t(jnp.where(mine, q, zero), k) + masked
            p = jnp.exp2((s - jnp.max(s, axis=-1, keepdims=True)) * (size ** -0.5 * LOG2_E))
            p = p * (1.0 / jnp.sum(p, axis=-1, keepdims=True))
            mixed.append(times(p.astype(jnp.bfloat16), v))
        ctx_ref[:, at:at + 2 * size] = jnp.where(low, mixed[0], mixed[1]).astype(jnp.bfloat16)

    a = (times_t(ctx_ref[...], w_out_ref[...]) + vec_ref[6:7, :]).astype(jnp.bfloat16)
    z = x_ref[...].astype(jnp.float32) + a.astype(jnp.float32)
    x_ref[...] = norm(z, vec_ref[2:3, :], vec_ref[3:4, :]).astype(jnp.bfloat16)

    total = jnp.zeros((seq, width), jnp.float32)
    for at in range(0, b_in_ref.shape[1], FFN_PART):
        h = times_t(x_ref[...], w_in_ref[at:at + FFN_PART, :]) + b_in_ref[:, at:at + FFN_PART]
        h = (0.5 * h * (1.0 + lax.erf(h * SQRT_HALF))).astype(jnp.bfloat16)
        total += times(h, w_back_ref[at:at + FFN_PART, :])
    z = x_ref[...].astype(jnp.float32) + (total + vec_ref[7:8, :])
    out_ref[0] = norm(z, vec_ref[4:5, :], vec_ref[5:6, :]).astype(jnp.bfloat16)


def whole(*shape):
    return pl.BlockSpec(shape, lambda b: (0,) * len(shape), pipeline_mode=pl.Buffered(1))


def each(*shape):
    return pl.BlockSpec((1,) + shape, lambda b: (b,) + (0,) * len(shape))


def pieces(weights, sizes):
    out, at = [], 0
    for rows in sizes:
        out.append(pl.BlockSpec((pl.Element(weights.shape[0]), pl.Element(rows), pl.Element(weights.shape[2])),
                                functools.partial(lambda i, b: (0, i, 0), at), pipeline_mode=pl.Buffered(1)))
        at += rows
    return out


def layer(heads, size, batch, spot, got, pos_table, type_row, vecs, b_qkv, b_in, weights, sizes):
    seq = spot.shape[0] // batch
    width = got.shape[1]
    block = pltpu.VMEM((seq, width), jnp.bfloat16)
    return pl.pallas_call(
        functools.partial(layer_kernel, (heads, size)),
        out_shape=jax.ShapeDtypeStruct((batch, seq, width), jnp.bfloat16),
        grid=(batch,),
        in_specs=[each(1, seq), whole(*got.shape), whole(*pos_table.shape), whole(1, width),
                  whole(8, width), whole(1, 3 * width), whole(1, b_in.shape[0])] + pieces(weights, sizes),
        out_specs=each(seq, width),
        scratch_shapes=[pltpu.VMEM((seq, 3 * width), jnp.bfloat16), block, block],
        compiler_params=pltpu.CompilerParams(vmem_limit_bytes=60 << 20),
        cost_estimate=pl.CostEstimate(flops=20 * 10 ** 9, bytes_accessed=15 * 10 ** 6, transcendentals=7 * 10 ** 6))(
            spot.reshape(batch, 1, seq), got, pos_table, type_row[None, :], vecs,
            b_qkv[None, :], b_in[None, :], *([weights] * len(sizes)))


HEAD = 2048
CAPS = ((0, 1, 152), (1, 2, 88), (2, 4, 72), (4, 8, 48), (8, 32, 40))
HOT = 2
EXTRA = 48
PLANE = 8
MESH = pl.DeviceIdType.MESH


def others(n, me, one):
    def body(k, carry):
        one(k, lax.rem(me + k, n))
        return carry

    lax.fori_loop(1, n, body, 0)


def meet(n, me):
    barrier = pltpu.get_barrier_semaphore()
    others(n, me, lambda k, dev: pl.semaphore_signal(barrier, inc=1, device_id=(dev,), device_id_type=MESH))
    pl.semaphore_wait(barrier, n - 1)


def tell_kernel(n, part, msg_ref, table_ref, told_ref, piece_ref, relay_ref, send_sem, recv_sem, out_sem, in_sem, relay_sem,
                own_sem):
    me = lax.axis_index('fsdp')
    planes = n // PLANE
    group = part * planes
    meet(n, me)

    def note(k, dev, slot):
        return pltpu.make_async_remote_copy(msg_ref, told_ref.at[slot], send_sem.at[k], recv_sem.at[slot],
                                            device_id=(dev,), device_id_type=MESH)

    def lend(p):
        return pltpu.make_async_remote_copy(table_ref.at[pl.ds(p * group, group)], relay_ref, out_sem.at[p], relay_sem,
                                            device_id=(p,), device_id_type=MESH)

    def part_of(ref, z, dev):
        return pltpu.make_async_remote_copy(ref.at[pl.ds(z * part, part)], piece_ref, out_sem.at[PLANE + z], in_sem,
                                            device_id=(dev,), device_id_type=MESH)

    def own():
        return pltpu.make_async_copy(table_ref.at[pl.ds(0, part)], piece_ref, own_sem)

    others(n, me, lambda k, dev: note(k, dev, me).start())

    @pl.when(me == 0)
    def _():
        for p in range(PLANE - 1, 0, -1):
            lend(p).start()
        for z in range(1, planes):
            part_of(table_ref, z, z * PLANE).start()
        own().start()

    told_ref[me] = msg_ref[...]

    @pl.when((me > 0) & (me < PLANE))
    def _():
        lend(0).wait_recv()
        for z in range(planes - 1, 0, -1):
            part_of(relay_ref, z, z * PLANE + me).start()
        piece_ref[...] = relay_ref[0:part, :]

    others(n, me, lambda k, dev: note(k, dev, dev).wait_recv())
    others(n, me, lambda k, dev: note(k, dev, me).wait_send())

    @pl.when(me == 0)
    def _():
        own().wait()
        for p in range(1, PLANE):
            lend(p).wait_send()
        for z in range(1, planes):
            part_of(table_ref, z, z * PLANE).wait_send()

    @pl.when((me > 0) & (me < PLANE))
    def _():
        for z in range(1, planes):
            part_of(relay_ref, z, z * PLANE + me).wait_send()

    @pl.when(me >= PLANE)
    def _():
        part_of(relay_ref, 0, me).wait_recv()


def tell(n, msg, table):
    part = HEAD // n
    return pl.pallas_call(
        lambda *refs: tell_kernel(n, part, *refs),
        out_shape=(jax.ShapeDtypeStruct((n,) + msg.shape, msg.dtype),
                   jax.ShapeDtypeStruct((part, table.shape[1]), table.dtype)),
        in_specs=[pl.BlockSpec(memory_space=pltpu.VMEM), pl.BlockSpec(memory_space=pl.ANY)],
        out_specs=(pl.BlockSpec(memory_space=pltpu.VMEM), pl.BlockSpec(memory_space=pltpu.VMEM)),
        scratch_shapes=[pltpu.VMEM((part * (n // PLANE), table.shape[1]), table.dtype),
                        pltpu.SemaphoreType.DMA((n,)), pltpu.SemaphoreType.DMA((n,)),
                        pltpu.SemaphoreType.DMA((PLANE + n // PLANE,)), pltpu.SemaphoreType.DMA, pltpu.SemaphoreType.DMA,
                        pltpu.SemaphoreType.DMA],
        compiler_params=pltpu.CompilerParams(collective_id=0, has_side_effects=True))(msg, table)


def head_spot(n, ids):
    part = HEAD // n
    planes = n // PLANE
    at = ids // part
    return ((at % planes) * PLANE + at // planes) * part + ids % part


def bases():
    out, at = [], 0
    for lo, hi, cap in CAPS:
        out.append(at)
        at += (hi - lo) * cap
    return out, at


def relayed(p, z):
    return z > 0 and 2 <= p and p < PLANE - 1 and (p, z) != (PLANE - 2, 3)


def swap_kernel(n, send_ref, recv_ref, relay_ref, send_sem, recv_sem, lend_sem, pass_sem, own_sem):
    me = lax.axis_index('fsdp')
    planes = n // PLANE
    meet(n, me)
    starts, _ = bases()

    def spot(c, dev):
        lo, _, cap = CAPS[c]
        return recv_ref.at[pl.ds(pl.multiple_of(starts[c] + (dev - lo) * cap, 8), cap)]

    def block(c, dev):
        return send_ref.at[lax.rem(dev, PLANE) * planes + lax.div(dev, PLANE), pl.ds(0, CAPS[c][2])]

    def row(c, k, dev, owner):
        return pltpu.make_async_remote_copy(block(c, dev), spot(c, owner), send_sem.at[k], recv_sem.at[owner],
                                            device_id=(dev,), device_id_type=MESH)

    def held(c, z):
        return relay_ref.at[c, z - 1, pl.ds(0, CAPS[c][2])]

    def lend(c, p, z):
        return pltpu.make_async_remote_copy(send_ref.at[p * planes + z, pl.ds(0, CAPS[c][2])], held(c, z),
                                            send_sem.at[z * PLANE + p], lend_sem.at[c, z - 1], device_id=(p,),
                                            device_id_type=MESH)

    def hand_on(c, z):
        return pltpu.make_async_remote_copy(held(c, z), spot(c, c), pass_sem.at[c, z - 1], recv_sem.at[c],
                                            device_id=(z * PLANE + me,), device_id_type=MESH)

    def own(c):
        return pltpu.make_async_copy(block(c, me), spot(c, me), own_sem)

    def hot_sends(c):
        for z in range(planes - 1, -1, -1):
            for p in range(PLANE):
                dev = z * PLANE + p
                if relayed(p, z):
                    yield lend(c, p, z)
                elif dev != c:
                    yield row(c, dev, jnp.int32(dev), c)

    def relays():
        for p in range(PLANE):
            zs = [z for z in range(planes - 1, 0, -1) if relayed(p, z)]
            if zs:
                yield p, zs

    for c, (lo, hi, cap) in enumerate(CAPS):
        @pl.when((me >= lo) & (me < hi))
        def _(c=c):
            own(c).start()
            if c < HOT:
                for copy in hot_sends(c):
                    copy.start()
            else:
                others(n, me, lambda k, dev: row(c, k, dev, me).start())

    for p, zs in relays():
        @pl.when(me == p)
        def _(zs=zs):
            for z in zs:
                for c in range(HOT):
                    lend(c, 0, z).wait_recv()
                    hand_on(c, z).start()

    for c, (lo, hi, cap) in enumerate(CAPS):
        def one(dev, carry, c=c):
            @pl.when(dev != me)
            def _():
                row(c, 0, dev, dev).wait_recv()

            return carry

        lax.fori_loop(lo, hi, one, 0)

    for c, (lo, hi, cap) in enumerate(CAPS):
        @pl.when((me >= lo) & (me < hi))
        def _(c=c):
            own(c).wait()
            if c < HOT:
                for copy in hot_sends(c):
                    copy.wait_send()
            else:
                others(n, me, lambda k, dev: row(c, k, dev, me).wait_send())

    for p, zs in relays():
        @pl.when(me == p)
        def _(zs=zs):
            for z in zs:
                for c in range(HOT):
                    hand_on(c, z).wait_send()


def swap(n, rows):
    planes = n // PLANE
    most = max(cap for _, _, cap in CAPS[:HOT])
    return pl.pallas_call(
        lambda *refs: swap_kernel(n, *refs),
        out_shape=jax.ShapeDtypeStruct((bases()[1], rows.shape[2]), rows.dtype),
        in_specs=[pl.BlockSpec(memory_space=pl.ANY)], out_specs=pl.BlockSpec(memory_space=pl.ANY),
        scratch_shapes=[pltpu.VMEM((HOT, planes - 1, most, rows.shape[2]), rows.dtype), pltpu.SemaphoreType.DMA((n,)),
                        pltpu.SemaphoreType.DMA((n,)), pltpu.SemaphoreType.DMA((HOT, planes - 1)),
                        pltpu.SemaphoreType.DMA((HOT, planes - 1)), pltpu.SemaphoreType.DMA],
        compiler_params=pltpu.CompilerParams(collective_id=1, has_side_effects=True))(rows)


def solution(mesh):
    def local_step(token_ids, tok_shard, pos_table, type_row, emb_gain, emb_bias, w_qkv, b_qkv, w_out, b_out,
                   ln1_gain, ln1_bias, w_ffn_in, b_ffn_in, w_ffn_out, b_ffn_out, ln2_gain, ln2_bias):
        n_dev = mesh.shape['fsdp']
        me = lax.axis_index('fsdp')
        batch_dev, seq_len = token_ids.shape
        n_tok = batch_dev * seq_len
        shard_rows, width = tok_shard.shape
        num_heads, head_dim = w_out.shape[0], w_out.shape[1]
        ids = token_ids.reshape(n_tok)
        keep = ids != PAD_ID
        asks = keep & (ids >= HEAD)
        owner = jnp.where(asks, ids // shard_rows, n_dev)
        place = jnp.arange(n_tok, dtype=jnp.int32)
        lanes = jnp.arange(128, dtype=jnp.int32)
        mine = (owner[:, None] == lanes[None, :]) & (lanes < n_dev)[None, :]
        before = (place[None, :] < place[:, None]).astype(jnp.bfloat16)
        ranks = jnp.dot(before, mine.astype(jnp.bfloat16), preferred_element_type=jnp.float32)
        count = jnp.sum(mine.astype(jnp.float32), axis=0)
        rank = jnp.sum(jnp.where(mine, ranks, 0.0), axis=1).astype(jnp.int32)
        starts, slots = bases()
        cap, base = jnp.zeros_like(owner), jnp.zeros_like(owner)
        for (lo, hi, c), b in zip(CAPS, starts):
            inside = (owner >= lo) & (owner < hi)
            cap = jnp.where(inside, c, cap)
            base = jnp.where(inside, b + (owner - lo) * c, base)
        fits = rank < cap
        slot = jnp.where(fits, base + rank, -1)
        wide = slots + -slots % 128
        slotted = jnp.sum(jnp.where(slot[:, None] == jnp.arange(wide, dtype=jnp.int32)[None, :],
                                    ids.astype(jnp.float32)[:, None], 0.0), axis=0)

        small = [emb_gain, emb_bias, ln1_gain, ln1_bias, ln2_gain, ln2_bias, b_out, b_ffn_out, b_qkv, b_ffn_in]
        message = jnp.concatenate([slotted, count] + small)
        message = jnp.pad(message, (0, -message.shape[0] % 1024))
        told, piece = tell(n_dev, message.reshape(-1, 128), tok_shard)
        told = told.reshape(n_dev, -1)
        parts = [piece, w_qkv.T, w_out.reshape(num_heads * head_dim, -1).T, w_ffn_in.T, w_ffn_out]
        weights = lax.all_gather(jnp.concatenate(parts, axis=0), 'fsdp', axis=0, tiled=False)

        at = wide + 128
        vectors = []
        for v in small:
            vectors.append(told[:, at:at + v.shape[0]].reshape(-1))
            at += v.shape[0]
        emb_g, emb_b, ln1_g, ln1_b, ln2_g, ln2_b, b_out_f, b_back_f, b_qkv_f, b_in_f = vectors

        my_base = jnp.int32(0)
        for (lo, hi, c), b in zip(CAPS, starts):
            my_base = jnp.where((me >= lo) & (me < hi), b + (me - lo) * c, my_base)
        most = max(c for _, _, c in CAPS)
        wanted = lax.dynamic_slice(told, (0, my_base), (n_dev, most)).astype(jnp.int32) - me * shard_rows
        wanted = jnp.clip(wanted, 0, shard_rows - 1)
        wanted = wanted.reshape(n_dev // PLANE, PLANE, most).transpose(1, 0, 2)
        rows = jnp.take(tok_shard, wanted.reshape(-1), axis=0, mode='clip').reshape(n_dev, most, width)
        got = swap(n_dev, rows)
        spot = jnp.where(ids < HEAD, head_spot(n_dev, ids), HEAD + jnp.maximum(slot, 0))

        caps = jnp.concatenate([jnp.full((hi - lo,), c, jnp.float32) for lo, hi, c in CAPS])
        left = jnp.max(told[:, wide:wide + n_dev] - caps[None, :])
        rounds = (jnp.maximum(left, 0.0).astype(jnp.int32) + EXTRA - 1) // EXTRA

        def again(state):
            r, rows_now = state
            extra = rank - cap - r * EXTRA
            live = asks & (extra >= 0) & (extra < EXTRA)
            at_slot = jnp.where(live, owner * EXTRA + extra, n_dev * EXTRA)
            ask = jnp.zeros((n_dev * EXTRA + 1,), jnp.int32).at[at_slot].set(ids)[:-1]
            asked = lax.all_to_all(ask.reshape(n_dev, EXTRA), 'fsdp', 0, 0, tiled=True)
            asked = jnp.clip(asked - me * shard_rows, 0, shard_rows - 1)
            found = jnp.take(tok_shard, asked.reshape(-1), axis=0, mode='clip').reshape(n_dev, EXTRA, width)
            back = lax.all_to_all(found, 'fsdp', 0, 0, tiled=True).reshape(n_dev * EXTRA, width)
            new = jnp.take(back, jnp.where(live, at_slot, 0), axis=0, mode='clip')
            return r + 1, jnp.where(live[:, None], new, rows_now)

        def slow(got_now, spot_now):
            head = weights[:, :piece.shape[0]].reshape(HEAD, width)
            rows_now = jnp.take(jnp.concatenate([head, got_now], axis=0), spot_now, axis=0, mode='clip')
            _, rows_now = lax.while_loop(lambda state: state[0] < rounds, again, (jnp.int32(0), rows_now))
            return jnp.pad(rows_now, ((0, slots - n_tok), (0, 0))), jnp.where(ids == PAD_ID, spot_now, HEAD + place)

        got, spot = lax.cond(rounds > 0, slow, lambda g, p: (g, p), got, spot)
        vecs = jnp.stack([emb_g, emb_b, ln1_g, ln1_b, ln2_g, ln2_b, b_out_f, b_back_f])
        return layer(num_heads, head_dim, batch_dev, spot, got, pos_table, type_row, vecs, b_qkv_f, b_in_f, weights,
                     [w.shape[0] for w in parts])

    vec_spec = P('fsdp')
    in_specs = (P('fsdp', None), P('fsdp', None), P(None, None), P(None), vec_spec, vec_spec,
                P(None, 'fsdp'), vec_spec, P(None, None, 'fsdp'), vec_spec, vec_spec, vec_spec,
                P(None, 'fsdp'), vec_spec, P('fsdp', None), vec_spec, vec_spec, vec_spec)
    return jax.shard_map(local_step, mesh=mesh, in_specs=in_specs, out_specs=P('fsdp', None, None), check_vma=False)
```

```python
import functools

import jax
import jax.numpy as jnp
from jax import lax
from jax.experimental import pallas as pl
from jax.experimental.pallas import tpu as pltpu
from jax.sharding import PartitionSpec as P

PAD_ID = 1
LN_EPS = 1e-5


SQRT_HALF = 0.5 ** 0.5
LOG2_E = 1.4426950408889634
FFN_PART = 768


def norm(z, gain, shift):
    centered = z - jnp.mean(z, axis=-1, keepdims=True)
    var = jnp.mean(centered * centered, axis=-1, keepdims=True)
    return centered * lax.rsqrt(var + LN_EPS) * gain + shift


def times(a, b):
    return jnp.dot(a, b, preferred_element_type=jnp.float32)


def times_t(a, b):
    return lax.dot_general(a, b, (((1,), (1,)), ((), ())), preferred_element_type=jnp.float32)


def flat(ref):
    return ref.reshape(ref.shape[0] * ref.shape[1], ref.shape[2])


def layer_kernel(dims, spot_row_ref, got_ref, pos_ref, type_ref, vec_ref, b_qkv_ref, b_in_ref, head_ref, w_qkv_ref, w_out_ref,
                 w_in_ref, w_back_ref, out_ref, qkv_ref, ctx_ref, x_ref):
    heads, size = dims
    seq, width = out_ref.shape[1:]
    head_ref, w_qkv_ref, w_out_ref, w_in_ref, w_back_ref = (
        flat(r) for r in (head_ref, w_qkv_ref, w_out_ref, w_in_ref, w_back_ref))
    spot = jnp.transpose(jnp.broadcast_to(spot_row_ref[0].astype(jnp.float32), (8, seq)))[:, 0:1].astype(jnp.int32)
    total = jnp.zeros((seq, width), jnp.float32)
    step = 256
    for ref, first in ((head_ref, 0), (got_ref, head_ref.shape[0])):
        for at in range(0, ref.shape[0], step):
            hit = spot == lax.broadcasted_iota(jnp.int32, (seq, step), 1) + (first + at)
            total += times(jnp.where(hit, 1.0, 0.0).astype(jnp.bfloat16), ref[at:at + step, :])
    pos = jnp.where(spot != PAD_ID, pos_ref[2:2 + seq, :].astype(jnp.float32), pos_ref[1:2, :].astype(jnp.float32))
    embedded = total + pos + type_ref[...].astype(jnp.float32)
    x_ref[...] = norm(embedded, vec_ref[0:1, :], vec_ref[1:2, :]).astype(jnp.bfloat16)

    part = 2 * width // 2
    for at in range(0, 3 * width, part):
        qkv_ref[:, at:at + part] = (times_t(x_ref[...], w_qkv_ref[at:at + part, :])
                                    + b_qkv_ref[:, at:at + part]).astype(jnp.bfloat16)

    masked = jnp.where(spot_row_ref[0] != PAD_ID, 0.0, -1e30)
    low = lax.broadcasted_iota(jnp.int32, (1, 2 * size), 1) < size
    for pair in range(heads // 2):
        at = pair * 2 * size
        q = qkv_ref[:, at:at + 2 * size]
        k = qkv_ref[:, width + at:width + at + 2 * size]
        v = qkv_ref[:, 2 * width + at:2 * width + at + 2 * size]
        zero = jnp.zeros_like(q)
        mixed = []
        for mine in (low, ~low):
            s = times_t(jnp.where(mine, q, zero), k) + masked
            p = jnp.exp2((s - jnp.max(s, axis=-1, keepdims=True)) * (size ** -0.5 * LOG2_E))
            p = p * (1.0 / jnp.sum(p, axis=-1, keepdims=True))
            mixed.append(times(p.astype(jnp.bfloat16), v))
        ctx_ref[:, at:at + 2 * size] = jnp.where(low, mixed[0], mixed[1]).astype(jnp.bfloat16)

    a = (times_t(ctx_ref[...], w_out_ref[...]) + vec_ref[6:7, :]).astype(jnp.bfloat16)
    z = x_ref[...].astype(jnp.float32) + a.astype(jnp.float32)
    x_ref[...] = norm(z, vec_ref[2:3, :], vec_ref[3:4, :]).astype(jnp.bfloat16)

    total = jnp.zeros((seq, width), jnp.float32)
    for at in range(0, b_in_ref.shape[1], FFN_PART):
        h = times_t(x_ref[...], w_in_ref[at:at + FFN_PART, :]) + b_in_ref[:, at:at + FFN_PART]
        h = (0.5 * h * (1.0 + lax.erf(h * SQRT_HALF))).astype(jnp.bfloat16)
        total += times(h, w_back_ref[at:at + FFN_PART, :])
    z = x_ref[...].astype(jnp.float32) + (total + vec_ref[7:8, :])
    out_ref[0] = norm(z, vec_ref[4:5, :], vec_ref[5:6, :]).astype(jnp.bfloat16)


def whole(*shape):
    return pl.BlockSpec(shape, lambda b: (0,) * len(shape), pipeline_mode=pl.Buffered(1))


def each(*shape):
    return pl.BlockSpec((1,) + shape, lambda b: (b,) + (0,) * len(shape))


def pieces(weights, sizes):
    out, at = [], 0
    for rows in sizes:
        out.append(pl.BlockSpec((pl.Element(weights.shape[0]), pl.Element(rows), pl.Element(weights.shape[2])),
                                functools.partial(lambda i, b: (0, i, 0), at), pipeline_mode=pl.Buffered(1)))
        at += rows
    return out


def layer(heads, size, batch, spot, got, pos_table, type_row, vecs, b_qkv, b_in, weights, sizes):
    seq = spot.shape[0] // batch
    width = got.shape[1]
    block = pltpu.VMEM((seq, width), jnp.bfloat16)
    return pl.pallas_call(
        functools.partial(layer_kernel, (heads, size)),
        out_shape=jax.ShapeDtypeStruct((batch, seq, width), jnp.bfloat16),
        grid=(batch,),
        in_specs=[each(1, seq), whole(*got.shape), whole(*pos_table.shape), whole(1, width),
                  whole(8, width), whole(1, 3 * width), whole(1, b_in.shape[0])] + pieces(weights, sizes),
        out_specs=each(seq, width),
        scratch_shapes=[pltpu.VMEM((seq, 3 * width), jnp.bfloat16), block, block],
        compiler_params=pltpu.CompilerParams(vmem_limit_bytes=60 << 20),
        cost_estimate=pl.CostEstimate(flops=20 * 10 ** 9, bytes_accessed=15 * 10 ** 6, transcendentals=7 * 10 ** 6))(
            spot.reshape(batch, 1, seq), got, pos_table, type_row[None, :], vecs,
            b_qkv[None, :], b_in[None, :], *([weights] * len(sizes)))


HEAD = 2048
CAPS = ((0, 1, 152), (1, 2, 88), (2, 4, 72), (4, 8, 48), (8, 32, 40))
HOT = 2
EXTRA = 48
PLANE = 8
MESH = pl.DeviceIdType.MESH


def others(n, me, one):
    def body(k, carry):
        one(k, lax.rem(me + k, n))
        return carry

    lax.fori_loop(1, n, body, 0)


def meet(n, me):
    barrier = pltpu.get_barrier_semaphore()
    others(n, me, lambda k, dev: pl.semaphore_signal(barrier, inc=1, device_id=(dev,), device_id_type=MESH))
    pl.semaphore_wait(barrier, n - 1)


def tell_kernel(n, part, msg_ref, table_ref, told_ref, piece_ref, relay_ref, send_sem, recv_sem, out_sem, in_sem, relay_sem,
                own_sem):
    me = lax.axis_index('fsdp')
    planes = n // PLANE
    group = part * planes
    meet(n, me)

    def note(k, dev, slot):
        return pltpu.make_async_remote_copy(msg_ref, told_ref.at[slot], send_sem.at[k], recv_sem.at[slot],
                                            device_id=(dev,), device_id_type=MESH)

    def lend(p):
        return pltpu.make_async_remote_copy(table_ref.at[pl.ds(p * group, group)], relay_ref, out_sem.at[p], relay_sem,
                                            device_id=(p,), device_id_type=MESH)

    def part_of(ref, z, dev):
        return pltpu.make_async_remote_copy(ref.at[pl.ds(z * part, part)], piece_ref, out_sem.at[PLANE + z], in_sem,
                                            device_id=(dev,), device_id_type=MESH)

    def own():
        return pltpu.make_async_copy(table_ref.at[pl.ds(0, part)], piece_ref, own_sem)

    others(n, me, lambda k, dev: note(k, dev, me).start())

    @pl.when(me == 0)
    def _():
        for p in range(PLANE - 1, 0, -1):
            lend(p).start()
        for z in range(1, planes):
            part_of(table_ref, z, z * PLANE).start()
        own().start()

    told_ref[me] = msg_ref[...]

    @pl.when((me > 0) & (me < PLANE))
    def _():
        lend(0).wait_recv()
        for z in range(planes - 1, 0, -1):
            part_of(relay_ref, z, z * PLANE + me).start()
        piece_ref[...] = relay_ref[0:part, :]

    others(n, me, lambda k, dev: note(k, dev, dev).wait_recv())
    others(n, me, lambda k, dev: note(k, dev, me).wait_send())

    @pl.when(me == 0)
    def _():
        own().wait()
        for p in range(1, PLANE):
            lend(p).wait_send()
        for z in range(1, planes):
            part_of(table_ref, z, z * PLANE).wait_send()

    @pl.when((me > 0) & (me < PLANE))
    def _():
        for z in range(1, planes):
            part_of(relay_ref, z, z * PLANE + me).wait_send()

    @pl.when(me >= PLANE)
    def _():
        part_of(relay_ref, 0, me).wait_recv()


def tell(n, msg, table):
    part = HEAD // n
    return pl.pallas_call(
        lambda *refs: tell_kernel(n, part, *refs),
        out_shape=(jax.ShapeDtypeStruct((n,) + msg.shape, msg.dtype),
                   jax.ShapeDtypeStruct((part, table.shape[1]), table.dtype)),
        in_specs=[pl.BlockSpec(memory_space=pltpu.VMEM), pl.BlockSpec(memory_space=pl.ANY)],
        out_specs=(pl.BlockSpec(memory_space=pltpu.VMEM), pl.BlockSpec(memory_space=pltpu.VMEM)),
        scratch_shapes=[pltpu.VMEM((part * (n // PLANE), table.shape[1]), table.dtype),
                        pltpu.SemaphoreType.DMA((n,)), pltpu.SemaphoreType.DMA((n,)),
                        pltpu.SemaphoreType.DMA((PLANE + n // PLANE,)), pltpu.SemaphoreType.DMA, pltpu.SemaphoreType.DMA,
                        pltpu.SemaphoreType.DMA],
        compiler_params=pltpu.CompilerParams(collective_id=0, has_side_effects=True))(msg, table)


def head_spot(n, ids):
    part = HEAD // n
    planes = n // PLANE
    at = ids // part
    return ((at % planes) * PLANE + at // planes) * part + ids % part


def bases():
    out, at = [], 0
    for lo, hi, cap in CAPS:
        out.append(at)
        at += (hi - lo) * cap
    return out, at


def relayed(p, z):
    return z > 0 and p >= PLANE // 2


def swap_kernel(n, send_ref, recv_ref, relay_ref, send_sem, recv_sem, lend_sem, pass_sem, own_sem):
    me = lax.axis_index('fsdp')
    planes = n // PLANE
    meet(n, me)
    starts, _ = bases()

    def spot(c, dev):
        lo, _, cap = CAPS[c]
        return recv_ref.at[pl.ds(pl.multiple_of(starts[c] + (dev - lo) * cap, 8), cap)]

    def block(c, dev):
        return send_ref.at[lax.rem(dev, PLANE) * planes + lax.div(dev, PLANE), pl.ds(0, CAPS[c][2])]

    def row(c, k, dev, owner):
        return pltpu.make_async_remote_copy(block(c, dev), spot(c, owner), send_sem.at[k], recv_sem.at[owner],
                                            device_id=(dev,), device_id_type=MESH)

    def held(c, z):
        return relay_ref.at[c, z - 1, pl.ds(0, CAPS[c][2])]

    def lend(c, p, z):
        return pltpu.make_async_remote_copy(send_ref.at[p * planes + z, pl.ds(0, CAPS[c][2])], held(c, z),
                                            send_sem.at[z * PLANE + p], lend_sem.at[c, z - 1], device_id=(p,),
                                            device_id_type=MESH)

    def hand_on(c, z):
        return pltpu.make_async_remote_copy(held(c, z), spot(c, c), pass_sem.at[c, z - 1], recv_sem.at[c],
                                            device_id=(z * PLANE + me,), device_id_type=MESH)

    def own(c):
        return pltpu.make_async_copy(block(c, me), spot(c, me), own_sem)

    def hot_sends(c):
        for z in range(planes - 1, -1, -1):
            for p in range(PLANE):
                dev = z * PLANE + p
                if relayed(p, z):
                    yield lend(c, p, z)
                elif dev != c:
                    yield row(c, dev, jnp.int32(dev), c)

    def relays():
        for p in range(PLANE):
            zs = [z for z in range(planes - 1, 0, -1) if relayed(p, z)]
            if zs:
                yield p, zs

    for c, (lo, hi, cap) in enumerate(CAPS):
        @pl.when((me >= lo) & (me < hi))
        def _(c=c):
            own(c).start()
            if c < HOT:
                for copy in hot_sends(c):
                    copy.start()
            else:
                others(n, me, lambda k, dev: row(c, k, dev, me).start())

    for p, zs in relays():
        @pl.when(me == p)
        def _(zs=zs):
            for z in zs:
                for c in range(HOT):
                    lend(c, 0, z).wait_recv()
                    hand_on(c, z).start()

    for c, (lo, hi, cap) in enumerate(CAPS):
        def one(dev, carry, c=c):
            @pl.when(dev != me)
            def _():
                row(c, 0, dev, dev).wait_recv()

            return carry

        lax.fori_loop(lo, hi, one, 0)

    for c, (lo, hi, cap) in enumerate(CAPS):
        @pl.when((me >= lo) & (me < hi))
        def _(c=c):
            own(c).wait()
            if c < HOT:
                for copy in hot_sends(c):
                    copy.wait_send()
            else:
                others(n, me, lambda k, dev: row(c, k, dev, me).wait_send())

    for p, zs in relays():
        @pl.when(me == p)
        def _(zs=zs):
            for z in zs:
                for c in range(HOT):
                    hand_on(c, z).wait_send()


def swap(n, rows):
    planes = n // PLANE
    most = max(cap for _, _, cap in CAPS[:HOT])
    return pl.pallas_call(
        lambda *refs: swap_kernel(n, *refs),
        out_shape=jax.ShapeDtypeStruct((bases()[1], rows.shape[2]), rows.dtype),
        in_specs=[pl.BlockSpec(memory_space=pl.ANY)], out_specs=pl.BlockSpec(memory_space=pl.ANY),
        scratch_shapes=[pltpu.VMEM((HOT, planes - 1, most, rows.shape[2]), rows.dtype), pltpu.SemaphoreType.DMA((n,)),
                        pltpu.SemaphoreType.DMA((n,)), pltpu.SemaphoreType.DMA((HOT, planes - 1)),
                        pltpu.SemaphoreType.DMA((HOT, planes - 1)), pltpu.SemaphoreType.DMA],
        compiler_params=pltpu.CompilerParams(collective_id=1, has_side_effects=True))(rows)


def solution(mesh):
    def local_step(token_ids, tok_shard, pos_table, type_row, emb_gain, emb_bias, w_qkv, b_qkv, w_out, b_out,
                   ln1_gain, ln1_bias, w_ffn_in, b_ffn_in, w_ffn_out, b_ffn_out, ln2_gain, ln2_bias):
        n_dev = mesh.shape['fsdp']
        me = lax.axis_index('fsdp')
        batch_dev, seq_len = token_ids.shape
        n_tok = batch_dev * seq_len
        shard_rows, width = tok_shard.shape
        num_heads, head_dim = w_out.shape[0], w_out.shape[1]
        ids = token_ids.reshape(n_tok)
        keep = ids != PAD_ID
        asks = keep & (ids >= HEAD)
        owner = jnp.where(asks, ids // shard_rows, n_dev)
        place = jnp.arange(n_tok, dtype=jnp.int32)
        lanes = jnp.arange(128, dtype=jnp.int32)
        mine = (owner[:, None] == lanes[None, :]) & (lanes < n_dev)[None, :]
        before = (place[None, :] < place[:, None]).astype(jnp.bfloat16)
        ranks = jnp.dot(before, mine.astype(jnp.bfloat16), preferred_element_type=jnp.float32)
        count = jnp.sum(mine.astype(jnp.float32), axis=0)
        rank = jnp.sum(jnp.where(mine, ranks, 0.0), axis=1).astype(jnp.int32)
        starts, slots = bases()
        cap, base = jnp.zeros_like(owner), jnp.zeros_like(owner)
        for (lo, hi, c), b in zip(CAPS, starts):
            inside = (owner >= lo) & (owner < hi)
            cap = jnp.where(inside, c, cap)
            base = jnp.where(inside, b + (owner - lo) * c, base)
        fits = rank < cap
        slot = jnp.where(fits, base + rank, -1)
        wide = slots + -slots % 128
        slotted = jnp.sum(jnp.where(slot[:, None] == jnp.arange(wide, dtype=jnp.int32)[None, :],
                                    ids.astype(jnp.float32)[:, None], 0.0), axis=0)

        small = [emb_gain, emb_bias, ln1_gain, ln1_bias, ln2_gain, ln2_bias, b_out, b_ffn_out, b_qkv, b_ffn_in]
        message = jnp.concatenate([slotted, count] + small)
        message = jnp.pad(message, (0, -message.shape[0] % 1024))
        told, piece = tell(n_dev, message.reshape(-1, 128), tok_shard)
        told = told.reshape(n_dev, -1)
        parts = [piece, w_qkv.T, w_out.reshape(num_heads * head_dim, -1).T, w_ffn_in.T, w_ffn_out]
        weights = lax.all_gather(jnp.concatenate(parts, axis=0), 'fsdp', axis=0, tiled=False)

        at = wide + 128
        vectors = []
        for v in small:
            vectors.append(told[:, at:at + v.shape[0]].reshape(-1))
            at += v.shape[0]
        emb_g, emb_b, ln1_g, ln1_b, ln2_g, ln2_b, b_out_f, b_back_f, b_qkv_f, b_in_f = vectors

        my_base = jnp.int32(0)
        for (lo, hi, c), b in zip(CAPS, starts):
            my_base = jnp.where((me >= lo) & (me < hi), b + (me - lo) * c, my_base)
        most = max(c for _, _, c in CAPS)
        wanted = lax.dynamic_slice(told, (0, my_base), (n_dev, most)).astype(jnp.int32) - me * shard_rows
        wanted = jnp.clip(wanted, 0, shard_rows - 1)
        wanted = wanted.reshape(n_dev // PLANE, PLANE, most).transpose(1, 0, 2)
        rows = jnp.take(tok_shard, wanted.reshape(-1), axis=0, mode='clip').reshape(n_dev, most, width)
        got = swap(n_dev, rows)
        spot = jnp.where(ids < HEAD, head_spot(n_dev, ids), HEAD + jnp.maximum(slot, 0))

        caps = jnp.concatenate([jnp.full((hi - lo,), c, jnp.float32) for lo, hi, c in CAPS])
        left = jnp.max(told[:, wide:wide + n_dev] - caps[None, :])
        rounds = (jnp.maximum(left, 0.0).astype(jnp.int32) + EXTRA - 1) // EXTRA

        def again(state):
            r, rows_now = state
            extra = rank - cap - r * EXTRA
            live = asks & (extra >= 0) & (extra < EXTRA)
            at_slot = jnp.where(live, owner * EXTRA + extra, n_dev * EXTRA)
            ask = jnp.zeros((n_dev * EXTRA + 1,), jnp.int32).at[at_slot].set(ids)[:-1]
            asked = lax.all_to_all(ask.reshape(n_dev, EXTRA), 'fsdp', 0, 0, tiled=True)
            asked = jnp.clip(asked - me * shard_rows, 0, shard_rows - 1)
            found = jnp.take(tok_shard, asked.reshape(-1), axis=0, mode='clip').reshape(n_dev, EXTRA, width)
            back = lax.all_to_all(found, 'fsdp', 0, 0, tiled=True).reshape(n_dev * EXTRA, width)
            new = jnp.take(back, jnp.where(live, at_slot, 0), axis=0, mode='clip')
            return r + 1, jnp.where(live[:, None], new, rows_now)

        def slow(got_now, spot_now):
            head = weights[:, :piece.shape[0]].reshape(HEAD, width)
            rows_now = jnp.take(jnp.concatenate([head, got_now], axis=0), spot_now, axis=0, mode='clip')
            _, rows_now = lax.while_loop(lambda state: state[0] < rounds, again, (jnp.int32(0), rows_now))
            return jnp.pad(rows_now, ((0, slots - n_tok), (0, 0))), jnp.where(ids == PAD_ID, spot_now, HEAD + place)

        got, spot = lax.cond(rounds > 0, slow, lambda g, p: (g, p), got, spot)
        vecs = jnp.stack([emb_g, emb_b, ln1_g, ln1_b, ln2_g, ln2_b, b_out_f, b_back_f])
        return layer(num_heads, head_dim, batch_dev, spot, got, pos_table, type_row, vecs, b_qkv_f, b_in_f, weights,
                     [w.shape[0] for w in parts])

    vec_spec = P('fsdp')
    in_specs = (P('fsdp', None), P('fsdp', None), P(None, None), P(None), vec_spec, vec_spec,
                P(None, 'fsdp'), vec_spec, P(None, None, 'fsdp'), vec_spec, vec_spec, vec_spec,
                P(None, 'fsdp'), vec_spec, P('fsdp', None), vec_spec, vec_spec, vec_spec)
    return jax.shard_map(local_step, mesh=mesh, in_specs=in_specs, out_specs=P('fsdp', None, None), check_vma=False)
```

```python
import functools

import jax
import jax.numpy as jnp
from jax import lax
from jax.experimental import pallas as pl
from jax.experimental.pallas import tpu as pltpu
from jax.sharding import PartitionSpec as P

PAD_ID = 1
LN_EPS = 1e-5


SQRT_HALF = 0.5 ** 0.5
LOG2_E = 1.4426950408889634
FFN_PART = 768


def norm(z, gain, shift):
    centered = z - jnp.mean(z, axis=-1, keepdims=True)
    var = jnp.mean(centered * centered, axis=-1, keepdims=True)
    return centered * lax.rsqrt(var + LN_EPS) * gain + shift


def times(a, b):
    return jnp.dot(a, b, preferred_element_type=jnp.float32)


def times_t(a, b):
    return lax.dot_general(a, b, (((1,), (1,)), ((), ())), preferred_element_type=jnp.float32)


def flat(ref):
    return ref.reshape(ref.shape[0] * ref.shape[1], ref.shape[2])


def layer_kernel(dims, spot_row_ref, rows_ref, pos_ref, type_ref, vec_ref, b_qkv_ref, b_in_ref, head_ref, w_qkv_ref, w_out_ref,
                 w_in_ref, w_back_ref, out_ref, qkv_ref, ctx_ref, x_ref):
    heads, size = dims
    seq, width = out_ref.shape[1:]
    head_ref, w_qkv_ref, w_out_ref, w_in_ref, w_back_ref = (
        flat(r) for r in (head_ref, w_qkv_ref, w_out_ref, w_in_ref, w_back_ref))
    spot = jnp.transpose(jnp.broadcast_to(spot_row_ref[0].astype(jnp.float32), (8, seq)))[:, 0:1].astype(jnp.int32)
    total = jnp.where(spot < head_ref.shape[0], 0.0, rows_ref[0].astype(jnp.float32))
    step = 256
    for at in range(0, head_ref.shape[0], step):
        hit = spot == lax.broadcasted_iota(jnp.int32, (seq, step), 1) + at
        total += times(jnp.where(hit, 1.0, 0.0).astype(jnp.bfloat16), head_ref[at:at + step, :])
    pos = jnp.where(spot != PAD_ID, pos_ref[2:2 + seq, :].astype(jnp.float32), pos_ref[1:2, :].astype(jnp.float32))
    embedded = total + pos + type_ref[...].astype(jnp.float32)
    x_ref[...] = norm(embedded, vec_ref[0:1, :], vec_ref[1:2, :]).astype(jnp.bfloat16)

    part = 2 * width // 2
    for at in range(0, 3 * width, part):
        qkv_ref[:, at:at + part] = (times_t(x_ref[...], w_qkv_ref[at:at + part, :])
                                    + b_qkv_ref[:, at:at + part]).astype(jnp.bfloat16)

    masked = jnp.where(spot_row_ref[0] != PAD_ID, 0.0, -1e30)
    low = lax.broadcasted_iota(jnp.int32, (1, 2 * size), 1) < size
    for pair in range(heads // 2):
        at = pair * 2 * size
        q = qkv_ref[:, at:at + 2 * size]
        k = qkv_ref[:, width + at:width + at + 2 * size]
        v = qkv_ref[:, 2 * width + at:2 * width + at + 2 * size]
        zero = jnp.zeros_like(q)
        mixed = []
        for mine in (low, ~low):
            s = times_t(jnp.where(mine, q, zero), k) + masked
            p = jnp.exp2((s - jnp.max(s, axis=-1, keepdims=True)) * (size ** -0.5 * LOG2_E))
            p = p * (1.0 / jnp.sum(p, axis=-1, keepdims=True))
            mixed.append(times(p.astype(jnp.bfloat16), v))
        ctx_ref[:, at:at + 2 * size] = jnp.where(low, mixed[0], mixed[1]).astype(jnp.bfloat16)

    a = (times_t(ctx_ref[...], w_out_ref[...]) + vec_ref[6:7, :]).astype(jnp.bfloat16)
    z = x_ref[...].astype(jnp.float32) + a.astype(jnp.float32)
    x_ref[...] = norm(z, vec_ref[2:3, :], vec_ref[3:4, :]).astype(jnp.bfloat16)

    total = jnp.zeros((seq, width), jnp.float32)
    for at in range(0, b_in_ref.shape[1], FFN_PART):
        h = times_t(x_ref[...], w_in_ref[at:at + FFN_PART, :]) + b_in_ref[:, at:at + FFN_PART]
        h = (0.5 * h * (1.0 + lax.erf(h * SQRT_HALF))).astype(jnp.bfloat16)
        total += times(h, w_back_ref[at:at + FFN_PART, :])
    z = x_ref[...].astype(jnp.float32) + (total + vec_ref[7:8, :])
    out_ref[0] = norm(z, vec_ref[4:5, :], vec_ref[5:6, :]).astype(jnp.bfloat16)


def whole(*shape):
    return pl.BlockSpec(shape, lambda b: (0,) * len(shape), pipeline_mode=pl.Buffered(1))


def each(*shape):
    return pl.BlockSpec((1,) + shape, lambda b: (b,) + (0,) * len(shape))


def pieces(weights, sizes):
    out, at = [], 0
    for rows in sizes:
        out.append(pl.BlockSpec((pl.Element(weights.shape[0]), pl.Element(rows), pl.Element(weights.shape[2])),
                                functools.partial(lambda i, b: (0, i, 0), at), pipeline_mode=pl.Buffered(1)))
        at += rows
    return out


def layer(heads, size, batch, spot, rows, pos_table, type_row, vecs, b_qkv, b_in, weights, sizes):
    seq = spot.shape[0] // batch
    width = rows.shape[1]
    block = pltpu.VMEM((seq, width), jnp.bfloat16)
    return pl.pallas_call(
        functools.partial(layer_kernel, (heads, size)),
        out_shape=jax.ShapeDtypeStruct((batch, seq, width), jnp.bfloat16),
        grid=(batch,),
        in_specs=[each(1, seq), each(seq, width), whole(*pos_table.shape), whole(1, width),
                  whole(8, width), whole(1, 3 * width), whole(1, b_in.shape[0])] + pieces(weights, sizes),
        out_specs=each(seq, width),
        scratch_shapes=[pltpu.VMEM((seq, 3 * width), jnp.bfloat16), block, block],
        compiler_params=pltpu.CompilerParams(vmem_limit_bytes=60 << 20),
        cost_estimate=pl.CostEstimate(flops=20 * 10 ** 9, bytes_accessed=15 * 10 ** 6, transcendentals=7 * 10 ** 6))(
            spot.reshape(batch, 1, seq), rows.reshape(batch, seq, width), pos_table, type_row[None, :], vecs,
            b_qkv[None, :], b_in[None, :], *([weights] * len(sizes)))


HEAD = 2048
CAPS = ((0, 1, 152), (1, 2, 88), (2, 4, 72), (4, 8, 48), (8, 32, 40))
HOT = 2
EXTRA = 48
PLANE = 8
MESH = pl.DeviceIdType.MESH


def others(n, me, one):
    def body(k, carry):
        one(k, lax.rem(me + k, n))
        return carry

    lax.fori_loop(1, n, body, 0)


def meet(n, me):
    barrier = pltpu.get_barrier_semaphore()
    others(n, me, lambda k, dev: pl.semaphore_signal(barrier, inc=1, device_id=(dev,), device_id_type=MESH))
    pl.semaphore_wait(barrier, n - 1)


def tell_kernel(n, part, msg_ref, table_ref, told_ref, piece_ref, relay_ref, send_sem, recv_sem, out_sem, in_sem, relay_sem,
                own_sem):
    me = lax.axis_index('fsdp')
    planes = n // PLANE
    group = part * planes
    meet(n, me)

    def note(k, dev, slot):
        return pltpu.make_async_remote_copy(msg_ref, told_ref.at[slot], send_sem.at[k], recv_sem.at[slot],
                                            device_id=(dev,), device_id_type=MESH)

    def lend(p):
        return pltpu.make_async_remote_copy(table_ref.at[pl.ds(p * group, group)], relay_ref, out_sem.at[p], relay_sem,
                                            device_id=(p,), device_id_type=MESH)

    def part_of(ref, z, dev):
        return pltpu.make_async_remote_copy(ref.at[pl.ds(z * part, part)], piece_ref, out_sem.at[PLANE + z], in_sem,
                                            device_id=(dev,), device_id_type=MESH)

    def own():
        return pltpu.make_async_copy(table_ref.at[pl.ds(0, part)], piece_ref, own_sem)

    others(n, me, lambda k, dev: note(k, dev, me).start())

    @pl.when(me == 0)
    def _():
        for p in range(PLANE - 1, 0, -1):
            lend(p).start()
        for z in range(1, planes):
            part_of(table_ref, z, z * PLANE).start()
        own().start()

    told_ref[me] = msg_ref[...]

    @pl.when((me > 0) & (me < PLANE))
    def _():
        lend(0).wait_recv()
        for z in range(planes - 1, 0, -1):
            part_of(relay_ref, z, z * PLANE + me).start()
        piece_ref[...] = relay_ref[0:part, :]

    others(n, me, lambda k, dev: note(k, dev, dev).wait_recv())
    others(n, me, lambda k, dev: note(k, dev, me).wait_send())

    @pl.when(me == 0)
    def _():
        own().wait()
        for p in range(1, PLANE):
            lend(p).wait_send()
        for z in range(1, planes):
            part_of(table_ref, z, z * PLANE).wait_send()

    @pl.when((me > 0) & (me < PLANE))
    def _():
        for z in range(1, planes):
            part_of(relay_ref, z, z * PLANE + me).wait_send()

    @pl.when(me >= PLANE)
    def _():
        part_of(relay_ref, 0, me).wait_recv()


def tell(n, msg, table):
    part = HEAD // n
    return pl.pallas_call(
        lambda *refs: tell_kernel(n, part, *refs),
        out_shape=(jax.ShapeDtypeStruct((n,) + msg.shape, msg.dtype),
                   jax.ShapeDtypeStruct((part, table.shape[1]), table.dtype)),
        in_specs=[pl.BlockSpec(memory_space=pltpu.VMEM), pl.BlockSpec(memory_space=pl.ANY)],
        out_specs=(pl.BlockSpec(memory_space=pltpu.VMEM), pl.BlockSpec(memory_space=pltpu.VMEM)),
        scratch_shapes=[pltpu.VMEM((part * (n // PLANE), table.shape[1]), table.dtype),
                        pltpu.SemaphoreType.DMA((n,)), pltpu.SemaphoreType.DMA((n,)),
                        pltpu.SemaphoreType.DMA((PLANE + n // PLANE,)), pltpu.SemaphoreType.DMA, pltpu.SemaphoreType.DMA,
                        pltpu.SemaphoreType.DMA],
        compiler_params=pltpu.CompilerParams(collective_id=0, has_side_effects=True))(msg, table)


def head_spot(n, ids):
    part = HEAD // n
    planes = n // PLANE
    at = ids // part
    return ((at % planes) * PLANE + at // planes) * part + ids % part


def bases():
    out, at = [], 0
    for lo, hi, cap in CAPS:
        out.append(at)
        at += (hi - lo) * cap
    return out, at


def relayed(p, z):
    return z > 0 and p >= PLANE // 2


def swap_kernel(n, send_ref, recv_ref, relay_ref, send_sem, recv_sem, lend_sem, pass_sem, own_sem):
    me = lax.axis_index('fsdp')
    planes = n // PLANE
    meet(n, me)
    starts, _ = bases()

    def spot(c, dev):
        lo, _, cap = CAPS[c]
        return recv_ref.at[pl.ds(pl.multiple_of(starts[c] + (dev - lo) * cap, 8), cap)]

    def block(c, dev):
        return send_ref.at[lax.rem(dev, PLANE) * planes + lax.div(dev, PLANE), pl.ds(0, CAPS[c][2])]

    def row(c, k, dev, owner):
        return pltpu.make_async_remote_copy(block(c, dev), spot(c, owner), send_sem.at[k], recv_sem.at[owner],
                                            device_id=(dev,), device_id_type=MESH)

    def held(c, z):
        return relay_ref.at[c, z - 1, pl.ds(0, CAPS[c][2])]

    def lend(c, p, z):
        return pltpu.make_async_remote_copy(send_ref.at[p * planes + z, pl.ds(0, CAPS[c][2])], held(c, z),
                                            send_sem.at[z * PLANE + p], lend_sem.at[c, z - 1], device_id=(p,),
                                            device_id_type=MESH)

    def hand_on(c, z):
        return pltpu.make_async_remote_copy(held(c, z), spot(c, c), pass_sem.at[c, z - 1], recv_sem.at[c],
                                            device_id=(z * PLANE + me,), device_id_type=MESH)

    def own(c):
        return pltpu.make_async_copy(block(c, me), spot(c, me), own_sem)

    def hot_sends(c):
        for z in range(planes - 1, -1, -1):
            for p in range(PLANE):
                dev = z * PLANE + p
                if relayed(p, z):
                    yield lend(c, p, z)
                elif dev != c:
                    yield row(c, dev, jnp.int32(dev), c)

    def relays():
        for p in range(PLANE):
            zs = [z for z in range(planes - 1, 0, -1) if relayed(p, z)]
            if zs:
                yield p, zs

    for c, (lo, hi, cap) in enumerate(CAPS):
        @pl.when((me >= lo) & (me < hi))
        def _(c=c):
            own(c).start()
            if c < HOT:
                for copy in hot_sends(c):
                    copy.start()
            else:
                others(n, me, lambda k, dev: row(c, k, dev, me).start())

    for p, zs in relays():
        @pl.when(me == p)
        def _(zs=zs):
            for z in zs:
                for c in range(HOT):
                    lend(c, 0, z).wait_recv()
                    hand_on(c, z).start()

    for c, (lo, hi, cap) in enumerate(CAPS):
        def one(dev, carry, c=c):
            @pl.when(dev != me)
            def _():
                row(c, 0, dev, dev).wait_recv()

            return carry

        lax.fori_loop(lo, hi, one, 0)

    for c, (lo, hi, cap) in enumerate(CAPS):
        @pl.when((me >= lo) & (me < hi))
        def _(c=c):
            own(c).wait()
            if c < HOT:
                for copy in hot_sends(c):
                    copy.wait_send()
            else:
                others(n, me, lambda k, dev: row(c, k, dev, me).wait_send())

    for p, zs in relays():
        @pl.when(me == p)
        def _(zs=zs):
            for z in zs:
                for c in range(HOT):
                    hand_on(c, z).wait_send()


def swap(n, rows):
    planes = n // PLANE
    most = max(cap for _, _, cap in CAPS[:HOT])
    return pl.pallas_call(
        lambda *refs: swap_kernel(n, *refs),
        out_shape=jax.ShapeDtypeStruct((bases()[1], rows.shape[2]), rows.dtype),
        in_specs=[pl.BlockSpec(memory_space=pl.ANY)], out_specs=pl.BlockSpec(memory_space=pl.ANY),
        scratch_shapes=[pltpu.VMEM((HOT, planes - 1, most, rows.shape[2]), rows.dtype), pltpu.SemaphoreType.DMA((n,)),
                        pltpu.SemaphoreType.DMA((n,)), pltpu.SemaphoreType.DMA((HOT, planes - 1)),
                        pltpu.SemaphoreType.DMA((HOT, planes - 1)), pltpu.SemaphoreType.DMA],
        compiler_params=pltpu.CompilerParams(collective_id=1, has_side_effects=True))(rows)


def solution(mesh):
    def local_step(token_ids, tok_shard, pos_table, type_row, emb_gain, emb_bias, w_qkv, b_qkv, w_out, b_out,
                   ln1_gain, ln1_bias, w_ffn_in, b_ffn_in, w_ffn_out, b_ffn_out, ln2_gain, ln2_bias):
        n_dev = mesh.shape['fsdp']
        me = lax.axis_index('fsdp')
        batch_dev, seq_len = token_ids.shape
        n_tok = batch_dev * seq_len
        shard_rows, width = tok_shard.shape
        num_heads, head_dim = w_out.shape[0], w_out.shape[1]
        ids = token_ids.reshape(n_tok)
        keep = ids != PAD_ID
        asks = keep & (ids >= HEAD)
        owner = jnp.where(asks, ids // shard_rows, n_dev)
        place = jnp.arange(n_tok, dtype=jnp.int32)
        lanes = jnp.arange(128, dtype=jnp.int32)
        mine = (owner[:, None] == lanes[None, :]) & (lanes < n_dev)[None, :]
        before = (place[None, :] < place[:, None]).astype(jnp.bfloat16)
        ranks = jnp.dot(before, mine.astype(jnp.bfloat16), preferred_element_type=jnp.float32)
        count = jnp.sum(mine.astype(jnp.float32), axis=0)
        rank = jnp.sum(jnp.where(mine, ranks, 0.0), axis=1).astype(jnp.int32)
        starts, slots = bases()
        cap, base = jnp.zeros_like(owner), jnp.zeros_like(owner)
        for (lo, hi, c), b in zip(CAPS, starts):
            inside = (owner >= lo) & (owner < hi)
            cap = jnp.where(inside, c, cap)
            base = jnp.where(inside, b + (owner - lo) * c, base)
        fits = rank < cap
        slot = jnp.where(fits, base + rank, -1)
        wide = slots + -slots % 128
        slotted = jnp.sum(jnp.where(slot[:, None] == jnp.arange(wide, dtype=jnp.int32)[None, :],
                                    ids.astype(jnp.float32)[:, None], 0.0), axis=0)

        small = [emb_gain, emb_bias, ln1_gain, ln1_bias, ln2_gain, ln2_bias, b_out, b_ffn_out, b_qkv, b_ffn_in]
        message = jnp.concatenate([slotted, count] + small)
        message = jnp.pad(message, (0, -message.shape[0] % 1024))
        told, piece = tell(n_dev, message.reshape(-1, 128), tok_shard)
        told = told.reshape(n_dev, -1)
        parts = [piece, w_qkv.T, w_out.reshape(num_heads * head_dim, -1).T, w_ffn_in.T, w_ffn_out]
        weights = lax.all_gather(jnp.concatenate(parts, axis=0), 'fsdp', axis=0, tiled=False)

        at = wide + 128
        vectors = []
        for v in small:
            vectors.append(told[:, at:at + v.shape[0]].reshape(-1))
            at += v.shape[0]
        emb_g, emb_b, ln1_g, ln1_b, ln2_g, ln2_b, b_out_f, b_back_f, b_qkv_f, b_in_f = vectors

        my_base = jnp.int32(0)
        for (lo, hi, c), b in zip(CAPS, starts):
            my_base = jnp.where((me >= lo) & (me < hi), b + (me - lo) * c, my_base)
        most = max(c for _, _, c in CAPS)
        wanted = lax.dynamic_slice(told, (0, my_base), (n_dev, most)).astype(jnp.int32) - me * shard_rows
        wanted = jnp.clip(wanted, 0, shard_rows - 1)
        wanted = wanted.reshape(n_dev // PLANE, PLANE, most).transpose(1, 0, 2)
        rows = jnp.take(tok_shard, wanted.reshape(-1), axis=0, mode='clip').reshape(n_dev, most, width)
        got = swap(n_dev, rows)
        spot = jnp.where(ids < HEAD, head_spot(n_dev, ids), HEAD + jnp.maximum(slot, 0))

        caps = jnp.concatenate([jnp.full((hi - lo,), c, jnp.float32) for lo, hi, c in CAPS])
        left = jnp.max(told[:, wide:wide + n_dev] - caps[None, :])
        rounds = (jnp.maximum(left, 0.0).astype(jnp.int32) + EXTRA - 1) // EXTRA

        def again(state):
            r, rows_now = state
            extra = rank - cap - r * EXTRA
            live = asks & (extra >= 0) & (extra < EXTRA)
            at_slot = jnp.where(live, owner * EXTRA + extra, n_dev * EXTRA)
            ask = jnp.zeros((n_dev * EXTRA + 1,), jnp.int32).at[at_slot].set(ids)[:-1]
            asked = lax.all_to_all(ask.reshape(n_dev, EXTRA), 'fsdp', 0, 0, tiled=True)
            asked = jnp.clip(asked - me * shard_rows, 0, shard_rows - 1)
            found = jnp.take(tok_shard, asked.reshape(-1), axis=0, mode='clip').reshape(n_dev, EXTRA, width)
            back = lax.all_to_all(found, 'fsdp', 0, 0, tiled=True).reshape(n_dev * EXTRA, width)
            new = jnp.take(back, jnp.where(live, at_slot, 0), axis=0, mode='clip')
            return r + 1, jnp.where(live[:, None], new, rows_now)

        def slow(rows_now):
            return lax.while_loop(lambda state: state[0] < rounds, again, (jnp.int32(0), rows_now))[1]

        rows = jnp.take(got, jnp.maximum(slot, 0), axis=0, mode='clip')
        rows = lax.cond(rounds > 0, slow, lambda r: r, rows)
        vecs = jnp.stack([emb_g, emb_b, ln1_g, ln1_b, ln2_g, ln2_b, b_out_f, b_back_f])
        return layer(num_heads, head_dim, batch_dev, spot, rows, pos_table, type_row, vecs, b_qkv_f, b_in_f, weights,
                     [w.shape[0] for w in parts])

    vec_spec = P('fsdp')
    in_specs = (P('fsdp', None), P('fsdp', None), P(None, None), P(None), vec_spec, vec_spec,
                P(None, 'fsdp'), vec_spec, P(None, None, 'fsdp'), vec_spec, vec_spec, vec_spec,
                P(None, 'fsdp'), vec_spec, P('fsdp', None), vec_spec, vec_spec, vec_spec)
    return jax.shard_map(local_step, mesh=mesh, in_specs=in_specs, out_specs=P('fsdp', None, None), check_vma=False)
```
